32 devices in a mesh: gx: 4 (over z), gy: 4 (over x, core), gz: 2 (over y).
Axes of the slice: x: 2, y: 2, z: 4, core: 2. Of those that a mesh axis runs over, the one named last changes fastest.
Arguments:
- positions: float32 [3, 4, 4, 2, 128], P(None, 'gx', 'gy', 'gz'), may hold values from 0 to 24, as said below
- occupancy: int32 [4, 4, 2, 128], P('gx', 'gy', 'gz'), may hold values from 0 to 1
- neighbours: int32 [56, 4, 4, 2, 128], P(None, 'gx', 'gy', 'gz'), may hold values from 0 to 639, as said below
- keep: int32 [56, 4, 4, 2, 128], P(None, 'gx', 'gy', 'gz'), may hold values from 0 to 1, as said below
- face_x: int32 [4, 4, 2, 2, 64], P('gx', 'gy', 'gz'), may hold values from 0 to 127, as said below
- face_y: int32 [4, 4, 2, 2, 128], P('gx', 'gy', 'gz'), may hold values from 0 to 255, as said below
- face_z: int32 [4, 4, 2, 128], P('gx', 'gy', 'gz'), may hold values from 0 to 511, as said below
- radial_one: float32 [8, 128], replicated, may hold values from -2 to 2
- mix_one: bfloat16 [384, 128], replicated, may hold values from -0.3125 to 0.3125
- embed: float32 [128], replicated, may hold values from -3 to 3
- radial_two: float32 [8, 128], replicated, may hold values from -3 to 3
- mix_two: bfloat16 [384, 128], replicated, may hold values from -0.3125 to 0.3125
- read_one: float32 [128], replicated, may hold values from -0.4375 to 0.4375
- read_hidden: float32 [128, 16], replicated, may hold values from -0.5 to 0.5
- read_out: float32 [16], replicated, may hold values from -1.5 to 1.5
Outputs:
- energies: float32 [4, 4, 2, 128], P('gx', 'gy', 'gz')
- forces: float32 [3, 4, 4, 2, 128], P(None, 'gx', 'gy', 'gz')
The draws below stay inside these ranges and needn't reach their ends.
Inputs may be any that keep to these rules, and one draw needn't show every extreme that they name: `positions`: coordinates in angstrom in the box's own frame; any two atoms named by one list entry lie at least 1.4 apart, counted with the periodic images along gx and gy. `neighbours`: Where the neighbour would lie outside the slab, the entry names the atom at the opposite offset and keep is 0. `keep`: 0 where the atom's slot or the neighbour's slot is empty, or the entry is a pad. `face_x`: distinct own slots; entry 0 lists the slots seen by the lower box, entry 1 by the higher box. `face_y`: distinct rows of the own and x-ghost part of the list; entry 0 for the lower box along gy, entry 1 for the higher. `face_z`: distinct rows of the own, x- and y-ghost part of the list, seen by the other box along gz.
All inputs are finite; a program needn't handle non-finite values.
Results may differ from the reference program's by a relative error of at most 0.01.
Values may be sent and summed in bfloat16 or wider, within the bound.
No kernel may reach another device: no remote copies, remote signals or barrier semaphores. Data moves between devices by JAX's collectives and lax.ppermute only.
A program may use at most 128 MiB of HBM per device.

```python
import jax
import jax.numpy as jnp
import numpy as np
from jax import lax

C = 128
NB = 8
HID = 16
NEIGH = 56
DEPTH = 2
LX = 4
LY = 4
LZ = 8
SLOTS = 128
BOXES_X = 4
BOXES_Y = 4
BOXES_Z = 2


SPACING = 1.8


def offsets_table():
    entries = []
    for shift_x in range(-2, 3):
        for shift_y in range(-2, 3):
            for shift_z in range(-2, 3):
                reach_sq = shift_x * shift_x + shift_y * shift_y + shift_z * shift_z
                if 0 < reach_sq <= 5:
                    entries.append((shift_x, shift_y, shift_z))
    return np.array(entries, dtype=np.int32)


def site_coords(site_ids):
    return (site_ids // (LY * LZ), site_ids // LZ % LY, site_ids % LZ)


def slab_plan(key):
    grid_shape = (BOXES_X, BOXES_Y, BOXES_Z)
    scores = jax.random.randint(jax.random.fold_in(key, 11), grid_shape + (SLOTS,), 0, 2 ** 30 // SLOTS)
    scores = scores * SLOTS + jnp.arange(SLOTS, dtype=jnp.int32)
    site_of_slot = jnp.argsort(scores, axis=-1).astype(jnp.int32)
    slot_of_site = jnp.argsort(site_of_slot, axis=-1).astype(jnp.int32)
    vacancy = jax.random.randint(jax.random.fold_in(key, 12), grid_shape + (1,), 0, 31)
    present = (jax.random.randint(jax.random.fold_in(key, 13), grid_shape + (SLOTS,), 0, 100) >= vacancy).astype(jnp.int32)
    return (site_of_slot, slot_of_site, present)


def extended_slot(slot_of_site, coord_x, coord_y, coord_z):
    grid_shape = slot_of_site.shape[:3]
    coord_x, coord_y, coord_z = jnp.broadcast_arrays(jnp.asarray(coord_x).astype(jnp.int32), jnp.asarray(coord_y).astype(jnp.int32), jnp.asarray(coord_z).astype(jnp.int32))
    target_shape = grid_shape + coord_x.shape[-1:]
    coord_x = jnp.broadcast_to(coord_x, target_shape)
    coord_y = jnp.broadcast_to(coord_y, target_shape)
    coord_z = jnp.broadcast_to(coord_z, target_shape)
    x_face_len = DEPTH * LY * LZ
    y_face_len = DEPTH * (LX + 2 * DEPTH) * LZ
    first_end = SLOTS + 2 * x_face_len
    second_end = first_end + 2 * y_face_len
    inside_site = (jnp.clip(coord_x, 0, LX - 1) * LY + jnp.clip(coord_y, 0, LY - 1)) * LZ + jnp.clip(coord_z, 0, LZ - 1)
    result = jnp.take_along_axis(slot_of_site, inside_site, axis=-1)
    x_low = SLOTS + ((coord_x + DEPTH) * LY + coord_y) * LZ + coord_z
    x_high = SLOTS + x_face_len + ((coord_x - LX) * LY + coord_y) * LZ + coord_z
    y_low = first_end + ((coord_x + DEPTH) * DEPTH + coord_y + DEPTH) * LZ + coord_z
    y_high = first_end + y_face_len + ((coord_x + DEPTH) * DEPTH + coord_y - LY) * LZ + coord_z
    z_part = second_end + ((coord_x + DEPTH) * (LY + 2 * DEPTH) + coord_y + DEPTH) * DEPTH + jnp.where(coord_z >= LZ, coord_z - LZ, coord_z + DEPTH)
    result = jnp.where(coord_x < 0, x_low, result)
    result = jnp.where(coord_x >= LX, x_high, result)
    result = jnp.where(coord_y < 0, y_low, result)
    result = jnp.where(coord_y >= LY, y_high, result)
    result = jnp.where((coord_z < 0) | (coord_z >= LZ), z_part, result)
    return result.astype(jnp.int32)


def neighbour_plan(key):
    site_of_slot, slot_of_site, present = slab_plan(key)
    grid_shape = (BOXES_X, BOXES_Y, BOXES_Z)
    full_shape = grid_shape + (NEIGH, SLOTS)
    flat_shape = grid_shape + (NEIGH * SLOTS,)
    offset_table = offsets_table()
    base_x, base_y, base_z = site_coords(np.arange(SLOTS))
    target_x = base_x[None, :] + offset_table[:, 0:1]
    target_y = base_y[None, :] + offset_table[:, 1:2]
    target_z = base_z[None, :] + offset_table[:, 2:3]
    mirror_x = base_x[None, :] - offset_table[:, 0:1]
    mirror_y = base_y[None, :] - offset_table[:, 1:2]
    mirror_z = base_z[None, :] - offset_table[:, 2:3]
    box_x = jnp.arange(BOXES_X).reshape(BOXES_X, 1, 1, 1, 1)
    box_y = jnp.arange(BOXES_Y).reshape(1, BOXES_Y, 1, 1, 1)
    box_z = jnp.arange(BOXES_Z).reshape(1, 1, BOXES_Z, 1, 1)
    outside = (box_z == 0) & (target_z < 0) | (box_z == BOXES_Z - 1) & (target_z >= LZ)
    outside = jnp.broadcast_to(outside, full_shape)
    pick_x = jnp.where(outside, mirror_x, target_x)
    pick_y = jnp.where(outside, mirror_y, target_y)
    pick_z = jnp.where(outside, mirror_z, target_z)
    slots_site = extended_slot(slot_of_site, pick_x.reshape(flat_shape), pick_y.reshape(flat_shape), pick_z.reshape(flat_shape)).reshape(full_shape)
    owner_x = jnp.broadcast_to((box_x + target_x // LX) % BOXES_X, full_shape)
    owner_y = jnp.broadcast_to((box_y + target_y // LY) % BOXES_Y, full_shape)
    owner_z = jnp.broadcast_to((box_z + target_z // LZ) % BOXES_Z, full_shape)
    target_site = jnp.broadcast_to(jnp.asarray((target_x % LX * LY + target_y % LY) * LZ + target_z % LZ), full_shape)
    there_present = present[owner_x, owner_y, owner_z, target_site]
    here_present = jnp.broadcast_to(present[:, :, :, None, :], full_shape)
    keep_site = jnp.where(outside, 0, here_present * there_present)
    slot_order = jnp.broadcast_to(site_of_slot[:, :, :, None, :], full_shape)
    nbr_slot = jnp.take_along_axis(slots_site, slot_order, axis=-1)
    keep_slot = jnp.take_along_axis(keep_site, slot_order, axis=-1)
    return (jnp.moveaxis(nbr_slot, 3, 0).astype(jnp.int32), jnp.moveaxis(keep_slot, 3, 0).astype(jnp.int32))


def draw_positions(key, part):
    site_of_slot, slot_of_site, present = slab_plan(key)
    coord_x, coord_y, coord_z = site_coords(site_of_slot)
    lattice = (jnp.stack([coord_x, coord_y, coord_z]).astype(jnp.float32) + 0.5) * SPACING
    noise_key = jax.random.fold_in(key, 21)
    jitter = jnp.clip(0.1 * jax.random.normal(noise_key, lattice.shape, jnp.float32), -0.2, 0.2)
    return lattice + jitter


def draw_occupancy(key, part):
    site_of_slot, slot_of_site, present = slab_plan(key)
    return jnp.take_along_axis(present, site_of_slot, axis=-1).astype(jnp.int32)


def draw_neighbours(key, part):
    return neighbour_plan(key)[0]


def draw_keep(key, part):
    return neighbour_plan(key)[1]


def draw_face_x(key, part):
    site_of_slot, slot_of_site, present = slab_plan(key)
    x_face_len = DEPTH * LY * LZ
    return jnp.stack([slot_of_site[..., :x_face_len], slot_of_site[..., SLOTS - x_face_len:]], axis=-2).astype(jnp.int32)


def draw_face_y(key, part):
    site_of_slot, slot_of_site, present = slab_plan(key)
    coord_x, lane_y, coord_z = np.meshgrid(np.arange(-DEPTH, LX + DEPTH), np.arange(DEPTH), np.arange(LZ), indexing='ij')
    coord_x = coord_x.reshape(-1)
    lane_y = lane_y.reshape(-1)
    coord_z = coord_z.reshape(-1)
    lower = extended_slot(slot_of_site, coord_x, lane_y, coord_z)
    upper = extended_slot(slot_of_site, coord_x, LY - DEPTH + lane_y, coord_z)
    return jnp.stack([lower, upper], axis=-2).astype(jnp.int32)


def draw_face_z(key, part):
    site_of_slot, slot_of_site, present = slab_plan(key)
    coord_x, coord_y, lane_z = np.meshgrid(np.arange(-DEPTH, LX + DEPTH), np.arange(-DEPTH, LY + DEPTH), np.arange(DEPTH), indexing='ij')
    box_z = jnp.arange(BOXES_Z).reshape(1, 1, BOXES_Z, 1)
    coord_z = jnp.where(box_z == 0, LZ - DEPTH + lane_z.reshape(-1), lane_z.reshape(-1))
    return extended_slot(slot_of_site, coord_x.reshape(-1), coord_y.reshape(-1), coord_z)


def gaussian(own_key, dims, deviation, bound, held_as=jnp.bfloat16):
    values = deviation * jax.random.normal(own_key, dims, jnp.float32)
    return jnp.clip(values, min=-bound, max=bound).astype(held_as)


def setup_inputs(seed: int = 0) -> dict:
    key_of = jax.random.split(jax.random.key(seed), 16)
    return {
        "positions": draw_positions(jax.random.fold_in(key_of[15], 71), 0),
        "occupancy": draw_occupancy(jax.random.fold_in(key_of[15], 71), 0),
        "neighbours": draw_neighbours(jax.random.fold_in(key_of[15], 71), 0),
        "keep": draw_keep(jax.random.fold_in(key_of[15], 71), 0),
        "face_x": draw_face_x(jax.random.fold_in(key_of[15], 71), 0),
        "face_y": draw_face_y(jax.random.fold_in(key_of[15], 71), 0),
        "face_z": draw_face_z(jax.random.fold_in(key_of[15], 71), 0),
        "radial_one": gaussian(key_of[7], (NB, C), NB ** -0.5, 2.0, jnp.float32),
        "mix_one": gaussian(key_of[8], (3 * C, C), (3 * C) ** -0.5, 0.3125),
        "embed": gaussian(key_of[9], (C,), 0.5, 3.0, jnp.float32),
        "radial_two": gaussian(key_of[10], (NB, C), 0.8, 3.0, jnp.float32),
        "mix_two": gaussian(key_of[11], (3 * C, C), (3 * C) ** -0.5, 0.3125),
        "read_one": gaussian(key_of[12], (C,), 0.03, 0.4375, jnp.float32),
        "read_hidden": gaussian(key_of[13], (C, HID), C ** -0.5, 0.5, jnp.float32),
        "read_out": gaussian(key_of[14], (HID,), HID ** -0.5, 1.5, jnp.float32),
    }


SPACING = 1.8
CUTOFF = 5.0
SPREAD = 0.4
HIGHEST = lax.Precision.HIGHEST

def harmonics(unit_vec):
    unit_x, unit_y, unit_z = (unit_vec[0], unit_vec[1], unit_vec[2])
    root_three = 3.0 ** 0.5
    root_fifteen = 15.0 ** 0.5
    root_five = 5.0 ** 0.5
    return jnp.stack([jnp.ones_like(unit_x), root_three * unit_x, root_three * unit_y, root_three * unit_z, root_fifteen * unit_x * unit_y, root_fifteen * unit_y * unit_z, 0.5 * root_five * (3.0 * unit_z * unit_z - 1.0), root_fifteen * unit_x * unit_z, 0.5 * root_fifteen * (unit_x * unit_x - unit_y * unit_y)])

def radial_basis(distance):
    orders = jnp.arange(1, NB + 1).astype(jnp.float32)[:, None, None]
    scaled = distance / CUTOFF
    envelope = jnp.where(scaled < 1.0, (1.0 - scaled * scaled) ** 2, 0.0)
    return (2.0 / CUTOFF) ** 0.5 * jnp.sin(orders * jnp.pi * scaled) / distance * envelope

def edge_frame(source, centre, nbr_slots, edge_weight):
    offset_vec = source[:, nbr_slots] - centre[:, None, :]
    distance = jnp.sqrt(lax.optimization_barrier(jnp.sum(offset_vec * offset_vec, axis=0)))
    return (radial_basis(distance) * edge_weight, harmonics(offset_vec / distance))

def moments_one(source, centre, nbr_slots, edge_weight):
    basis, angular = edge_frame(source, centre, nbr_slots, edge_weight)
    return jnp.einsum('kja,mja->kma', basis, angular, precision=HIGHEST)

def invariants(amplitude):
    return jnp.concatenate([amplitude[:, 0, :], lax.optimization_barrier(jnp.sum(amplitude[:, 1:4, :] ** 2, axis=1)), lax.optimization_barrier(jnp.sum(amplitude[:, 4:9, :] ** 2, axis=1))], axis=1)

def layer_one_tail(moments, radial_one, mix_one, embed):
    amplitude = SPREAD * jnp.einsum('kma,kc->amc', moments, radial_one, precision=HIGHEST)
    mixed_in = invariants(amplitude).astype(jnp.bfloat16)
    return jnp.dot(mixed_in, mix_one, preferred_element_type=jnp.float32) + embed

def pick_block(total_rows):
    block_size = min(total_rows, 1152)
    while total_rows % block_size:
        block_size = block_size - 1
    return block_size

def layer_two(source, features, nbr_slots, edge_weight, occupied, radial_two, mix_two, read_one, read_hidden, read_out):
    edge_count, atom_count = nbr_slots.shape
    block_size = pick_block(atom_count)
    groups = atom_count // block_size
    widened = features.astype(jnp.float32)

    def per_block(pieces):
        block_slots, block_weight, centre, block_occupied, base_rows = pieces
        basis, angular = edge_frame(source, centre, block_slots, block_weight)
        radial = jnp.einsum('kja,kc->jac', basis, radial_two, precision=HIGHEST)
        message = radial * widened[block_slots]
        amplitude = SPREAD * jnp.einsum('mja,jac->amc', angular, message, precision=HIGHEST)
        mixed_rows = jnp.dot(invariants(amplitude).astype(jnp.bfloat16), mix_two, preferred_element_type=jnp.float32) + base_rows
        hidden = jax.nn.silu(jnp.dot(mixed_rows, read_hidden, precision=HIGHEST))
        return block_occupied * (jnp.dot(base_rows, read_one, precision=HIGHEST) + jnp.dot(hidden, read_out, precision=HIGHEST))
    pieces = (nbr_slots.reshape(edge_count, groups, block_size).transpose(1, 0, 2), edge_weight.reshape(edge_count, groups, block_size).transpose(1, 0, 2), source[:, :atom_count].reshape(3, groups, block_size).transpose(1, 0, 2), occupied.reshape(groups, block_size), widened[:atom_count].reshape(groups, block_size, widened.shape[1]))
    return lax.map(per_block, pieces).reshape(atom_count)

def box_take(values, lists, axis_pos):

    def single(values_box, slot_list):
        return jnp.take(values_box, slot_list, axis=axis_pos)
    return jax.vmap(jax.vmap(jax.vmap(single)))(values, lists)

def ghost_positions(coords, face_x, face_y, face_z):
    step_x = jnp.array([LX * SPACING, 0.0, 0.0], jnp.float32)[:, None]
    step_y = jnp.array([0.0, LY * SPACING, 0.0], jnp.float32)[:, None]
    step_z = jnp.array([0.0, 0.0, LZ * SPACING], jnp.float32)[:, None]
    payload = box_take(coords, face_x, 1)
    widened = jnp.concatenate([coords, jnp.roll(payload[..., 1, :], 1, axis=0) - step_x, jnp.roll(payload[..., 0, :], -1, axis=0) + step_x], axis=-1)
    payload = box_take(widened, face_y, 1)
    widened = jnp.concatenate([widened, jnp.roll(payload[..., 1, :], 1, axis=1) - step_y, jnp.roll(payload[..., 0, :], -1, axis=1) + step_y], axis=-1)
    payload = box_take(widened, face_z, 1)
    upward = jnp.where(jnp.arange(BOXES_Z) == 0, 1.0, -1.0).astype(jnp.float32)[None, None, :, None, None]
    return jnp.concatenate([widened, jnp.roll(payload, 1, axis=2) + upward * step_z], axis=-1)

def ghost_features(rows_grid, face_x, face_y, face_z):
    payload = box_take(rows_grid, face_x, 0)
    widened = jnp.concatenate([rows_grid, jnp.roll(payload[:, :, :, 1], 1, axis=0), jnp.roll(payload[:, :, :, 0], -1, axis=0)], axis=3)
    payload = box_take(widened, face_y, 0)
    widened = jnp.concatenate([widened, jnp.roll(payload[:, :, :, 1], 1, axis=1), jnp.roll(payload[:, :, :, 0], -1, axis=1)], axis=3)
    payload = box_take(widened, face_z, 0)
    return jnp.concatenate([widened, jnp.roll(payload, 1, axis=2)], axis=3)

def reference(positions, occupancy, neighbours, keep, face_x, face_y, face_z, radial_one, mix_one, embed, radial_two, mix_two, read_one, read_hidden, read_out):
    grid_shape = occupancy.shape[:3]
    slot_count = occupancy.shape[3]
    box_count = grid_shape[0] * grid_shape[1] * grid_shape[2]
    coords = jnp.moveaxis(positions, 0, 3)
    nbr_slots = jnp.moveaxis(neighbours, 0, 3)
    edge_weight = jnp.moveaxis(keep, 0, 3).astype(jnp.float32)
    occupied = occupancy.astype(jnp.float32)

    def flatten(values):
        return values.reshape((box_count,) + values.shape[3:])

    def first_moments(pieces):
        return moments_one(pieces[0], pieces[0][:, :slot_count], pieces[1], pieces[2])

    def first_tail(moments):
        return layer_one_tail(moments, radial_one, mix_one, embed)

    def second_layer(pieces):
        return layer_two(pieces[0], pieces[1], pieces[2], pieces[3], pieces[4], radial_two, mix_two, read_one, read_hidden, read_out)

    def energy_of(coords_in):
        source = flatten(ghost_positions(coords_in, face_x, face_y, face_z))
        moments = lax.map(jax.checkpoint(first_moments), (source, flatten(nbr_slots), flatten(edge_weight)))
        first_rows = lax.map(first_tail, moments)
        features = ghost_features(first_rows.reshape(grid_shape + first_rows.shape[1:]), face_x, face_y, face_z).astype(jnp.bfloat16)
        energies = lax.map(jax.checkpoint(second_layer), (source, flatten(features), flatten(nbr_slots), flatten(edge_weight), flatten(occupied)))
        return energies.reshape(occupancy.shape)
    energies, pull_back = jax.vjp(energy_of, coords)
    gradient, = pull_back(jnp.ones_like(energies))
    return (energies, -jnp.moveaxis(gradient, 3, 0))
```

```python
import functools
import math

import jax
import jax.numpy as jnp
from jax import lax
from jax.experimental import pallas as pl
from jax.experimental.pallas import tpu as pltpu
from jax.sharding import PartitionSpec as P

NB = 8
LX = 4
LY = 4
LZ = 8

SPACING = 1.8
CUTOFF = 5.0
SPREAD = 0.4
HIGHEST = lax.Precision.HIGHEST
F32 = jnp.float32
BF16 = jnp.bfloat16

ROOT3 = 3.0**0.5
ROOT5 = 5.0**0.5
ROOT15 = 15.0**0.5
GROUP = 4


def dot(a, b, ca=1, cb=0, precision=None):
    return lax.dot_general(
        a, b, (((ca,), (cb,)), ((), ())), precision=precision, preferred_element_type=F32
    )


def split2(x):
    hi = x.astype(BF16)
    lo = (x - hi.astype(F32)).astype(BF16)
    return hi, lo


def dot_split(a, b, ca=1, cb=0):
    hi, lo = split2(b)
    return dot(a, hi, ca, cb) + dot(a, lo, ca, cb)


def onehot(row, size):
    count = row.shape[-1]
    ids = lax.broadcasted_iota(jnp.int32, (size, count), 0)
    return jnp.where(ids == row, 1.0, 0.0).astype(BF16)


def lane_pick(blocks, rows):
    width = blocks[0].shape[-1]
    shift = width.bit_length() - 1
    lane = rows & (width - 1)
    block = rows >> shift
    out = jnp.take_along_axis(blocks[0], lane, axis=1)
    for index in range(1, len(blocks)):
        part = jnp.take_along_axis(blocks[index], lane, axis=1)
        out = jnp.where(block == index, part, out)
    return out


def spread_rows(row, count):
    return jnp.broadcast_to(row, (count, row.shape[-1]))


def padded_coords(pos_ref):
    rows = [pos_ref[i : i + 1, :] for i in range(3)]
    return jnp.concatenate(rows + [jnp.zeros_like(rows[0])] * 5, axis=0)


def face_row(fx_ref):
    return jnp.concatenate([fx_ref[1:2, :], fx_ref[0:1, :]], axis=1)


def low_lanes(shape):
    return lax.broadcasted_iota(jnp.int32, shape, 1) < shape[1] // 2


def shift_rows(shape, axis, amount):
    ids = lax.broadcasted_iota(jnp.int32, shape, 0)
    return jnp.where(ids == axis, amount, 0.0)


def pos_x_kernel(pos_ref, fx_ref, out_ref):
    coords = padded_coords(pos_ref)
    out_ref[...] = lane_pick([coords], spread_rows(face_row(fx_ref), 8))


def pos_y_kernel(pos_ref, lo_ref, hi_ref, fy_ref, p1_ref, up_ref, down_ref):
    coords = padded_coords(pos_ref)
    shape = coords.shape
    low = lo_ref[...] - shift_rows(shape, 0, LX * SPACING)
    high = hi_ref[...] + shift_rows(shape, 0, LX * SPACING)
    ghost = jnp.where(low_lanes(shape), low, high)
    p1_ref[...] = ghost
    up_ref[...] = lane_pick([coords, ghost], spread_rows(fy_ref[1:2, :], 8))
    down_ref[...] = lane_pick([coords, ghost], spread_rows(fy_ref[0:1, :], 8))


def pos_z_kernel(pos_ref, p1_ref, lo_ref, hi_ref, fz_ref, p2_ref, p3_ref, out_ref):
    coords = padded_coords(pos_ref)
    shape = coords.shape
    low = lo_ref[...] - shift_rows(shape, 1, LY * SPACING)
    high = hi_ref[...] + shift_rows(shape, 1, LY * SPACING)
    p2_ref[...] = low
    p3_ref[...] = high
    out_ref[...] = lane_pick([coords, p1_ref[...], low, high], spread_rows(fz_ref[...], 8))


def layer_one_kernel(
    pos_ref,
    p1_ref,
    p2_ref,
    p3_ref,
    pz_ref,
    zs_ref,
    nbr_ref,
    keep_ref,
    fx_ref,
    radial_ref,
    mix_ref,
    embed_ref,
    unit_ref,
    rinv_ref,
    basis_ref,
    slope_ref,
    amp_ref,
    h0_ref,
    send_ref,
    mom_ref,
):
    entries, atoms = nbr_ref.shape
    nbr = nbr_ref[...]
    lane = nbr & (atoms - 1)
    block = nbr >> (atoms.bit_length() - 1)
    last = pz_ref[...] + shift_rows(pz_ref.shape, 2, zs_ref[0])
    tables = [padded_coords(pos_ref), p1_ref[...], p2_ref[...], p3_ref[...], last]
    vec = []
    for axis in range(3):
        got = None
        for index, table in enumerate(tables):
            spread = spread_rows(table[axis : axis + 1, :], entries)
            part = jnp.take_along_axis(spread, lane, axis=1)
            got = part if index == 0 else jnp.where(block == index, part, got)
        vec.append(got - pos_ref[axis : axis + 1, :])
    r_sq = vec[0] * vec[0] + vec[1] * vec[1] + vec[2] * vec[2]
    dist = jnp.sqrt(r_sq)
    rinv = 1.0 / dist
    ux, uy, uz = (v * rinv for v in vec)
    rinv_ref[...] = rinv
    unit_ref[0:entries, :] = ux
    unit_ref[entries : 2 * entries, :] = uy
    unit_ref[2 * entries : 3 * entries, :] = uz
    scaled = jnp.minimum(dist * (1.0 / CUTOFF), 1.0)
    phase = scaled * math.pi
    sine = jnp.sin(phase)
    cosine = jnp.cos(phase)
    inner = 1.0 - scaled * scaled
    weight = keep_ref[...].astype(F32) * (2.0 / CUTOFF) ** 0.5
    env = weight * inner * inner * rinv
    env_slope = -env * rinv - weight * rinv * (4.0 / CUTOFF) * scaled * inner
    twice = 2.0 * cosine
    s_prev, s_now = jnp.zeros_like(sine), sine
    c_prev, c_now = jnp.ones_like(cosine), cosine
    basis = []
    for k in range(NB):
        bk = s_now * env
        basis.append(bk)
        basis_ref[k * entries : (k + 1) * entries, :] = bk
        slope_ref[k * entries : (k + 1) * entries, :] = (
            c_now * env * ((k + 1) * math.pi / CUTOFF) + s_now * env_slope
        )
        s_prev, s_now = s_now, twice * s_now - s_prev
        c_prev, c_now = c_now, twice * c_now - c_prev
    angular = harmonics(ux, uy, uz)
    for m in range(9):
        for k in range(NB):
            prod = basis[k] if m == 0 else basis[k] * angular[m]
            mom_ref[k : k + 1, m * atoms : (m + 1) * atoms] = jnp.sum(prod, axis=0, keepdims=True)
    amp = SPREAD * dot(radial_ref[...], mom_ref[...], 0, 0, HIGHEST)
    amp_ref[...] = amp
    inv = invariants([amp[:, m * atoms : (m + 1) * atoms] for m in range(9)])
    h1 = dot(mix_ref[...], inv, 0, 0)
    h1 = h1 + dot(embed_ref[...], jnp.ones((1, atoms), F32), 0, 0, HIGHEST)
    h1b = h1.astype(BF16)
    h0_ref[...] = h1b
    send_ref[...] = dot(h1b, onehot(face_row(fx_ref), atoms)).astype(BF16)


def harmonics(ux, uy, uz):
    return [
        None,
        ROOT3 * ux,
        ROOT3 * uy,
        ROOT3 * uz,
        ROOT15 * ux * uy,
        ROOT15 * uy * uz,
        0.5 * ROOT5 * (3.0 * uz * uz - 1.0),
        ROOT15 * ux * uz,
        0.5 * ROOT15 * (ux * ux - uy * uy),
    ]


def invariants(amp):
    first = amp[1] * amp[1] + amp[2] * amp[2] + amp[3] * amp[3]
    second = amp[4] * amp[4] + amp[5] * amp[5] + amp[6] * amp[6]
    second = second + amp[7] * amp[7] + amp[8] * amp[8]
    return jnp.concatenate([amp[0], first, second], axis=0).astype(BF16)


def feat_y_kernel(h0_ref, lo_ref, hi_ref, fy_ref, h1_ref, up_ref, down_ref):
    low = lo_ref[...]
    ghost = jnp.where(low_lanes(low.shape), low.astype(F32), hi_ref[...].astype(F32)).astype(BF16)
    h1_ref[...] = ghost
    table = jnp.concatenate([h0_ref[...], ghost], axis=1)
    size = table.shape[1]
    up_ref[...] = dot(table, onehot(fy_ref[1:2, :], size)).astype(BF16)
    down_ref[...] = dot(table, onehot(fy_ref[0:1, :], size)).astype(BF16)


def feat_z_kernel(h0_ref, h1_ref, h2_ref, h3_ref, fz_ref, out_ref):
    table = jnp.concatenate([h0_ref[...], h1_ref[...], h2_ref[...], h3_ref[...]], axis=1)
    out_ref[...] = dot(table, onehot(fz_ref[...], table.shape[1])).astype(BF16)


def stack3(hi, lo):
    return jnp.concatenate([hi, lo, hi], axis=0).astype(BF16)


def layer_two_kernel(
    h0_ref,
    h1_ref,
    h2_ref,
    h3_ref,
    h4_ref,
    nbr_ref,
    occ_ref,
    unit_ref,
    rinv_ref,
    basis_ref,
    slope_ref,
    radial_ref,
    mix_ref,
    rone_ref,
    rhid_ref,
    rout_ref,
    en_ref,
    gin_ref,
    gz_ref,
    grad_ref,
    oh_ref,
    hg_ref,
    rad_ref,
    slo_ref,
    rq_ref,
    acc_ref,
    d_ref,
    dh_ref,
    rts_ref,
    y_ref,
    table_ref,
):
    entries, atoms = nbr_ref.shape
    channels = h0_ref.shape[0]
    total = 5 * atoms
    steps = entries // GROUP
    width = GROUP * atoms
    blocks = channels // 8
    for index, ref in enumerate((h0_ref, h1_ref, h2_ref, h3_ref, h4_ref)):
        table_ref[:, index * atoms : (index + 1) * atoms] = ref[...]
    rt = radial_ref[...]
    hi = rt.astype(BF16).astype(F32)
    lo = rt - hi
    pad = jnp.zeros((channels - 3 * NB, channels), F32)
    rts_ref[...] = jnp.transpose(jnp.concatenate([hi, hi, lo, pad], axis=0)).astype(BF16)
    ux = unit_ref[0:entries, :]
    uy = unit_ref[entries : 2 * entries, :]
    uz = unit_ref[2 * entries : 3 * entries, :]
    for m, val in enumerate(harmonics(ux, uy, uz)):
        if m:
            y_ref[(m - 1) * entries : m * entries, :] = val
    acc_ref[...] = jnp.zeros_like(acc_ref)

    def radial_cols(ref, first):
        cols = [ref[pl.ds(first + jj, NB, stride=entries), :] for jj in range(GROUP)]
        value = jnp.concatenate(cols, axis=1)
        top = value.astype(BF16).astype(F32)
        return stack3(top, value - top)

    def prepare(step):
        first = step * GROUP
        rows = [nbr_ref[pl.ds(first + jj, 1), :] for jj in range(GROUP)]
        hot = onehot(jnp.concatenate(rows, axis=1), total)
        oh_ref[step] = hot
        hg_ref[step] = dot(table_ref[...], hot)
        rts = rts_ref[:, 0 : 3 * NB]
        rad_ref[step] = dot(rts, radial_cols(basis_ref, first))
        slo_ref[step] = dot(rts, radial_cols(slope_ref, first))

    def accumulate(step):
        first = step * GROUP
        for cb in range(blocks):
            rows = slice(cb * 8, cb * 8 + 8)
            msgs = []
            for jj in range(GROUP):
                cols = slice(jj * atoms, (jj + 1) * atoms)
                msgs.append(hg_ref[step, rows, cols] * rad_ref[step, rows, cols])
            for m in range(9):
                value = acc_ref[m, rows, :]
                for jj in range(GROUP):
                    if m == 0:
                        value = value + msgs[jj]
                    else:
                        yv = y_ref[pl.ds((m - 1) * entries + first + jj, 1), :]
                        value = value + msgs[jj] * yv
                acc_ref[m, rows, :] = value

    prepare(0)

    def forward_body(step, carry):
        accumulate(step - 1)
        prepare(step)
        return carry

    lax.fori_loop(1, steps, forward_body, 0)
    accumulate(steps - 1)

    occ = occ_ref[...].astype(F32)
    ones = jnp.ones((1, atoms), F32)
    amp = [SPREAD * acc_ref[m] for m in range(9)]
    own = h0_ref[...].astype(F32)
    h2 = dot(mix_ref[...], invariants(amp), 0, 0) + own
    pre = dot(rhid_ref[...], h2, 0, 0, HIGHEST)
    sig = 1.0 / (1.0 + jnp.exp(-pre))
    rout = dot(rout_ref[...], ones, 0, 0, HIGHEST)
    rone = dot(rone_ref[...], ones, 0, 0, HIGHEST)
    energy = jnp.sum(own * rone, axis=0, keepdims=True)
    energy = energy + jnp.sum(rout * pre * sig, axis=0, keepdims=True)
    en_ref[...] = occ * energy
    dpre = occ * rout * sig * (1.0 + pre * (1.0 - sig))
    dh2 = dot(rhid_ref[...], dpre, 1, 0, HIGHEST)
    dinv = dot_split(mix_ref[...], dh2)
    low = dinv[channels : 2 * channels]
    top = dinv[2 * channels :]
    own_extra = dh2 + occ * rone
    twice = 2.0 * SPREAD
    d6 = twice * amp[6] * top
    d_ref[0] = SPREAD * dinv[0:channels] - 0.5 * ROOT5 * d6
    for m in range(1, 4):
        d_ref[m] = (twice * ROOT3) * amp[m] * low
    for m in (4, 5, 7, 8):
        d_ref[m] = (twice * 0.5 * ROOT15) * amp[m] * top
    d_ref[6] = (1.5 * ROOT5) * d6
    dh_ref[...] = jnp.zeros_like(dh_ref)

    def reverse(step):
        first = step * GROUP
        units = []
        for jj in range(GROUP):
            units.append([unit_ref[pl.ds(i * entries + first + jj, 1), :] for i in range(3)])
        sums = [[None] * 4 for _ in range(GROUP)]
        for cb in range(blocks):
            rows = slice(cb * 8, cb * 8 + 8)
            d = [d_ref[m, rows, :] for m in range(9)]
            for jj in range(GROUP):
                cols = slice(jj * atoms, (jj + 1) * atoms)
                vx, vy, vz = units[jj]
                hg = hg_ref[step, rows, cols]
                rad = rad_ref[step, rows, cols]
                cx = vy * d[4] + vz * d[7] + vx * d[8]
                cy = vx * d[4] + vz * d[5] - vy * d[8]
                cz = vy * d[5] + vx * d[7] + vz * d[6]
                ex, ey, ez = d[1] + cx, d[2] + cy, d[3] + cz
                q = d[0] + vx * ex + vy * ey + vz * ez
                rq_ref[rows, cols] = rad * q
                msg = hg * rad
                parts = [
                    msg * (ex + cx),
                    msg * (ey + cy),
                    msg * (ez + cz),
                    hg * q * slo_ref[step, rows, cols],
                ]
                for i in range(4):
                    prior = sums[jj][i]
                    sums[jj][i] = parts[i] if prior is None else prior + parts[i]
        for jj in range(GROUP):
            for i in range(4):
                row = pl.ds(i * entries + first + jj, 1)
                grad_ref[row, :] = jnp.sum(sums[jj][i], axis=0, keepdims=True)
        dh_ref[...] += dot(oh_ref[step], rq_ref[...].astype(BF16), 1, 1)

    def reverse_body(step, carry):
        reverse(step)
        return carry

    lax.fori_loop(0, steps, reverse_body, 0)

    inner = 4 * atoms
    gin_ref[0:atoms, :] = (dh_ref[0:atoms, :] + jnp.transpose(own_extra)).astype(BF16)
    gin_ref[atoms:inner, :] = dh_ref[atoms:inner, :].astype(BF16)
    gz_ref[...] = dh_ref[inner:, :].astype(BF16)


def fold_z_kernel(gin_ref, az_ref, fz_ref, acc_ref, low_ref, high_ref):
    size = gin_ref.shape[0]
    half = size // 2
    quarter = half // 2
    rows = gin_ref[...].astype(F32) + dot(onehot(fz_ref[...], size), az_ref[...])
    acc_ref[...] = rows[0:half]
    low_ref[...] = rows[half : half + quarter].astype(BF16)
    high_ref[...] = rows[half + quarter :].astype(BF16)


def fold_y_kernel(acc_ref, a0_ref, a1_ref, fy_ref, own_ref, low_ref, high_ref):
    size = acc_ref.shape[0]
    half = size // 2
    quarter = half // 2
    rows = acc_ref[...]
    rows = rows + dot(onehot(fy_ref[0:1, :], size), a0_ref[...])
    rows = rows + dot(onehot(fy_ref[1:2, :], size), a1_ref[...])
    own_ref[...] = rows[0:half]
    low_ref[...] = rows[half : half + quarter].astype(BF16)
    high_ref[...] = rows[half + quarter :].astype(BF16)


def layer_one_reverse_kernel(
    own_ref,
    a0_ref,
    a1_ref,
    fx_ref,
    amp_ref,
    nbr_ref,
    unit_ref,
    rinv_ref,
    basis_ref,
    slope_ref,
    grad_ref,
    radial_ref,
    mix_ref,
    f0_ref,
    f1_ref,
    f2_ref,
    f3_ref,
    f4_ref,
    dv_ref,
    sc_ref,
):
    entries, atoms = nbr_ref.shape
    channels = own_ref.shape[1]
    rows = own_ref[...]
    rows = rows + dot(onehot(fx_ref[0:1, :], atoms), a0_ref[...])
    rows = rows + dot(onehot(fx_ref[1:2, :], atoms), a1_ref[...])
    cot = jnp.transpose(rows)
    dinv = dot_split(mix_ref[...], cot)
    low = dinv[channels : 2 * channels]
    top = dinv[2 * channels :]
    pieces = [dinv[0:channels]]
    for m in range(1, 9):
        amp = amp_ref[:, m * atoms : (m + 1) * atoms]
        pieces.append(2.0 * amp * (low if m < 4 else top))
    dmom = SPREAD * dot(radial_ref[...], jnp.concatenate(pieces, axis=1), 1, 0, HIGHEST)
    ux = unit_ref[0:entries, :]
    uy = unit_ref[entries : 2 * entries, :]
    uz = unit_ref[2 * entries : 3 * entries, :]
    basis = [basis_ref[k * entries : (k + 1) * entries, :] for k in range(NB)]
    slope = [slope_ref[k * entries : (k + 1) * entries, :] for k in range(NB)]
    angular = harmonics(ux, uy, uz)
    dr = grad_ref[3 * entries : 4 * entries, :]
    dy = []
    for m in range(9):
        part = None
        sl = None
        for k in range(NB):
            row = dmom[k : k + 1, m * atoms : (m + 1) * atoms]
            sl = slope[k] * row if sl is None else sl + slope[k] * row
            if m:
                part = basis[k] * row if part is None else part + basis[k] * row
        dr = dr + (sl if m == 0 else sl * angular[m])
        dy.append(part)
    wx = grad_ref[0:entries, :] + ROOT3 * dy[1]
    wx = wx + ROOT15 * (uy * dy[4] + uz * dy[7] + ux * dy[8])
    wy = grad_ref[entries : 2 * entries, :] + ROOT3 * dy[2]
    wy = wy + ROOT15 * (ux * dy[4] + uz * dy[5] - uy * dy[8])
    wz = grad_ref[2 * entries : 3 * entries, :] + ROOT3 * dy[3]
    wz = wz + ROOT15 * (uy * dy[5] + ux * dy[7]) + (3.0 * ROOT5) * uz * dy[6]
    rinv = rinv_ref[...]
    along = dr - rinv * (ux * wx + uy * wy + uz * wz)
    grads = [wx * rinv + along * ux, wy * rinv + along * uy, wz * rinv + along * uz]
    centre = []
    for i in range(3):
        centre.append(jnp.sum(grads[i], axis=0, keepdims=True))
        top16 = grads[i].astype(BF16).astype(F32)
        dv_ref[i * entries : (i + 1) * entries, :] = top16
        dv_ref[(3 + i) * entries : (4 + i) * entries, :] = grads[i] - top16
    shift = atoms.bit_length() - 1
    sc_ref[...] = jnp.zeros_like(sc_ref)

    def body(step, carry):
        first = step * GROUP
        row = jnp.concatenate([nbr_ref[pl.ds(first + jj, 1), :] for jj in range(GROUP)], axis=1)
        hot = onehot(row & (atoms - 1), atoms)
        block = row >> shift
        cols = [dv_ref[pl.ds(first + jj, 6, stride=entries), :] for jj in range(GROUP)]
        value = jnp.concatenate(cols, axis=1)
        value = jnp.concatenate([value, jnp.zeros_like(value[0:2])], axis=0)
        parts = [jnp.where(block == index, value, 0.0) for index in range(5)]
        sc_ref[...] += dot(jnp.concatenate(parts, axis=0).astype(BF16), hot, 1, 1)
        return carry

    lax.fori_loop(0, entries // GROUP, body, 0)
    zero = jnp.zeros((5, atoms), F32)
    own = jnp.concatenate(centre + [zero], axis=0)
    for index, ref in enumerate((f0_ref, f1_ref, f2_ref, f3_ref, f4_ref)):
        base = index * 8
        value = sc_ref[base : base + 3, :] + sc_ref[base + 3 : base + 6, :]
        value = jnp.concatenate([value, zero], axis=0)
        ref[...] = value - own if index == 0 else value


def scatter_lanes(values, row, size):
    return dot(values, onehot(row, size).astype(F32), 1, 1, HIGHEST)


def force_z_kernel(f0_ref, f1_ref, f2_ref, f3_ref, az_ref, fz_ref, out_ref, low_ref, high_ref):
    atoms = f0_ref.shape[1]
    add = scatter_lanes(az_ref[...], fz_ref[...], 4 * atoms)
    out_ref[:, 0:atoms] = f0_ref[...] + add[:, 0:atoms]
    out_ref[:, atoms : 2 * atoms] = f1_ref[...] + add[:, atoms : 2 * atoms]
    low_ref[...] = f2_ref[...] + add[:, 2 * atoms : 3 * atoms]
    high_ref[...] = f3_ref[...] + add[:, 3 * atoms :]


def force_y_kernel(acc_ref, a0_ref, a1_ref, fy_ref, own_ref, ghost_ref):
    size = acc_ref.shape[1]
    rows = acc_ref[...]
    rows = rows + scatter_lanes(a0_ref[...], fy_ref[0:1, :], size)
    rows = rows + scatter_lanes(a1_ref[...], fy_ref[1:2, :], size)
    own_ref[...] = rows[:, 0 : size // 2]
    ghost_ref[...] = rows[:, size // 2 :]


def force_x_kernel(own_ref, a0_ref, a1_ref, fx_ref, out_ref):
    size = own_ref.shape[1]
    from_low = a0_ref[...][:, size // 2 :]
    from_high = a1_ref[...][:, 0 : size // 2]
    rows = own_ref[...]
    rows = rows + scatter_lanes(from_low, fx_ref[0:1, :], size)
    rows = rows + scatter_lanes(from_high, fx_ref[1:2, :], size)
    out_ref[...] = -rows[0:3]


def call(kernel, outs, *args, scratch=(), vmem=8, scalars=()):
    specs = []
    for index in range(len(args)):
        space = pltpu.SMEM if index in scalars else pltpu.VMEM
        specs.append(pl.BlockSpec(memory_space=space))
    single = not isinstance(outs, (list, tuple))
    shapes = [outs] if single else list(outs)
    result = pl.pallas_call(
        kernel,
        out_shape=shapes,
        in_specs=specs,
        out_specs=[pl.BlockSpec(memory_space=pltpu.VMEM)] * len(shapes),
        scratch_shapes=list(scratch),
        compiler_params=pltpu.CompilerParams(vmem_limit_bytes=vmem * 1024 * 1024),
    )(*args)
    return result[0] if single else result


def moved(x, axis, step):
    count = lax.axis_size(axis)
    return lax.ppermute(x, axis, [(i, (i + step) % count) for i in range(count)])


def partner(x, axis):
    return lax.ppermute(x, axis, [(i, i ^ 1) for i in range(lax.axis_size(axis))])


def per_device(
    positions,
    occupancy,
    neighbours,
    keep,
    face_x,
    face_y,
    face_z,
    radial_one,
    mix_one,
    embed,
    radial_two,
    mix_two,
    read_one,
    read_hidden,
    read_out,
):
    atoms = positions.shape[-1]
    entries = neighbours.shape[0]
    channels = radial_one.shape[1]
    pos = positions.reshape(3, atoms)
    nbr = neighbours.reshape(entries, atoms)
    kept = keep.reshape(entries, atoms)
    occ = occupancy.reshape(1, atoms)
    fx = face_x.reshape(2, face_x.shape[-1])
    fy = face_y.reshape(2, face_y.shape[-1])
    fz = face_z.reshape(1, face_z.shape[-1])
    zshift = jnp.where(lax.axis_index("gz") == 0, LZ * SPACING, -LZ * SPACING)
    zshift = zshift.astype(F32).reshape(1)
    embed = embed.reshape(1, channels)
    read_one = read_one.reshape(1, channels)
    read_out = read_out.reshape(1, read_out.shape[0])

    def f32(*shape):
        return jax.ShapeDtypeStruct(shape, F32)

    def b16(*shape):
        return jax.ShapeDtypeStruct(shape, BF16)

    small = f32(8, atoms)
    sent = call(pos_x_kernel, small, pos, fx)
    lo, hi = moved(sent, "gx", 1), moved(sent, "gx", -1)
    p1, up, down = call(pos_y_kernel, [small] * 3, pos, lo, hi, fy)
    lo, hi = moved(up, "gy", 1), moved(down, "gy", -1)
    p2, p3, sent = call(pos_z_kernel, [small] * 3, pos, p1, lo, hi, fz)
    pz = partner(sent, "gz")

    square = b16(channels, atoms)
    unit, rinv, basis, slope, amp, h0, sent = call(
        layer_one_kernel,
        [
            f32(3 * entries, atoms),
            f32(entries, atoms),
            f32(NB * entries, atoms),
            f32(NB * entries, atoms),
            f32(channels, 9 * atoms),
            square,
            square,
        ],
        pos,
        p1,
        p2,
        p3,
        pz,
        zshift,
        nbr,
        kept,
        fx,
        radial_one,
        mix_one,
        embed,
        scratch=[pltpu.VMEM((NB, 9 * atoms), F32)],
        scalars=(5,),
    )
    lo, hi = moved(sent, "gx", 1), moved(sent, "gx", -1)
    h1, up, down = call(feat_y_kernel, [square] * 3, h0, lo, hi, fy)
    h2, h3 = moved(up, "gy", 1), moved(down, "gy", -1)
    sent = call(feat_z_kernel, square, h0, h1, h2, h3, fz)
    h4 = partner(sent, "gz")

    steps = entries // GROUP
    width = GROUP * atoms
    energies, gin, gz, grad = call(
        layer_two_kernel,
        [f32(1, atoms), b16(4 * atoms, channels), b16(atoms, channels), f32(4 * entries, atoms)],
        h0,
        h1,
        h2,
        h3,
        h4,
        nbr,
        occ,
        unit,
        rinv,
        basis,
        slope,
        radial_two,
        mix_two,
        read_one,
        read_hidden,
        read_out,
        scratch=[
            pltpu.VMEM((steps, 5 * atoms, width), BF16),
            pltpu.VMEM((steps, channels, width), F32),
            pltpu.VMEM((steps, channels, width), F32),
            pltpu.VMEM((steps, channels, width), F32),
            pltpu.VMEM((channels, width), F32),
            pltpu.VMEM((9, channels, atoms), F32),
            pltpu.VMEM((9, channels, atoms), F32),
            pltpu.VMEM((5 * atoms, channels), F32),
            pltpu.VMEM((channels, channels), BF16),
            pltpu.VMEM((8 * entries, atoms), F32),
            pltpu.VMEM((channels, 5 * atoms), BF16),
        ],
        vmem=40,
    )
    az = partner(gz, "gz")
    acc, low, high = call(
        fold_z_kernel,
        [f32(2 * atoms, channels), b16(atoms, channels), b16(atoms, channels)],
        gin,
        az,
        fz,
    )
    a0, a1 = moved(high, "gy", 1), moved(low, "gy", -1)
    half = atoms // 2
    own, low, high = call(
        fold_y_kernel,
        [f32(atoms, channels), b16(half, channels), b16(half, channels)],
        acc,
        a0,
        a1,
        fy,
    )
    a0, a1 = moved(high, "gx", 1), moved(low, "gx", -1)
    f0, f1, f2, f3, f4 = call(
        layer_one_reverse_kernel,
        [small] * 5,
        own,
        a0,
        a1,
        fx,
        amp,
        nbr,
        unit,
        rinv,
        basis,
        slope,
        grad,
        radial_one,
        mix_one,
        scratch=[pltpu.VMEM((6 * entries, atoms), F32), pltpu.VMEM((40, atoms), F32)],
    )
    az = partner(f4, "gz")
    acc, low, high = call(
        force_z_kernel, [f32(8, 2 * atoms), small, small], f0, f1, f2, f3, az, fz
    )
    a0, a1 = moved(high, "gy", 1), moved(low, "gy", -1)
    own, ghost = call(force_y_kernel, [small, small], acc, a0, a1, fy)
    a0, a1 = moved(ghost, "gx", 1), moved(ghost, "gx", -1)
    forces = call(force_x_kernel, f32(3, atoms), own, a0, a1, fx)
    return (energies.reshape(occupancy.shape), forces.reshape(positions.shape))


def solution(mesh):
    return jax.shard_map(
        per_device,
        mesh=mesh,
        in_specs=(
            P(None, "gx", "gy", "gz", None),
            P("gx", "gy", "gz", None),
            P(None, "gx", "gy", "gz", None),
            P(None, "gx", "gy", "gz", None),
            P("gx", "gy", "gz", None, None),
            P("gx", "gy", "gz", None, None),
            P("gx", "gy", "gz", None),
            P(),
            P(),
            P(),
            P(),
            P(),
            P(),
            P(),
            P(),
        ),
        out_specs=(P("gx", "gy", "gz", None), P(None, "gx", "gy", "gz", None)),
        check_vma=False,
    )
```

```python
import functools
import math

import jax
import jax.numpy as jnp
from jax import lax
from jax.experimental import pallas as pl
from jax.experimental.pallas import tpu as pltpu
from jax.sharding import PartitionSpec as P

NB = 8
LX = 4
LY = 4
LZ = 8

SPACING = 1.8
CUTOFF = 5.0
SPREAD = 0.4
HIGHEST = lax.Precision.HIGHEST
F32 = jnp.float32
BF16 = jnp.bfloat16

ROOT3 = 3.0**0.5
ROOT5 = 5.0**0.5
ROOT15 = 15.0**0.5
GROUP = 4


def dot(a, b, ca=1, cb=0, precision=None):
    return lax.dot_general(
        a, b, (((ca,), (cb,)), ((), ())), precision=precision, preferred_element_type=F32
    )


def split2(x):
    hi = x.astype(BF16)
    lo = (x - hi.astype(F32)).astype(BF16)
    return hi, lo


def dot_split(a, b, ca=1, cb=0):
    hi, lo = split2(b)
    return dot(a, hi, ca, cb) + dot(a, lo, ca, cb)


def onehot(row, size):
    count = row.shape[-1]
    ids = lax.broadcasted_iota(jnp.int32, (size, count), 0)
    return jnp.where(ids == row, 1.0, 0.0).astype(BF16)


def lane_pick(blocks, rows):
    width = blocks[0].shape[-1]
    shift = width.bit_length() - 1
    lane = rows & (width - 1)
    block = rows >> shift
    out = jnp.take_along_axis(blocks[0], lane, axis=1)
    for index in range(1, len(blocks)):
        part = jnp.take_along_axis(blocks[index], lane, axis=1)
        out = jnp.where(block == index, part, out)
    return out


def spread_rows(row, count):
    return jnp.broadcast_to(row, (count, row.shape[-1]))


def by_side(side_ref, axis, if_odd, if_even):
    odd = side_ref[axis : axis + 1, 0 : if_odd.shape[1]] == 1
    return jnp.where(odd, if_odd, if_even)


def near_far(side_ref, axis, face_ref):
    low, high = face_ref[0:1, :], face_ref[1:2, :]
    return by_side(side_ref, axis, low, high), by_side(side_ref, axis, high, low)


def face_row(side_ref, fx_ref):
    return jnp.concatenate(near_far(side_ref, 0, fx_ref), axis=1)


def half_turn(x):
    half = x.shape[1] // 2
    return jnp.concatenate([x[:, half:], x[:, :half]], axis=1)


def low_lanes(shape):
    return lax.broadcasted_iota(jnp.int32, shape, 1) < shape[1] // 2


def shift_rows(shape, axis, amount):
    ids = lax.broadcasted_iota(jnp.int32, shape, 0)
    return jnp.where(ids == axis, amount, 0.0)


def pos_x_kernel(pos_ref, fx_ref, side_ref, coords_ref, send_ref):
    ids = lax.broadcasted_iota(jnp.int32, side_ref.shape, 0)
    first, second = lax.axis_index("gx") % 2, lax.axis_index("gy") % 2
    value = jnp.where(ids == 0, first, jnp.where(ids == 1, second, lax.axis_index("gz")))
    side_ref[...] = value
    rows = [pos_ref[i] for i in range(3)]
    coords = jnp.concatenate(rows + [jnp.zeros_like(rows[0])] * 5, axis=0)
    coords_ref[...] = coords
    send_ref[...] = lane_pick([coords], spread_rows(face_row(side_ref, fx_ref), 8))


def pos_y_kernel(side_ref, pos_ref, near_ref, far_ref, fy_ref, p1_ref, to_near_ref, to_far_ref):
    coords = pos_ref[...]
    shape = coords.shape
    first = low_lanes(shape)
    both = jnp.where(first, near_ref[...], far_ref[...])
    both = by_side(side_ref, 0, both, half_turn(both))
    step = shift_rows(shape, 0, LX * SPACING)
    ghost = jnp.where(first, both - step, both + step)
    p1_ref[...] = ghost
    near, far = near_far(side_ref, 1, fy_ref)
    to_near_ref[...] = lane_pick([coords, ghost], spread_rows(near, 8))
    to_far_ref[...] = lane_pick([coords, ghost], spread_rows(far, 8))


def pos_z_kernel(side_ref, pos_ref, p1_ref, near_ref, far_ref, fz_ref, p2_ref, p3_ref, out_ref):
    coords = pos_ref[...]
    shape = coords.shape
    near, far = near_ref[...], far_ref[...]
    low = by_side(side_ref, 1, near, far) - shift_rows(shape, 1, LY * SPACING)
    high = by_side(side_ref, 1, far, near) + shift_rows(shape, 1, LY * SPACING)
    p2_ref[...] = low
    p3_ref[...] = high
    out_ref[...] = lane_pick([coords, p1_ref[...], low, high], spread_rows(fz_ref[...], 8))


def layer_one_kernel(
    side_ref,
    pos_ref,
    p1_ref,
    p2_ref,
    p3_ref,
    pz_ref,
    nbr_ref,
    keep_ref,
    fx_ref,
    radial_ref,
    mix_ref,
    embed_ref,
    unit_ref,
    rinv_ref,
    basis_ref,
    slope_ref,
    amp_ref,
    h0_ref,
    to_near_ref,
    to_far_ref,
    mom_ref,
):
    entries, atoms = nbr_ref.shape
    nbr = nbr_ref[...]
    lane = nbr & (atoms - 1)
    block = nbr >> (atoms.bit_length() - 1)
    rise = jnp.where(side_ref[2:3, :] == 0, LZ * SPACING, -LZ * SPACING)
    last = pz_ref[...] + shift_rows(pz_ref.shape, 2, rise)
    tables = [pos_ref[...], p1_ref[...], p2_ref[...], p3_ref[...], last]
    vec = []
    for axis in range(3):
        got = None
        for index, table in enumerate(tables):
            spread = spread_rows(table[axis : axis + 1, :], entries)
            part = jnp.take_along_axis(spread, lane, axis=1)
            got = part if index == 0 else jnp.where(block == index, part, got)
        vec.append(got - pos_ref[axis : axis + 1, :])
    r_sq = vec[0] * vec[0] + vec[1] * vec[1] + vec[2] * vec[2]
    dist = jnp.sqrt(r_sq)
    rinv = 1.0 / dist
    ux, uy, uz = (v * rinv for v in vec)
    rinv_ref[...] = rinv
    unit_ref[0:entries, :] = ux
    unit_ref[entries : 2 * entries, :] = uy
    unit_ref[2 * entries : 3 * entries, :] = uz
    scaled = jnp.minimum(dist * (1.0 / CUTOFF), 1.0)
    phase = scaled * math.pi
    sine = jnp.sin(phase)
    cosine = jnp.cos(phase)
    inner = 1.0 - scaled * scaled
    weight = keep_ref[...].astype(F32) * (2.0 / CUTOFF) ** 0.5
    env = weight * inner * inner * rinv
    env_slope = -env * rinv - weight * rinv * (4.0 / CUTOFF) * scaled * inner
    twice = 2.0 * cosine
    s_prev, s_now = jnp.zeros_like(sine), sine
    c_prev, c_now = jnp.ones_like(cosine), cosine
    basis = []
    for k in range(NB):
        bk = s_now * env
        basis.append(bk)
        basis_ref[k * entries : (k + 1) * entries, :] = bk
        slope_ref[k * entries : (k + 1) * entries, :] = (
            c_now * env * ((k + 1) * math.pi / CUTOFF) + s_now * env_slope
        )
        s_prev, s_now = s_now, twice * s_now - s_prev
        c_prev, c_now = c_now, twice * c_now - c_prev
    angular = harmonics(ux, uy, uz)
    for m in range(9):
        for k in range(NB):
            prod = basis[k] if m == 0 else basis[k] * angular[m]
            mom_ref[k : k + 1, m * atoms : (m + 1) * atoms] = jnp.sum(prod, axis=0, keepdims=True)
    amp = SPREAD * dot(radial_ref[...], mom_ref[...], 0, 0, HIGHEST)
    amp_ref[...] = amp
    inv = invariants([amp[:, m * atoms : (m + 1) * atoms] for m in range(9)])
    h1 = dot(mix_ref[...], inv, 0, 0)
    h1 = h1 + dot(embed_ref[...], jnp.ones((1, atoms), F32), 0, 0, HIGHEST)
    h1b = h1.astype(BF16)
    h0_ref[...] = h1b
    both = dot(h1b, onehot(face_row(side_ref, fx_ref), atoms))
    to_near_ref[...], to_far_ref[...] = pack_halves(both)


def harmonics(ux, uy, uz):
    return [
        None,
        ROOT3 * ux,
        ROOT3 * uy,
        ROOT3 * uz,
        ROOT15 * ux * uy,
        ROOT15 * uy * uz,
        0.5 * ROOT5 * (3.0 * uz * uz - 1.0),
        ROOT15 * ux * uz,
        0.5 * ROOT15 * (ux * ux - uy * uy),
    ]


def invariants(amp):
    first = amp[1] * amp[1] + amp[2] * amp[2] + amp[3] * amp[3]
    second = amp[4] * amp[4] + amp[5] * amp[5] + amp[6] * amp[6]
    second = second + amp[7] * amp[7] + amp[8] * amp[8]
    return jnp.concatenate([amp[0], first, second], axis=0).astype(BF16)


def pack_halves(both):
    rows, _ = both.shape
    top, low = both[0 : rows // 2], both[rows // 2 :]
    first = low_lanes(top.shape)
    near = jnp.where(first, top, half_turn(low))
    far = jnp.where(first, half_turn(top), low)
    return near.astype(BF16), far.astype(BF16)


def unpack_halves(low, high):
    first = low_lanes(low.shape)
    top = jnp.where(first, low, half_turn(high))
    bottom = jnp.where(first, half_turn(low), high)
    return jnp.concatenate([top, bottom], axis=0)


def feat_y_kernel(side_ref, h0_ref, near_ref, far_ref, fy_ref, h1_ref, to_near_ref, to_far_ref):
    near, far = near_ref[...].astype(F32), far_ref[...].astype(F32)
    low, high = by_side(side_ref, 0, near, far), by_side(side_ref, 0, far, near)
    ghost = unpack_halves(low, high).astype(BF16)
    h1_ref[...] = ghost
    table = jnp.concatenate([h0_ref[...], ghost], axis=1)
    size = table.shape[1]
    near, far = near_far(side_ref, 1, fy_ref)
    to_near_ref[...] = dot(table, onehot(near, size)).astype(BF16)
    to_far_ref[...] = dot(table, onehot(far, size)).astype(BF16)


def sides(side_ref, axis, near_ref, far_ref):
    near, far = near_ref[...].astype(F32), far_ref[...].astype(F32)
    low, high = by_side(side_ref, axis, near, far), by_side(side_ref, axis, far, near)
    return low.astype(BF16), high.astype(BF16)


def feat_z_kernel(side_ref, h0_ref, h1_ref, near_ref, far_ref, fz_ref, out_ref, h2_ref, h3_ref):
    low, high = sides(side_ref, 1, near_ref, far_ref)
    h2_ref[...] = low
    h3_ref[...] = high
    table = jnp.concatenate([h0_ref[...], h1_ref[...], low, high], axis=1)
    out_ref[...] = dot(table, onehot(fz_ref[...], table.shape[1])).astype(BF16)


def entry_rows(ref, first):
    return jnp.concatenate([ref[pl.ds(first + jj, 1), :] for jj in range(GROUP)], axis=1)


def hot_kernel(nbr_ref, hot_ref, lane_ref):
    atoms = nbr_ref.shape[1]

    def body(step, carry):
        row = entry_rows(nbr_ref, step * GROUP)
        hot_ref[step] = onehot(row, hot_ref.shape[1])
        lane_ref[step] = onehot(row & (atoms - 1), atoms)
        return carry

    lax.fori_loop(0, hot_ref.shape[0], body, 0)


def stack3(hi, lo):
    return jnp.concatenate([hi, lo, hi], axis=0).astype(BF16)


def radial_kernel(basis_ref, slope_ref, unit_ref, radial_ref, rad_ref, slo_ref, y_ref, rts_ref):
    entries = basis_ref.shape[0] // NB
    channels = radial_ref.shape[1]
    rt = radial_ref[...]
    hi = rt.astype(BF16).astype(F32)
    lo = rt - hi
    pad = jnp.zeros((channels - 3 * NB, channels), F32)
    rts_ref[...] = jnp.transpose(jnp.concatenate([hi, hi, lo, pad], axis=0)).astype(BF16)
    ux = unit_ref[0:entries, :]
    uy = unit_ref[entries : 2 * entries, :]
    uz = unit_ref[2 * entries : 3 * entries, :]
    for m, val in enumerate(harmonics(ux, uy, uz)):
        if m:
            y_ref[(m - 1) * entries : m * entries, :] = val

    def radial_cols(ref, first):
        cols = [ref[pl.ds(first + jj, NB, stride=entries), :] for jj in range(GROUP)]
        value = jnp.concatenate(cols, axis=1)
        top = value.astype(BF16).astype(F32)
        return stack3(top, value - top)

    rts = rts_ref[:, 0 : 3 * NB]
    for step in range(rad_ref.shape[0]):
        rad_ref[step] = dot(rts, radial_cols(basis_ref, step * GROUP))
        slo_ref[step] = dot(rts, radial_cols(slope_ref, step * GROUP))


def gather_first_kernel(h0_ref, h1_ref, hot_ref, hg_ref, table_ref):
    atoms = h0_ref.shape[1]
    table_ref[:, 0:atoms] = h0_ref[...]
    table_ref[:, atoms:] = h1_ref[...]

    for step in range(hot_ref.shape[0]):
        hg_ref[step] = dot(table_ref[...], hot_ref[step, 0 : 2 * atoms, :])


def gather_more_kernel(h2_ref, h3_ref, hot_ref, old_ref, hg_ref, table_ref):
    atoms = h2_ref.shape[1]
    table_ref[:, 0:atoms] = h2_ref[...]
    table_ref[:, atoms:] = h3_ref[...]

    for step in range(hot_ref.shape[0]):
        more = dot(table_ref[...], hot_ref[step, 2 * atoms : 4 * atoms, :])
        hg_ref[step] = old_ref[step] + more


def layer_two_kernel(
    h0_ref,
    h4_ref,
    hot_ref,
    old_ref,
    rad_ref,
    y_ref,
    occ_ref,
    mix_ref,
    rone_ref,
    rhid_ref,
    rout_ref,
    hg_ref,
    en_ref,
    raw_ref,
    extra_ref,
    rq_ref,
    gy_ref,
    gz_ref,
    acc_ref,
    dh_ref,
):
    channels, atoms = h0_ref.shape
    steps = hot_ref.shape[0]
    entries = steps * GROUP
    blocks = channels // 8
    acc_ref[...] = jnp.zeros_like(acc_ref)

    def prepare(step):
        hg_ref[step] = old_ref[step] + dot(h4_ref[...], hot_ref[step, 4 * atoms :, :])

    def accumulate(step):
        first = step * GROUP
        for pair in range(blocks // 2):
            spans = [slice(cb * 8, cb * 8 + 8) for cb in (2 * pair, 2 * pair + 1)]
            msgs = []
            for rows in spans:
                line = []
                for jj in range(GROUP):
                    cols = slice(jj * atoms, (jj + 1) * atoms)
                    line.append(hg_ref[step, rows, cols] * rad_ref[step, rows, cols])
                msgs.append(line)
            for m in range(9):
                if m:
                    at = (m - 1) * entries + first
                    yvs = [y_ref[pl.ds(at + jj, 1), :] for jj in range(GROUP)]
                for rows, line in zip(spans, msgs):
                    if m:
                        terms = [line[jj] * yvs[jj] for jj in range(GROUP)]
                    else:
                        terms = line
                    while len(terms) > 1:
                        terms = [a + b for a, b in zip(terms[::2], terms[1::2])]
                    acc_ref[m, rows, :] += terms[0]

    prepare(0)

    def forward_body(step, carry):
        accumulate(step - 1)
        prepare(step)
        return carry

    lax.fori_loop(1, steps, forward_body, 0)
    accumulate(steps - 1)

    occ = occ_ref[...].astype(F32)
    ones = jnp.ones((1, atoms), F32)
    amp = [SPREAD * acc_ref[m] for m in range(9)]
    own = h0_ref[...].astype(F32)
    h2 = dot(mix_ref[...], invariants(amp), 0, 0) + own
    pre = dot(rhid_ref[...], h2, 1, 0, HIGHEST)
    sig = 1.0 / (1.0 + jnp.exp(-pre))
    rout = dot(rout_ref[...], ones, 0, 0, HIGHEST)
    rone = dot(rone_ref[...], ones, 0, 0, HIGHEST)
    energy = jnp.sum(own * rone, axis=0, keepdims=True)
    energy = energy + jnp.sum(rout * pre * sig, axis=0, keepdims=True)
    en_ref[...] = occ * energy
    dpre = occ * rout * sig * (1.0 + pre * (1.0 - sig))
    dh2 = dot(rhid_ref[...], dpre, 0, 0, HIGHEST)
    dinv = dot_split(mix_ref[...], dh2)
    low = dinv[channels : 2 * channels]
    top = dinv[2 * channels :]
    extra_ref[...] = dh2 + occ * rone
    twice = 2.0 * SPREAD
    raw_ref[0] = SPREAD * dinv[0:channels]
    for m in range(1, 9):
        raw_ref[m] = (twice * amp[m]) * (low if m < 4 else top)
    dh_ref[...] = jnp.zeros_like(dh_ref)

    def reverse(step):
        first = step * GROUP
        for pair in range(blocks // 2):
            spans = [slice(cb * 8, cb * 8 + 8) for cb in (2 * pair, 2 * pair + 1)]
            ds = [[raw_ref[m, rows, :] for m in range(9)] for rows in spans]
            for jj in range(GROUP):
                cols = slice(jj * atoms, (jj + 1) * atoms)
                yvs = [y_ref[pl.ds((m - 1) * entries + first + jj, 1), :] for m in range(1, 9)]
                parts = []
                for rows, d in zip(spans, ds):
                    terms = [d[0]] + [yv * dm for yv, dm in zip(yvs, d[1:])]
                    q = terms[0] + terms[1]
                    for a, b in ((2, 3), (4, 5), (6, 7)):
                        q = q + (terms[a] + terms[b])
                    parts.append(rad_ref[step, rows, cols] * (q + terms[8]))
                value = jnp.concatenate(parts, axis=0).astype(BF16)
                rq_ref[step, pair * 16 : pair * 16 + 16, cols] = value

    def send(step):
        dh_ref[...] += dot(hot_ref[step, 2 * atoms :, :], rq_ref[step], 1, 1)

    reverse(0)

    def reverse_body(step, carry):
        send(step - 1)
        reverse(step)
        return carry

    lax.fori_loop(1, steps, reverse_body, 0)
    send(steps - 1)
    gy_ref[...] = dh_ref[0 : 2 * atoms, :].astype(BF16)
    gz_ref[...] = dh_ref[2 * atoms :, :].astype(BF16)


def directions(d, unit):
    vx, vy, vz = unit
    cx = vy * d[4] + vz * d[7] + vx * d[8]
    cy = vx * d[4] + vz * d[5] - vy * d[8]
    cz = vy * d[5] + vx * d[7] + vz * d[6]
    return d[1] + cx, d[2] + cy, d[3] + cz, (cx, cy, cz)


def scatter_kernel(first, hot_ref, rq_ref, out_ref):
    size = out_ref.shape[0]
    total = None
    for step in range(hot_ref.shape[0]):
        part = dot(hot_ref[step, first : first + size, :], rq_ref[step], 1, 1)
        total = part if total is None else total + part
    out_ref[...] = total


def edge_kernel(start, hg_ref, rad_ref, slo_ref, d_ref, unit_ref, grad_ref, dd_ref):
    channels, atoms = d_ref.shape[1:]
    entries = hg_ref.shape[0] * GROUP
    count = grad_ref.shape[0] // (4 * GROUP)
    for m in range(9):
        if m == 0:
            dd_ref[m] = d_ref[0] - (0.5 * ROOT5) * d_ref[6]
        elif m < 4:
            dd_ref[m] = ROOT3 * d_ref[m]
        else:
            dd_ref[m] = (1.5 * ROOT5 if m == 6 else 0.5 * ROOT15) * d_ref[m]

    def body(step, carry):
        first = step * GROUP
        units = []
        for jj in range(GROUP):
            units.append([unit_ref[pl.ds(i * entries + first + jj, 1), :] for i in range(3)])
        sums = [[None] * 4 for _ in range(GROUP)]
        for cb in range(channels // 8):
            rows = slice(cb * 8, cb * 8 + 8)
            d = [dd_ref[m, rows, :] for m in range(9)]
            for jj in range(GROUP):
                cols = slice(jj * atoms, (jj + 1) * atoms)
                hg = hg_ref[step, rows, cols]
                ex, ey, ez, (cx, cy, cz) = directions(d, units[jj])
                vx, vy, vz = units[jj]
                q = d[0] + vx * ex + vy * ey + vz * ez
                msg = hg * rad_ref[step, rows, cols]
                parts = [
                    msg * (ex + cx),
                    msg * (ey + cy),
                    msg * (ez + cz),
                    hg * q * slo_ref[step, rows, cols],
                ]
                for i in range(4):
                    prior = sums[jj][i]
                    sums[jj][i] = parts[i] if prior is None else prior + parts[i]
        for jj in range(GROUP):
            for i in range(4):
                row = pl.ds(i * count * GROUP + first - start * GROUP + jj, 1)
                grad_ref[row, :] = jnp.sum(sums[jj][i], axis=0, keepdims=True)
        return carry

    lax.fori_loop(start, start + count, body, 0)


def fold_z_kernel(side_ref, gy_ref, az_ref, fz_ref, acc_ref, to_near_ref, to_far_ref):
    size = gy_ref.shape[0]
    quarter = size // 2
    add = dot(onehot(fz_ref[...], 2 * size), az_ref[...])
    acc_ref[...] = add[0:size]
    rows = gy_ref[...].astype(F32) + add[size:]
    low, high = rows[0:quarter], rows[quarter:]
    to_near_ref[...] = by_side(side_ref, 1, low, high).astype(BF16)
    to_far_ref[...] = by_side(side_ref, 1, high, low).astype(BF16)


def fold_y_kernel(
    side_ref, acc_ref, gx_ref, extra_ref, near_ref, far_ref, fy_ref, own_ref, to_near_ref, to_far_ref
):
    size = acc_ref.shape[0]
    half = size // 2
    quarter = half // 2
    near, far = near_far(side_ref, 1, fy_ref)
    rows = acc_ref[...] + dot(onehot(near, size), near_ref[...])
    rows = rows + dot(onehot(far, size), far_ref[...])
    own = gx_ref[0:half, :] + jnp.transpose(extra_ref[...])
    own_ref[...] = rows[0:half] + own.astype(BF16).astype(F32)
    ghost = rows[half:] + gx_ref[half:, :].astype(BF16).astype(F32)
    low, high = ghost[0:quarter], ghost[quarter:]
    to_near_ref[...] = by_side(side_ref, 0, low, high).astype(BF16)
    to_far_ref[...] = by_side(side_ref, 0, high, low).astype(BF16)


def layer_one_reverse_kernel(
    side_ref,
    own_ref,
    near_ref,
    far_ref,
    fx_ref,
    amp_ref,
    nbr_ref,
    unit_ref,
    rinv_ref,
    basis_ref,
    slope_ref,
    ga_ref,
    gb_ref,
    gc_ref,
    lane_ref,
    radial_ref,
    mix_ref,
    f0_ref,
    f1_ref,
    f2_ref,
    f3_ref,
    f4_ref,
    dv_ref,
    sc_ref,
):
    entries, atoms = nbr_ref.shape
    channels = own_ref.shape[1]
    rows = own_ref[...]
    near, far = near_far(side_ref, 0, fx_ref)
    rows = rows + dot(onehot(near, atoms), near_ref[...])
    rows = rows + dot(onehot(far, atoms), far_ref[...])
    cot = jnp.transpose(rows)
    dinv = dot_split(mix_ref[...], cot)
    low = dinv[channels : 2 * channels]
    top = dinv[2 * channels :]
    pieces = [dinv[0:channels]]
    for m in range(1, 9):
        amp = amp_ref[:, m * atoms : (m + 1) * atoms]
        pieces.append(2.0 * amp * (low if m < 4 else top))
    dmom = SPREAD * dot(radial_ref[...], jnp.concatenate(pieces, axis=1), 1, 0, HIGHEST)
    ux = unit_ref[0:entries, :]
    uy = unit_ref[entries : 2 * entries, :]
    uz = unit_ref[2 * entries : 3 * entries, :]
    basis = [basis_ref[k * entries : (k + 1) * entries, :] for k in range(NB)]
    slope = [slope_ref[k * entries : (k + 1) * entries, :] for k in range(NB)]
    angular = harmonics(ux, uy, uz)
    edge = []
    for i in range(4):
        rows = []
        for ref in (ga_ref, gb_ref, gc_ref):
            count = ref.shape[0] // 4
            rows.append(ref[i * count : (i + 1) * count, :])
        edge.append(jnp.concatenate(rows, axis=0))
    dr = edge[3]
    dy = []
    for m in range(9):
        part = None
        sl = None
        for k in range(NB):
            row = dmom[k : k + 1, m * atoms : (m + 1) * atoms]
            sl = slope[k] * row if sl is None else sl + slope[k] * row
            if m:
                part = basis[k] * row if part is None else part + basis[k] * row
        dr = dr + (sl if m == 0 else sl * angular[m])
        dy.append(part)
    wx = edge[0] + ROOT3 * dy[1]
    wx = wx + ROOT15 * (uy * dy[4] + uz * dy[7] + ux * dy[8])
    wy = edge[1] + ROOT3 * dy[2]
    wy = wy + ROOT15 * (ux * dy[4] + uz * dy[5] - uy * dy[8])
    wz = edge[2] + ROOT3 * dy[3]
    wz = wz + ROOT15 * (uy * dy[5] + ux * dy[7]) + (3.0 * ROOT5) * uz * dy[6]
    rinv = rinv_ref[...]
    along = dr - rinv * (ux * wx + uy * wy + uz * wz)
    grads = [wx * rinv + along * ux, wy * rinv + along * uy, wz * rinv + along * uz]
    centre = []
    for i in range(3):
        centre.append(jnp.sum(grads[i], axis=0, keepdims=True))
        top16 = grads[i].astype(BF16).astype(F32)
        dv_ref[i * entries : (i + 1) * entries, :] = top16
        dv_ref[(3 + i) * entries : (4 + i) * entries, :] = grads[i] - top16
    shift = atoms.bit_length() - 1
    total = None
    for step in range(entries // GROUP):
        first = step * GROUP
        block = entry_rows(nbr_ref, first) >> shift
        cols = [dv_ref[pl.ds(first + jj, 6, stride=entries), :] for jj in range(GROUP)]
        value = jnp.concatenate(cols, axis=1)
        value = jnp.concatenate([value, jnp.zeros_like(value[0:2])], axis=0)
        parts = [jnp.where(block == index, value, 0.0) for index in range(5)]
        part = dot(jnp.concatenate(parts, axis=0).astype(BF16), lane_ref[step], 1, 1)
        total = part if total is None else total + part
    sc_ref[...] = total
    zero = jnp.zeros((5, atoms), F32)
    own = jnp.concatenate(centre + [zero], axis=0)
    for index, ref in enumerate((f0_ref, f1_ref, f2_ref, f3_ref, f4_ref)):
        base = index * 8
        value = sc_ref[base : base + 3, :] + sc_ref[base + 3 : base + 6, :]
        value = jnp.concatenate([value, zero], axis=0)
        ref[...] = value - own if index == 0 else value


def scatter_lanes(values, row, size):
    return dot(values, onehot(row, size).astype(F32), 1, 1, HIGHEST)


def force_z_kernel(
    side_ref, f0_ref, f1_ref, f2_ref, f3_ref, az_ref, fz_ref, out_ref, to_near_ref, to_far_ref
):
    atoms = f0_ref.shape[1]
    add = scatter_lanes(az_ref[...], fz_ref[...], 4 * atoms)
    out_ref[:, 0:atoms] = f0_ref[...] + add[:, 0:atoms]
    out_ref[:, atoms : 2 * atoms] = f1_ref[...] + add[:, atoms : 2 * atoms]
    low = f2_ref[...] + add[:, 2 * atoms : 3 * atoms]
    high = f3_ref[...] + add[:, 3 * atoms :]
    to_near_ref[...] = by_side(side_ref, 1, low, high)
    to_far_ref[...] = by_side(side_ref, 1, high, low)


def force_y_kernel(side_ref, acc_ref, near_ref, far_ref, fy_ref, own_ref, ghost_ref):
    size = acc_ref.shape[1]
    rows = acc_ref[...]
    near, far = near_far(side_ref, 1, fy_ref)
    rows = rows + scatter_lanes(near_ref[...], near, size)
    rows = rows + scatter_lanes(far_ref[...], far, size)
    own_ref[...] = rows[:, 0 : size // 2]
    ghost = rows[:, size // 2 :]
    ghost_ref[...] = by_side(side_ref, 0, ghost, half_turn(ghost))


def force_x_kernel(side_ref, own_ref, near_ref, far_ref, fx_ref, out_ref):
    size = own_ref.shape[1]
    both = jnp.where(low_lanes(own_ref.shape), near_ref[...], far_ref[...])
    rows = own_ref[...] + scatter_lanes(both, face_row(side_ref, fx_ref), size)
    for i in range(3):
        out_ref[i] = -rows[i : i + 1]


def call(kernel, outs, *args, scratch=(), vmem=8, aliases={}, cost=1):
    specs = []
    for arg in args:
        specs.append(pl.BlockSpec(memory_space=pltpu.VMEM))
    single = not isinstance(outs, (list, tuple))
    shapes = [outs] if single else list(outs)
    result = pl.pallas_call(
        kernel,
        out_shape=shapes,
        in_specs=specs,
        out_specs=[pl.BlockSpec(memory_space=pltpu.VMEM)] * len(shapes),
        scratch_shapes=list(scratch),
        input_output_aliases=aliases,
        cost_estimate=pl.CostEstimate(
            flops=cost * 10**9, bytes_accessed=cost * 10**6, transcendentals=0
        ),
        compiler_params=pltpu.CompilerParams(vmem_limit_bytes=vmem * 1024 * 1024),
    )(*args)
    return result[0] if single else result


def pair_swap(x, axis, far):
    count = lax.axis_size(axis)
    assert count % 2 == 0
    pairs = []
    for i in range(count):
        up = (i % 2 == 0) != far
        pairs.append((i, (i + (1 if up else -1)) % count))
    return lax.ppermute(x, axis, pairs)


def partner(x):
    axis = "gz"
    return lax.ppermute(x, axis, [(i, i ^ 1) for i in range(lax.axis_size(axis))])


def swap_both(near, far, axis):
    from_far = pair_swap(far, axis, True)
    from_near = pair_swap(near, axis, False)
    return from_near, from_far


def per_device(
    positions,
    occupancy,
    neighbours,
    keep,
    face_x,
    face_y,
    face_z,
    radial_one,
    mix_one,
    embed,
    radial_two,
    mix_two,
    read_one,
    read_hidden,
    read_out,
):
    atoms = positions.shape[-1]
    entries = neighbours.shape[0]
    channels = radial_one.shape[1]
    pos = positions.reshape(3, 1, atoms)
    nbr = neighbours.reshape(entries, atoms)
    kept = keep.reshape(entries, atoms)
    occ = occupancy.reshape(1, atoms)
    fx = face_x.reshape(2, face_x.shape[-1])
    fy = face_y.reshape(2, face_y.shape[-1])
    fz = face_z.reshape(1, face_z.shape[-1])
    embed = embed.reshape(1, channels)
    read_one = read_one.reshape(1, channels)
    read_out = read_out.reshape(1, read_out.shape[0])
    read_hidden = read_hidden.T

    def f32(*shape):
        return jax.ShapeDtypeStruct(shape, F32)

    def b16(*shape):
        return jax.ShapeDtypeStruct(shape, BF16)

    small = f32(8, atoms)
    side = jax.ShapeDtypeStruct((8, atoms), jnp.int32)
    side, pos, sent = call(pos_x_kernel, [side, small, small], pos, fx)
    steps = entries // GROUP
    width = GROUP * atoms
    hot, lanes = call(
        hot_kernel, [b16(steps, 5 * atoms, width), b16(steps, atoms, width)], nbr
    )
    near, far = swap_both(sent, sent, "gx")
    p1, near, far = call(pos_y_kernel, [small] * 3, side, pos, near, far, fy)
    near, far = swap_both(near, far, "gy")
    p2, p3, sent = call(pos_z_kernel, [small] * 3, side, pos, p1, near, far, fz)
    pz = partner(sent)

    half = atoms // 2
    square = b16(channels, atoms)
    unit, rinv, basis, slope, amp, h0, near, far = call(
        layer_one_kernel,
        [
            f32(3 * entries, atoms),
            f32(entries, atoms),
            f32(NB * entries, atoms),
            f32(NB * entries, atoms),
            f32(channels, 9 * atoms),
            square,
            b16(channels // 2, atoms),
            b16(channels // 2, atoms),
        ],
        side,
        pos,
        p1,
        p2,
        p3,
        pz,
        nbr,
        kept,
        fx,
        radial_one,
        mix_one,
        embed,
        scratch=[pltpu.VMEM((NB, 9 * atoms), F32)],
    )
    big = f32(steps, channels, width)
    rad, slo, ylm = call(
        radial_kernel,
        [big, big, f32(8 * entries, atoms)],
        basis,
        slope,
        unit,
        radial_two,
        scratch=[pltpu.VMEM((channels, channels), BF16)],
    )
    near, far = swap_both(near, far, "gx")
    h1, near, far = call(feat_y_kernel, [square] * 3, side, h0, near, far, fy)
    table = [pltpu.VMEM((channels, 2 * atoms), BF16)]
    hg = call(gather_first_kernel, big, h0, h1, hot, scratch=table)
    near, far = swap_both(near, far, "gy")
    sent, h2, h3 = call(feat_z_kernel, [square] * 3, side, h0, h1, near, far, fz)
    hg = call(gather_more_kernel, big, h2, h3, hot, hg, scratch=table, aliases={3: 0})
    h4 = partner(sent)

    hg, energies, dmat, extra, rq, gy, gz = call(
        layer_two_kernel,
        [
            big,
            f32(1, atoms),
            f32(9, channels, atoms),
            f32(channels, atoms),
            b16(steps, channels, width),
            b16(2 * atoms, channels),
            b16(atoms, channels),
        ],
        h0,
        h4,
        hot,
        hg,
        rad,
        ylm,
        occ,
        mix_two,
        read_one,
        read_hidden,
        read_out,
        scratch=[pltpu.VMEM((9, channels, atoms), F32), pltpu.VMEM((3 * atoms, channels), F32)],
        aliases={3: 0},
    )
    az = partner(gz)
    rows = f32(2 * atoms, channels)

    def edges(start, count):
        out = f32(4 * count * GROUP, atoms)
        scaled = [pltpu.VMEM((9, channels, atoms), F32)]
        kernel = functools.partial(edge_kernel, start)
        return call(kernel, out, hg, rad, slo, dmat, unit, scratch=scaled)

    cuts = [0, 3 * (steps // 7), 4 * (steps // 7), steps]
    ga = edges(cuts[0], cuts[1] - cuts[0])
    acc, near, far = call(
        fold_z_kernel,
        [rows, b16(atoms, channels), b16(atoms, channels)],
        side,
        gy,
        az,
        fz,
    )
    dx = call(functools.partial(scatter_kernel, 0), rows, hot, rq)
    gb = edges(cuts[1], cuts[2] - cuts[1])
    near, far = swap_both(near, far, "gy")
    own, near, far = call(
        fold_y_kernel,
        [f32(atoms, channels), b16(half, channels), b16(half, channels)],
        side,
        acc,
        dx,
        extra,
        near,
        far,
        fy,
    )
    gc = edges(cuts[2], cuts[3] - cuts[2])
    near, far = swap_both(near, far, "gx")
    f0, f1, f2, f3, f4 = call(
        layer_one_reverse_kernel,
        [small] * 5,
        side,
        own,
        near,
        far,
        fx,
        amp,
        nbr,
        unit,
        rinv,
        basis,
        slope,
        ga,
        gb,
        gc,
        lanes,
        radial_one,
        mix_one,
        scratch=[pltpu.VMEM((6 * entries, atoms), F32), pltpu.VMEM((40, atoms), F32)],
    )
    az = partner(f4)
    acc, near, far = call(
        force_z_kernel, [f32(8, 2 * atoms), small, small], side, f0, f1, f2, f3, az, fz
    )
    near, far = swap_both(near, far, "gy")
    own, ghost = call(force_y_kernel, [small, small], side, acc, near, far, fy)
    near, far = swap_both(ghost, ghost, "gx")
    forces = call(force_x_kernel, f32(3, 1, atoms), side, own, near, far, fx)
    return (energies.reshape(occupancy.shape), forces.reshape(positions.shape))


def solution(mesh):
    return jax.shard_map(
        per_device,
        mesh=mesh,
        in_specs=(
            P(None, "gx", "gy", "gz", None),
            P("gx", "gy", "gz", None),
            P(None, "gx", "gy", "gz", None),
            P(None, "gx", "gy", "gz", None),
            P("gx", "gy", "gz", None, None),
            P("gx", "gy", "gz", None, None),
            P("gx", "gy", "gz", None),
            P(),
            P(),
            P(),
            P(),
            P(),
            P(),
            P(),
            P(),
        ),
        out_specs=(P("gx", "gy", "gz", None), P(None, "gx", "gy", "gz", None)),
        check_vma=False,
    )
```

```python
import functools
import math

import jax
import jax.numpy as jnp
from jax import lax
from jax.experimental import pallas as pl
from jax.experimental.pallas import tpu as pltpu
from jax.sharding import PartitionSpec as P

NB = 8
LX = 4
LY = 4
LZ = 8

SPACING = 1.8
CUTOFF = 5.0
SPREAD = 0.4
F32 = jnp.float32
BF16 = jnp.bfloat16

ROOT3 = 3.0**0.5
ROOT5 = 5.0**0.5
ROOT15 = 15.0**0.5
GROUP = 4


def dot(a, b, ca=1, cb=0, precision=None):
    return lax.dot_general(
        a, b, (((ca,), (cb,)), ((), ())), precision=precision, preferred_element_type=F32
    )


def rounded(x):
    return x.astype(BF16).astype(F32)


def dot3(a, b, ca=1, cb=0):
    a_hi, b_hi = rounded(a), rounded(b)
    left = jnp.concatenate([a_hi, a_hi, a - a_hi], axis=ca).astype(BF16)
    right = jnp.concatenate([b_hi, b - b_hi, b_hi], axis=cb).astype(BF16)
    return dot(left, right, ca, cb)


def dot_split(a, b):
    hi = rounded(b)
    right = jnp.concatenate([hi, b - hi], axis=0).astype(BF16)
    return dot(jnp.concatenate([a, a], axis=1), right)


def columns(row, count):
    hi = rounded(row)
    mid = rounded(row - hi)
    parts = jnp.concatenate([hi, mid, row - hi - mid], axis=0).astype(BF16)
    return dot(parts, jnp.ones((3, count), BF16), 0, 0)


def onehot(row, size):
    count = row.shape[-1]
    ids = lax.broadcasted_iota(jnp.int32, (size, count), 0)
    return jnp.where(ids == row, 1.0, 0.0).astype(BF16)


def lane_pick(blocks, rows):
    width = blocks[0].shape[-1]
    shift = width.bit_length() - 1
    lane = rows & (width - 1)
    block = rows >> shift
    out = jnp.take_along_axis(blocks[0], lane, axis=1)
    for index in range(1, len(blocks)):
        part = jnp.take_along_axis(blocks[index], lane, axis=1)
        out = jnp.where(block == index, part, out)
    return out


def spread_rows(row, count):
    return jnp.broadcast_to(row, (count, row.shape[-1]))


def by_side(side_ref, axis, if_odd, if_even):
    odd = side_ref[axis : axis + 1, 0 : if_odd.shape[1]] == 1
    return jnp.where(odd, if_odd, if_even)


def near_far(side_ref, axis, face_ref):
    low, high = face_ref[0:1, :], face_ref[1:2, :]
    return by_side(side_ref, axis, low, high), by_side(side_ref, axis, high, low)


def face_row(side_ref, fx_ref):
    return jnp.concatenate(near_far(side_ref, 0, fx_ref), axis=1)


def half_turn(x):
    half = x.shape[1] // 2
    return jnp.concatenate([x[:, half:], x[:, :half]], axis=1)


def low_lanes(shape):
    return lax.broadcasted_iota(jnp.int32, shape, 1) < shape[1] // 2


def shift_rows(shape, axis, amount):
    ids = lax.broadcasted_iota(jnp.int32, shape, 0)
    return jnp.where(ids == axis, amount, 0.0)


def pos_x_kernel(pos_ref, fx_ref, side_ref, coords_ref, send_ref):
    ids = lax.broadcasted_iota(jnp.int32, side_ref.shape, 0)
    first, second = lax.axis_index("gx") % 2, lax.axis_index("gy") % 2
    value = jnp.where(ids == 0, first, jnp.where(ids == 1, second, lax.axis_index("gz")))
    side_ref[...] = value
    rows = [pos_ref[i] for i in range(3)]
    coords = jnp.concatenate(rows + [jnp.zeros_like(rows[0])] * 5, axis=0)
    coords_ref[...] = coords
    send_ref[...] = lane_pick([coords], spread_rows(face_row(side_ref, fx_ref), 8))


def pos_y_kernel(side_ref, pos_ref, near_ref, far_ref, fy_ref, p1_ref, to_near_ref, to_far_ref):
    coords = pos_ref[...]
    shape = coords.shape
    first = low_lanes(shape)
    both = jnp.where(first, near_ref[...], far_ref[...])
    both = by_side(side_ref, 0, both, half_turn(both))
    step = shift_rows(shape, 0, LX * SPACING)
    ghost = jnp.where(first, both - step, both + step)
    p1_ref[...] = ghost
    near, far = near_far(side_ref, 1, fy_ref)
    to_near_ref[...] = lane_pick([coords, ghost], spread_rows(near, 8))
    to_far_ref[...] = lane_pick([coords, ghost], spread_rows(far, 8))


def pos_z_kernel(side_ref, pos_ref, p1_ref, near_ref, far_ref, fz_ref, p2_ref, p3_ref, out_ref):
    coords = pos_ref[...]
    shape = coords.shape
    near, far = near_ref[...], far_ref[...]
    low = by_side(side_ref, 1, near, far) - shift_rows(shape, 1, LY * SPACING)
    high = by_side(side_ref, 1, far, near) + shift_rows(shape, 1, LY * SPACING)
    p2_ref[...] = low
    p3_ref[...] = high
    out_ref[...] = lane_pick([coords, p1_ref[...], low, high], spread_rows(fz_ref[...], 8))


def layer_one_kernel(
    side_ref,
    pos_ref,
    p1_ref,
    p2_ref,
    p3_ref,
    pz_ref,
    nbr_ref,
    keep_ref,
    fx_ref,
    radial_ref,
    mix_ref,
    embed_ref,
    unit_ref,
    rinv_ref,
    basis_ref,
    slope_ref,
    amp_ref,
    h0_ref,
    to_near_ref,
    to_far_ref,
    mom_ref,
):
    entries, atoms = nbr_ref.shape
    nbr = nbr_ref[...]
    lane = nbr & (atoms - 1)
    block = nbr >> (atoms.bit_length() - 1)
    rise = jnp.where(side_ref[2:3, :] == 0, LZ * SPACING, -LZ * SPACING)
    last = pz_ref[...] + shift_rows(pz_ref.shape, 2, rise)
    tables = [pos_ref[...], p1_ref[...], p2_ref[...], p3_ref[...], last]
    vec = []
    for axis in range(3):
        got = None
        for index, table in enumerate(tables):
            spread = spread_rows(table[axis : axis + 1, :], entries)
            part = jnp.take_along_axis(spread, lane, axis=1)
            got = part if index == 0 else jnp.where(block == index, part, got)
        vec.append(got - pos_ref[axis : axis + 1, :])
    r_sq = vec[0] * vec[0] + vec[1] * vec[1] + vec[2] * vec[2]
    dist = jnp.sqrt(r_sq)
    rinv = 1.0 / dist
    ux, uy, uz = (v * rinv for v in vec)
    rinv_ref[...] = rinv
    unit_ref[0:entries, :] = ux
    unit_ref[entries : 2 * entries, :] = uy
    unit_ref[2 * entries : 3 * entries, :] = uz
    scaled = jnp.minimum(dist * (1.0 / CUTOFF), 1.0)
    phase = scaled * math.pi
    sine = jnp.sin(phase)
    cosine = jnp.cos(phase)
    inner = 1.0 - scaled * scaled
    weight = keep_ref[...].astype(F32) * (2.0 / CUTOFF) ** 0.5
    env = weight * inner * inner * rinv
    env_slope = -env * rinv - weight * rinv * (4.0 / CUTOFF) * scaled * inner
    twice = 2.0 * cosine
    s_prev, s_now = jnp.zeros_like(sine), sine
    c_prev, c_now = jnp.ones_like(cosine), cosine
    basis = []
    for k in range(NB):
        bk = s_now * env
        basis.append(bk)
        basis_ref[k * entries : (k + 1) * entries, :] = bk
        slope_ref[k * entries : (k + 1) * entries, :] = (
            c_now * env * ((k + 1) * math.pi / CUTOFF) + s_now * env_slope
        )
        s_prev, s_now = s_now, twice * s_now - s_prev
        c_prev, c_now = c_now, twice * c_now - c_prev
    angular = harmonics(ux, uy, uz)
    for m in range(9):
        for k in range(NB):
            prod = basis[k] if m == 0 else basis[k] * angular[m]
            mom_ref[k : k + 1, m * atoms : (m + 1) * atoms] = jnp.sum(prod, axis=0, keepdims=True)
    amp = SPREAD * dot3(radial_ref[...], mom_ref[...], 0, 0)
    amp_ref[...] = amp
    inv = invariants([amp[:, m * atoms : (m + 1) * atoms] for m in range(9)])
    h1 = dot(mix_ref[...], inv, 0, 0)
    h1 = h1 + columns(embed_ref[...], atoms)
    h1b = h1.astype(BF16)
    h0_ref[...] = h1b
    both = dot(h1b, onehot(face_row(side_ref, fx_ref), atoms))
    to_near_ref[...], to_far_ref[...] = pack_halves(both)


def harmonics(ux, uy, uz):
    return [
        None,
        ROOT3 * ux,
        ROOT3 * uy,
        ROOT3 * uz,
        ROOT15 * ux * uy,
        ROOT15 * uy * uz,
        0.5 * ROOT5 * (3.0 * uz * uz - 1.0),
        ROOT15 * ux * uz,
        0.5 * ROOT15 * (ux * ux - uy * uy),
    ]


def invariants(amp):
    first = amp[1] * amp[1] + amp[2] * amp[2] + amp[3] * amp[3]
    second = amp[4] * amp[4] + amp[5] * amp[5] + amp[6] * amp[6]
    second = second + amp[7] * amp[7] + amp[8] * amp[8]
    return jnp.concatenate([amp[0], first, second], axis=0).astype(BF16)


def pack_halves(both):
    rows, _ = both.shape
    top, low = both[0 : rows // 2], both[rows // 2 :]
    first = low_lanes(top.shape)
    near = jnp.where(first, top, half_turn(low))
    far = jnp.where(first, half_turn(top), low)
    return near.astype(BF16), far.astype(BF16)


def unpack_halves(low, high):
    first = low_lanes(low.shape)
    top = jnp.where(first, low, half_turn(high))
    bottom = jnp.where(first, half_turn(low), high)
    return jnp.concatenate([top, bottom], axis=0)


def feat_y_kernel(side_ref, h0_ref, near_ref, far_ref, fy_ref, h1_ref, to_near_ref, to_far_ref):
    near, far = near_ref[...].astype(F32), far_ref[...].astype(F32)
    low, high = by_side(side_ref, 0, near, far), by_side(side_ref, 0, far, near)
    ghost = unpack_halves(low, high).astype(BF16)
    h1_ref[...] = ghost
    table = jnp.concatenate([h0_ref[...], ghost], axis=1)
    size = table.shape[1]
    near, far = near_far(side_ref, 1, fy_ref)
    to_near_ref[...] = dot(table, onehot(near, size)).astype(BF16)
    to_far_ref[...] = dot(table, onehot(far, size)).astype(BF16)


def sides(side_ref, axis, near_ref, far_ref):
    near, far = near_ref[...].astype(F32), far_ref[...].astype(F32)
    low, high = by_side(side_ref, axis, near, far), by_side(side_ref, axis, far, near)
    return low.astype(BF16), high.astype(BF16)


def feat_z_kernel(side_ref, h0_ref, h1_ref, near_ref, far_ref, fz_ref, out_ref, h2_ref, h3_ref):
    low, high = sides(side_ref, 1, near_ref, far_ref)
    h2_ref[...] = low
    h3_ref[...] = high
    table = jnp.concatenate([h0_ref[...], h1_ref[...], low, high], axis=1)
    out_ref[...] = dot(table, onehot(fz_ref[...], table.shape[1])).astype(BF16)


def entry_rows(ref, first):
    return jnp.concatenate([ref[pl.ds(first + jj, 1), :] for jj in range(GROUP)], axis=1)


def hot_kernel(nbr_ref, hot_ref, lane_ref):
    atoms = nbr_ref.shape[1]

    def body(step, carry):
        row = entry_rows(nbr_ref, step * GROUP)
        hot_ref[step] = onehot(row, hot_ref.shape[1])
        lane_ref[step] = onehot(row & (atoms - 1), atoms)
        return carry

    lax.fori_loop(0, hot_ref.shape[0], body, 0)


def stack3(hi, lo):
    return jnp.concatenate([hi, lo, hi], axis=0).astype(BF16)


def radial_kernel(basis_ref, slope_ref, unit_ref, radial_ref, rad_ref, slo_ref, y_ref, rts_ref):
    entries = basis_ref.shape[0] // NB
    channels = radial_ref.shape[1]
    rt = radial_ref[...]
    hi = rt.astype(BF16).astype(F32)
    lo = rt - hi
    pad = jnp.zeros((channels - 3 * NB, channels), F32)
    rts_ref[...] = jnp.transpose(jnp.concatenate([hi, hi, lo, pad], axis=0)).astype(BF16)
    ux = unit_ref[0:entries, :]
    uy = unit_ref[entries : 2 * entries, :]
    uz = unit_ref[2 * entries : 3 * entries, :]
    for m, val in enumerate(harmonics(ux, uy, uz)):
        if m:
            y_ref[(m - 1) * entries : m * entries, :] = val

    def radial_cols(ref, first):
        cols = [ref[pl.ds(first + jj, NB, stride=entries), :] for jj in range(GROUP)]
        value = jnp.concatenate(cols, axis=1)
        top = value.astype(BF16).astype(F32)
        return stack3(top, value - top)

    rts = rts_ref[:, 0 : 3 * NB]
    for step in range(rad_ref.shape[0]):
        rad_ref[step] = dot(rts, radial_cols(basis_ref, step * GROUP))
        slo_ref[step] = dot(rts, radial_cols(slope_ref, step * GROUP))


def gather_first_kernel(h0_ref, h1_ref, hot_ref, hg_ref, table_ref):
    atoms = h0_ref.shape[1]
    table_ref[:, 0:atoms] = h0_ref[...]
    table_ref[:, atoms:] = h1_ref[...]

    for step in range(hot_ref.shape[0]):
        hg_ref[step] = dot(table_ref[...], hot_ref[step, 0 : 2 * atoms, :])


def gather_more_kernel(h2_ref, h3_ref, hot_ref, old_ref, hg_ref, table_ref):
    atoms = h2_ref.shape[1]
    table_ref[:, 0:atoms] = h2_ref[...]
    table_ref[:, atoms:] = h3_ref[...]

    for step in range(hot_ref.shape[0]):
        more = dot(table_ref[...], hot_ref[step, 2 * atoms : 4 * atoms, :])
        hg_ref[step] = old_ref[step] + more


def layer_two_kernel(
    h0_ref,
    h4_ref,
    hot_ref,
    old_ref,
    rad_ref,
    y_ref,
    occ_ref,
    mix_ref,
    rone_ref,
    rhid_ref,
    rout_ref,
    hg_ref,
    en_ref,
    raw_ref,
    extra_ref,
    rq_ref,
    gz_ref,
    acc_ref,
    dh_ref,
):
    channels, atoms = h0_ref.shape
    steps = hot_ref.shape[0]
    entries = steps * GROUP
    blocks = channels // 8
    acc_ref[...] = jnp.zeros_like(acc_ref)

    def prepare(step):
        hg_ref[step] = old_ref[step] + dot(h4_ref[...], hot_ref[step, 4 * atoms :, :])

    def accumulate(step):
        first = step * GROUP
        for pair in range(blocks // 2):
            spans = [slice(cb * 8, cb * 8 + 8) for cb in (2 * pair, 2 * pair + 1)]
            msgs = []
            for rows in spans:
                line = []
                for jj in range(GROUP):
                    cols = slice(jj * atoms, (jj + 1) * atoms)
                    line.append(hg_ref[step, rows, cols] * rad_ref[step, rows, cols])
                msgs.append(line)
            for m in range(9):
                if m:
                    at = (m - 1) * entries + first
                    yvs = [y_ref[pl.ds(at + jj, 1), :] for jj in range(GROUP)]
                for rows, line in zip(spans, msgs):
                    if m:
                        terms = [line[jj] * yvs[jj] for jj in range(GROUP)]
                    else:
                        terms = line
                    while len(terms) > 1:
                        terms = [a + b for a, b in zip(terms[::2], terms[1::2])]
                    acc_ref[m, rows, :] += terms[0]

    prepare(0)
    prepare(1)

    def forward_body(trip, carry):
        for part in range(2):
            accumulate(2 * trip + part)
        for part in range(2):
            prepare(2 * trip + 2 + part)
        return carry

    lax.fori_loop(0, steps // 2 - 1, forward_body, 0)
    for part in range(2):
        accumulate(steps - 2 + part)

    occ = occ_ref[...].astype(F32)
    amp = [SPREAD * acc_ref[m] for m in range(9)]
    own = h0_ref[...].astype(F32)
    h2 = dot(mix_ref[...], invariants(amp), 0, 0) + own
    pre = dot3(rhid_ref[...], h2, 1, 0)
    sig = 1.0 / (1.0 + jnp.exp(-pre))
    rout = columns(rout_ref[...], atoms)
    rone = columns(rone_ref[...], atoms)
    energy = jnp.sum(own * rone, axis=0, keepdims=True)
    energy = energy + jnp.sum(rout * pre * sig, axis=0, keepdims=True)
    en_ref[...] = occ * energy
    dpre = occ * rout * sig * (1.0 + pre * (1.0 - sig))
    dh2 = dot3(rhid_ref[...], dpre, 0, 0)
    dinv = dot_split(mix_ref[...], dh2)
    low = dinv[channels : 2 * channels]
    top = dinv[2 * channels :]
    extra_ref[...] = dh2 + occ * rone
    twice = 2.0 * SPREAD
    raw_ref[0] = SPREAD * dinv[0:channels]
    for m in range(1, 9):
        raw_ref[m] = (twice * amp[m]) * (low if m < 4 else top)
    dh_ref[...] = jnp.zeros_like(dh_ref)

    def reverse(step):
        first = step * GROUP
        for pair in range(blocks // 2):
            spans = [slice(cb * 8, cb * 8 + 8) for cb in (2 * pair, 2 * pair + 1)]
            ds = [[raw_ref[m, rows, :] for m in range(9)] for rows in spans]
            for jj in range(GROUP):
                cols = slice(jj * atoms, (jj + 1) * atoms)
                yvs = [y_ref[pl.ds((m - 1) * entries + first + jj, 1), :] for m in range(1, 9)]
                parts = []
                for rows, d in zip(spans, ds):
                    terms = [d[0]] + [yv * dm for yv, dm in zip(yvs, d[1:])]
                    q = terms[0] + terms[1]
                    for a, b in ((2, 3), (4, 5), (6, 7)):
                        q = q + (terms[a] + terms[b])
                    parts.append(rad_ref[step, rows, cols] * (q + terms[8]))
                value = jnp.concatenate(parts, axis=0).astype(BF16)
                rq_ref[step, pair * 16 : pair * 16 + 16, cols] = value

    def send(step):
        low = dot(hot_ref[step, 4 * atoms :, :], rq_ref[step], 1, 1)
        return low + dot(hot_ref[step + 1, 4 * atoms :, :], rq_ref[step + 1], 1, 1)

    reverse(0)
    reverse(1)

    def reverse_body(trip, carry):
        dh_ref[...] += send(2 * trip)
        for part in range(2):
            reverse(2 * trip + 2 + part)
        return carry

    lax.fori_loop(0, steps // 2 - 1, reverse_body, 0)
    gz_ref[...] = (dh_ref[...] + send(steps - 2)).astype(BF16)


def directions(d, unit):
    vx, vy, vz = unit
    cx = vy * d[4] + vz * d[7] + vx * d[8]
    cy = vx * d[4] + vz * d[5] - vy * d[8]
    cz = vy * d[5] + vx * d[7] + vz * d[6]
    return d[1] + cx, d[2] + cy, d[3] + cz, (cx, cy, cz)


def scatter_kernel(first, hot_ref, rq_ref, out_ref):
    size = out_ref.shape[0]
    total = None
    for step in range(hot_ref.shape[0]):
        part = dot(hot_ref[step, first : first + size, :], rq_ref[step], 1, 1)
        total = part if total is None else total + part
    out_ref[...] = total


def edge_kernel(start, hg_ref, rad_ref, slo_ref, d_ref, unit_ref, grad_ref, dd_ref):
    channels, atoms = d_ref.shape[1:]
    entries = hg_ref.shape[0] * GROUP
    count = grad_ref.shape[0] // (4 * GROUP)
    for m in range(9):
        if m == 0:
            dd_ref[m] = d_ref[0] - (0.5 * ROOT5) * d_ref[6]
        elif m < 4:
            dd_ref[m] = ROOT3 * d_ref[m]
        else:
            dd_ref[m] = (1.5 * ROOT5 if m == 6 else 0.5 * ROOT15) * d_ref[m]

    def body(step, carry):
        first = step * GROUP
        units = []
        for jj in range(GROUP):
            units.append([unit_ref[pl.ds(i * entries + first + jj, 1), :] for i in range(3)])
        sums = [[None] * 4 for _ in range(GROUP)]
        for cb in range(channels // 8):
            rows = slice(cb * 8, cb * 8 + 8)
            d = [dd_ref[m, rows, :] for m in range(9)]
            for jj in range(GROUP):
                cols = slice(jj * atoms, (jj + 1) * atoms)
                hg = hg_ref[step, rows, cols]
                ex, ey, ez, (cx, cy, cz) = directions(d, units[jj])
                vx, vy, vz = units[jj]
                q = d[0] + vx * ex + vy * ey + vz * ez
                msg = hg * rad_ref[step, rows, cols]
                parts = [
                    msg * (ex + cx),
                    msg * (ey + cy),
                    msg * (ez + cz),
                    hg * q * slo_ref[step, rows, cols],
                ]
                for i in range(4):
                    prior = sums[jj][i]
                    sums[jj][i] = parts[i] if prior is None else prior + parts[i]
        for jj in range(GROUP):
            for i in range(4):
                row = pl.ds(i * count * GROUP + first - start * GROUP + jj, 1)
                grad_ref[row, :] = jnp.sum(sums[jj][i], axis=0, keepdims=True)
        return carry

    lax.fori_loop(start, start + count, body, 0)


def fold_z_kernel(side_ref, gy_ref, az_ref, fz_ref, acc_ref, to_near_ref, to_far_ref):
    size = gy_ref.shape[0]
    quarter = size // 2
    add = dot(onehot(fz_ref[...], 2 * size), az_ref[...])
    acc_ref[...] = add[0:size]
    rows = rounded(gy_ref[...]) + add[size:]
    low, high = rows[0:quarter], rows[quarter:]
    to_near_ref[...] = by_side(side_ref, 1, low, high).astype(BF16)
    to_far_ref[...] = by_side(side_ref, 1, high, low).astype(BF16)


def fold_y_kernel(
    side_ref, acc_ref, gx_ref, extra_ref, near_ref, far_ref, fy_ref, own_ref, to_near_ref, to_far_ref
):
    size = acc_ref.shape[0]
    half = size // 2
    quarter = half // 2
    near, far = near_far(side_ref, 1, fy_ref)
    rows = acc_ref[...] + dot(onehot(near, size), near_ref[...])
    rows = rows + dot(onehot(far, size), far_ref[...])
    own = gx_ref[0:half, :] + jnp.transpose(extra_ref[...])
    own_ref[...] = rows[0:half] + own.astype(BF16).astype(F32)
    ghost = rows[half:] + gx_ref[half:, :].astype(BF16).astype(F32)
    low, high = ghost[0:quarter], ghost[quarter:]
    to_near_ref[...] = by_side(side_ref, 0, low, high).astype(BF16)
    to_far_ref[...] = by_side(side_ref, 0, high, low).astype(BF16)


def layer_one_reverse_kernel(
    side_ref,
    own_ref,
    near_ref,
    far_ref,
    fx_ref,
    amp_ref,
    nbr_ref,
    unit_ref,
    rinv_ref,
    basis_ref,
    slope_ref,
    ga_ref,
    gb_ref,
    gc_ref,
    lane_ref,
    radial_ref,
    mix_ref,
    f0_ref,
    f1_ref,
    f2_ref,
    f3_ref,
    f4_ref,
    dv_ref,
    sc_ref,
):
    entries, atoms = nbr_ref.shape
    channels = own_ref.shape[1]
    rows = own_ref[...]
    near, far = near_far(side_ref, 0, fx_ref)
    rows = rows + dot(onehot(near, atoms), near_ref[...])
    rows = rows + dot(onehot(far, atoms), far_ref[...])
    cot = jnp.transpose(rows)
    dinv = dot_split(mix_ref[...], cot)
    low = dinv[channels : 2 * channels]
    top = dinv[2 * channels :]
    pieces = [dinv[0:channels]]
    for m in range(1, 9):
        amp = amp_ref[:, m * atoms : (m + 1) * atoms]
        pieces.append(2.0 * amp * (low if m < 4 else top))
    dmom = SPREAD * dot3(radial_ref[...], jnp.concatenate(pieces, axis=1), 1, 0)
    ux = unit_ref[0:entries, :]
    uy = unit_ref[entries : 2 * entries, :]
    uz = unit_ref[2 * entries : 3 * entries, :]
    basis = [basis_ref[k * entries : (k + 1) * entries, :] for k in range(NB)]
    slope = [slope_ref[k * entries : (k + 1) * entries, :] for k in range(NB)]
    angular = harmonics(ux, uy, uz)
    edge = []
    for i in range(4):
        rows = []
        for ref in (ga_ref, gb_ref, gc_ref):
            count = ref.shape[0] // 4
            rows.append(ref[i * count : (i + 1) * count, :])
        edge.append(jnp.concatenate(rows, axis=0))
    dr = edge[3]
    dy = []
    for m in range(9):
        part = None
        sl = None
        for k in range(NB):
            row = dmom[k : k + 1, m * atoms : (m + 1) * atoms]
            sl = slope[k] * row if sl is None else sl + slope[k] * row
            if m:
                part = basis[k] * row if part is None else part + basis[k] * row
        dr = dr + (sl if m == 0 else sl * angular[m])
        dy.append(part)
    wx = edge[0] + ROOT3 * dy[1]
    wx = wx + ROOT15 * (uy * dy[4] + uz * dy[7] + ux * dy[8])
    wy = edge[1] + ROOT3 * dy[2]
    wy = wy + ROOT15 * (ux * dy[4] + uz * dy[5] - uy * dy[8])
    wz = edge[2] + ROOT3 * dy[3]
    wz = wz + ROOT15 * (uy * dy[5] + ux * dy[7]) + (3.0 * ROOT5) * uz * dy[6]
    rinv = rinv_ref[...]
    along = dr - rinv * (ux * wx + uy * wy + uz * wz)
    grads = [wx * rinv + along * ux, wy * rinv + along * uy, wz * rinv + along * uz]
    centre = []
    for i in range(3):
        centre.append(jnp.sum(grads[i], axis=0, keepdims=True))
        top16 = grads[i].astype(BF16).astype(F32)
        dv_ref[i * entries : (i + 1) * entries, :] = top16
        dv_ref[(3 + i) * entries : (4 + i) * entries, :] = grads[i] - top16
    shift = atoms.bit_length() - 1
    total = None
    for step in range(entries // GROUP):
        first = step * GROUP
        block = entry_rows(nbr_ref, first) >> shift
        cols = [dv_ref[pl.ds(first + jj, 6, stride=entries), :] for jj in range(GROUP)]
        value = jnp.concatenate(cols, axis=1)
        value = jnp.concatenate([value, jnp.zeros_like(value[0:2])], axis=0)
        parts = [jnp.where(block == index, value, 0.0) for index in range(5)]
        part = dot(jnp.concatenate(parts, axis=0).astype(BF16), lane_ref[step], 1, 1)
        total = part if total is None else total + part
    sc_ref[...] = total
    zero = jnp.zeros((5, atoms), F32)
    own = jnp.concatenate(centre + [zero], axis=0)
    for index, ref in enumerate((f0_ref, f1_ref, f2_ref, f3_ref, f4_ref)):
        base = index * 8
        value = sc_ref[base : base + 3, :] + sc_ref[base + 3 : base + 6, :]
        value = jnp.concatenate([value, zero], axis=0)
        ref[...] = value - own if index == 0 else value


def scatter_lanes(values, row, size):
    hi = rounded(values)
    mid = rounded(values - hi)
    parts = jnp.concatenate([hi, mid, values - hi - mid], axis=0).astype(BF16)
    out = dot(parts, onehot(row, size), 1, 1)
    rows = values.shape[0]
    return out[0:rows] + out[rows : 2 * rows] + out[2 * rows :]


def force_z_kernel(
    side_ref, f0_ref, f1_ref, f2_ref, f3_ref, az_ref, fz_ref, out_ref, to_near_ref, to_far_ref
):
    atoms = f0_ref.shape[1]
    add = scatter_lanes(az_ref[...], fz_ref[...], 4 * atoms)
    out_ref[:, 0:atoms] = f0_ref[...] + add[:, 0:atoms]
    out_ref[:, atoms : 2 * atoms] = f1_ref[...] + add[:, atoms : 2 * atoms]
    low = f2_ref[...] + add[:, 2 * atoms : 3 * atoms]
    high = f3_ref[...] + add[:, 3 * atoms :]
    to_near_ref[...] = by_side(side_ref, 1, low, high)
    to_far_ref[...] = by_side(side_ref, 1, high, low)


def force_y_kernel(side_ref, acc_ref, near_ref, far_ref, fy_ref, own_ref, ghost_ref):
    size = acc_ref.shape[1]
    rows = acc_ref[...]
    near, far = near_far(side_ref, 1, fy_ref)
    rows = rows + scatter_lanes(near_ref[...], near, size)
    rows = rows + scatter_lanes(far_ref[...], far, size)
    own_ref[...] = rows[:, 0 : size // 2]
    ghost = rows[:, size // 2 :]
    ghost_ref[...] = by_side(side_ref, 0, ghost, half_turn(ghost))


def force_x_kernel(side_ref, own_ref, near_ref, far_ref, fx_ref, en_ref, out_ref, total_ref):
    total_ref[...] = en_ref[...]
    size = own_ref.shape[1]
    both = jnp.where(low_lanes(own_ref.shape), near_ref[...], far_ref[...])
    rows = own_ref[...] + scatter_lanes(both, face_row(side_ref, fx_ref), size)
    for i in range(3):
        out_ref[i] = -rows[i : i + 1]


def call(kernel, outs, *args, scratch=(), vmem=8, aliases={}, cost=1):
    specs = []
    for arg in args:
        specs.append(pl.BlockSpec(memory_space=pltpu.VMEM))
    single = not isinstance(outs, (list, tuple))
    shapes = [outs] if single else list(outs)
    result = pl.pallas_call(
        kernel,
        out_shape=shapes,
        in_specs=specs,
        out_specs=[pl.BlockSpec(memory_space=pltpu.VMEM)] * len(shapes),
        scratch_shapes=list(scratch),
        input_output_aliases=aliases,
        cost_estimate=pl.CostEstimate(
            flops=cost * 10**9, bytes_accessed=cost * 10**6, transcendentals=0
        ),
        compiler_params=pltpu.CompilerParams(vmem_limit_bytes=vmem * 1024 * 1024),
    )(*args)
    return result[0] if single else result


def pair_swap(x, axis, far):
    count = lax.axis_size(axis)
    assert count % 2 == 0
    pairs = []
    for i in range(count):
        up = (i % 2 == 0) != far
        pairs.append((i, (i + (1 if up else -1)) % count))
    return lax.ppermute(x, axis, pairs)


def partner(x):
    axis = "gz"
    return lax.ppermute(x, axis, [(i, i ^ 1) for i in range(lax.axis_size(axis))])


def swap_both(near, far, axis):
    from_far = pair_swap(far, axis, True)
    from_near = pair_swap(near, axis, False)
    return from_near, from_far


def per_device(
    positions,
    occupancy,
    neighbours,
    keep,
    face_x,
    face_y,
    face_z,
    radial_one,
    mix_one,
    embed,
    radial_two,
    mix_two,
    read_one,
    read_hidden,
    read_out,
):
    atoms = positions.shape[-1]
    entries = neighbours.shape[0]
    channels = radial_one.shape[1]
    pos = positions.reshape(3, 1, atoms)
    nbr = neighbours.reshape(entries, atoms)
    kept = keep.reshape(entries, atoms)
    occ = occupancy.reshape(1, atoms)
    fx = face_x.reshape(2, face_x.shape[-1])
    fy = face_y.reshape(2, face_y.shape[-1])
    fz = face_z.reshape(1, face_z.shape[-1])
    embed = embed.reshape(1, channels)
    read_one = read_one.reshape(1, channels)
    read_out = read_out.reshape(1, read_out.shape[0])
    read_hidden = read_hidden.T

    def f32(*shape):
        return jax.ShapeDtypeStruct(shape, F32)

    def b16(*shape):
        return jax.ShapeDtypeStruct(shape, BF16)

    small = f32(8, atoms)
    side = jax.ShapeDtypeStruct((8, atoms), jnp.int32)
    side, pos, sent = call(pos_x_kernel, [side, small, small], pos, fx)
    steps = entries // GROUP
    width = GROUP * atoms
    hot, lanes = call(
        hot_kernel, [b16(steps, 5 * atoms, width), b16(steps, atoms, width)], nbr
    )
    near, far = swap_both(sent, sent, "gx")
    p1, near, far = call(pos_y_kernel, [small] * 3, side, pos, near, far, fy)
    near, far = swap_both(near, far, "gy")
    p2, p3, sent = call(pos_z_kernel, [small] * 3, side, pos, p1, near, far, fz)
    pz = partner(sent)

    half = atoms // 2
    square = b16(channels, atoms)
    unit, rinv, basis, slope, amp, h0, near, far = call(
        layer_one_kernel,
        [
            f32(3 * entries, atoms),
            f32(entries, atoms),
            f32(NB * entries, atoms),
            f32(NB * entries, atoms),
            f32(channels, 9 * atoms),
            square,
            b16(channels // 2, atoms),
            b16(channels // 2, atoms),
        ],
        side,
        pos,
        p1,
        p2,
        p3,
        pz,
        nbr,
        kept,
        fx,
        radial_one,
        mix_one,
        embed,
        scratch=[pltpu.VMEM((NB, 9 * atoms), F32)],
    )
    big = f32(steps, channels, width)
    rad, slo, ylm = call(
        radial_kernel,
        [big, big, f32(8 * entries, atoms)],
        basis,
        slope,
        unit,
        radial_two,
        scratch=[pltpu.VMEM((channels, channels), BF16)],
    )
    near, far = swap_both(near, far, "gx")
    h1, near, far = call(feat_y_kernel, [square] * 3, side, h0, near, far, fy)
    table = [pltpu.VMEM((channels, 2 * atoms), BF16)]
    hg = call(gather_first_kernel, big, h0, h1, hot, scratch=table)
    near, far = swap_both(near, far, "gy")
    sent, h2, h3 = call(feat_z_kernel, [square] * 3, side, h0, h1, near, far, fz)
    hg = call(gather_more_kernel, big, h2, h3, hot, hg, scratch=table, aliases={3: 0})
    h4 = partner(sent)

    hg, energies, dmat, extra, rq, gz = call(
        layer_two_kernel,
        [
            big,
            f32(1, atoms),
            f32(9, channels, atoms),
            f32(channels, atoms),
            b16(steps, channels, width),
            b16(atoms, channels),
        ],
        h0,
        h4,
        hot,
        hg,
        rad,
        ylm,
        occ,
        mix_two,
        read_one,
        read_hidden,
        read_out,
        scratch=[pltpu.VMEM((9, channels, atoms), F32), pltpu.VMEM((atoms, channels), F32)],
        aliases={3: 0},
    )
    az = partner(gz)
    rows = f32(2 * atoms, channels)

    def edges(start, count):
        out = f32(4 * count * GROUP, atoms)
        scaled = [pltpu.VMEM((9, channels, atoms), F32)]
        kernel = functools.partial(edge_kernel, start)
        return call(kernel, out, hg, rad, slo, dmat, unit, scratch=scaled)

    cuts = [0, 2 * (steps // 7), 3 * (steps // 7), steps]
    gy = call(functools.partial(scatter_kernel, 2 * atoms), rows, hot, rq)
    ga = edges(cuts[0], cuts[1] - cuts[0])
    acc, near, far = call(
        fold_z_kernel,
        [rows, b16(atoms, channels), b16(atoms, channels)],
        side,
        gy,
        az,
        fz,
    )
    dx = call(functools.partial(scatter_kernel, 0), rows, hot, rq)
    gb = edges(cuts[1], cuts[2] - cuts[1])
    near, far = swap_both(near, far, "gy")
    own, near, far = call(
        fold_y_kernel,
        [f32(atoms, channels), b16(half, channels), b16(half, channels)],
        side,
        acc,
        dx,
        extra,
        near,
        far,
        fy,
    )
    gc = edges(cuts[2], cuts[3] - cuts[2])
    near, far = swap_both(near, far, "gx")
    f0, f1, f2, f3, f4 = call(
        layer_one_reverse_kernel,
        [small] * 5,
        side,
        own,
        near,
        far,
        fx,
        amp,
        nbr,
        unit,
        rinv,
        basis,
        slope,
        ga,
        gb,
        gc,
        lanes,
        radial_one,
        mix_one,
        scratch=[pltpu.VMEM((6 * entries, atoms), F32), pltpu.VMEM((40, atoms), F32)],
    )
    az = partner(f4)
    acc, near, far = call(
        force_z_kernel, [f32(8, 2 * atoms), small, small], side, f0, f1, f2, f3, az, fz
    )
    near, far = swap_both(near, far, "gy")
    own, ghost = call(force_y_kernel, [small, small], side, acc, near, far, fy)
    near, far = swap_both(ghost, ghost, "gx")
    forces, energies = call(
        force_x_kernel, [f32(3, 1, atoms), f32(1, atoms)], side, own, near, far, fx, energies
    )
    return (energies.reshape(occupancy.shape), forces.reshape(positions.shape))


def solution(mesh):
    return jax.shard_map(
        per_device,
        mesh=mesh,
        in_specs=(
            P(None, "gx", "gy", "gz", None),
            P("gx", "gy", "gz", None),
            P(None, "gx", "gy", "gz", None),
            P(None, "gx", "gy", "gz", None),
            P("gx", "gy", "gz", None, None),
            P("gx", "gy", "gz", None, None),
            P("gx", "gy", "gz", None),
            P(),
            P(),
            P(),
            P(),
            P(),
            P(),
            P(),
            P(),
        ),
        out_specs=(P("gx", "gy", "gz", None), P(None, "gx", "gy", "gz", None)),
        check_vma=False,
    )
```

```python
import functools
import math

import jax
import jax.numpy as jnp
from jax import lax
from jax.experimental import pallas as pl
from jax.experimental.pallas import tpu as pltpu
from jax.sharding import PartitionSpec as P

NB = 8
LX = 4
LY = 4
LZ = 8

SPACING = 1.8
CUTOFF = 5.0
SPREAD = 0.4
F32 = jnp.float32
BF16 = jnp.bfloat16

ROOT3 = 3.0**0.5
ROOT5 = 5.0**0.5
ROOT15 = 15.0**0.5
GROUP = 4


def dot(a, b, ca=1, cb=0, precision=None):
    return lax.dot_general(
        a, b, (((ca,), (cb,)), ((), ())), precision=precision, preferred_element_type=F32
    )


def rounded(x):
    return x.astype(BF16).astype(F32)


def dot3(a, b, ca=1, cb=0):
    a_hi, b_hi = rounded(a), rounded(b)
    left = jnp.concatenate([a_hi, a_hi, a - a_hi], axis=ca).astype(BF16)
    right = jnp.concatenate([b_hi, b - b_hi, b_hi], axis=cb).astype(BF16)
    return dot(left, right, ca, cb)


def dot_split(a, b):
    hi = rounded(b)
    right = jnp.concatenate([hi, b - hi], axis=0).astype(BF16)
    return dot(jnp.concatenate([a, a], axis=1), right)


def columns(row, count):
    hi = rounded(row)
    mid = rounded(row - hi)
    parts = jnp.concatenate([hi, mid, row - hi - mid], axis=0).astype(BF16)
    return dot(parts, jnp.ones((3, count), BF16), 0, 0)


def onehot(row, size):
    count = row.shape[-1]
    ids = lax.broadcasted_iota(jnp.int32, (size, count), 0)
    return jnp.where(ids == row, 1.0, 0.0).astype(BF16)


def lane_pick(blocks, rows):
    width = blocks[0].shape[-1]
    shift = width.bit_length() - 1
    lane = rows & (width - 1)
    block = rows >> shift
    out = jnp.take_along_axis(blocks[0], lane, axis=1)
    for index in range(1, len(blocks)):
        part = jnp.take_along_axis(blocks[index], lane, axis=1)
        out = jnp.where(block == index, part, out)
    return out


def spread_rows(row, count):
    return jnp.broadcast_to(row, (count, row.shape[-1]))


def by_side(side_ref, axis, if_odd, if_even):
    odd = side_ref[axis : axis + 1, 0 : if_odd.shape[1]] == 1
    return jnp.where(odd, if_odd, if_even)


def near_far(side_ref, axis, face_ref):
    low, high = face_ref[0:1, :], face_ref[1:2, :]
    return by_side(side_ref, axis, low, high), by_side(side_ref, axis, high, low)


def face_row(side_ref, fx_ref):
    return jnp.concatenate(near_far(side_ref, 0, fx_ref), axis=1)


def half_turn(x):
    half = x.shape[1] // 2
    return jnp.concatenate([x[:, half:], x[:, :half]], axis=1)


def low_lanes(shape):
    return lax.broadcasted_iota(jnp.int32, shape, 1) < shape[1] // 2


def shift_rows(shape, axis, amount):
    ids = lax.broadcasted_iota(jnp.int32, shape, 0)
    return jnp.where(ids == axis, amount, 0.0)


def pos_x_kernel(pos_ref, fx_ref, side_ref, coords_ref, send_ref):
    ids = lax.broadcasted_iota(jnp.int32, side_ref.shape, 0)
    first, second = lax.axis_index("gx") % 2, lax.axis_index("gy") % 2
    value = jnp.where(ids == 0, first, jnp.where(ids == 1, second, lax.axis_index("gz")))
    side_ref[...] = value
    rows = [pos_ref[i] for i in range(3)]
    coords = jnp.concatenate(rows + [jnp.zeros_like(rows[0])] * 5, axis=0)
    coords_ref[...] = coords
    send_ref[...] = lane_pick([coords], spread_rows(face_row(side_ref, fx_ref), 8))


def pos_y_kernel(side_ref, pos_ref, near_ref, far_ref, fy_ref, p1_ref, to_near_ref, to_far_ref):
    coords = pos_ref[...]
    shape = coords.shape
    first = low_lanes(shape)
    both = jnp.where(first, near_ref[...], far_ref[...])
    both = by_side(side_ref, 0, both, half_turn(both))
    step = shift_rows(shape, 0, LX * SPACING)
    ghost = jnp.where(first, both - step, both + step)
    p1_ref[...] = ghost
    near, far = near_far(side_ref, 1, fy_ref)
    to_near_ref[...] = lane_pick([coords, ghost], spread_rows(near, 8))
    to_far_ref[...] = lane_pick([coords, ghost], spread_rows(far, 8))


def pos_z_kernel(side_ref, pos_ref, p1_ref, near_ref, far_ref, fz_ref, p2_ref, p3_ref, out_ref):
    coords = pos_ref[...]
    shape = coords.shape
    near, far = near_ref[...], far_ref[...]
    low = by_side(side_ref, 1, near, far) - shift_rows(shape, 1, LY * SPACING)
    high = by_side(side_ref, 1, far, near) + shift_rows(shape, 1, LY * SPACING)
    p2_ref[...] = low
    p3_ref[...] = high
    out_ref[...] = lane_pick([coords, p1_ref[...], low, high], spread_rows(fz_ref[...], 8))


def layer_one_kernel(
    side_ref,
    pos_ref,
    p1_ref,
    p2_ref,
    p3_ref,
    pz_ref,
    nbr_ref,
    keep_ref,
    fx_ref,
    radial_ref,
    mix_ref,
    embed_ref,
    unit_ref,
    rinv_ref,
    basis_ref,
    slope_ref,
    amp_ref,
    h0_ref,
    to_near_ref,
    to_far_ref,
    last_ref,
    mom_ref,
):
    entries, atoms = nbr_ref.shape
    nbr = nbr_ref[...]
    lane = nbr & (atoms - 1)
    block = nbr >> (atoms.bit_length() - 1)
    rise = jnp.where(side_ref[2:3, :] == 0, LZ * SPACING, -LZ * SPACING)
    last = pz_ref[...] + shift_rows(pz_ref.shape, 2, rise)
    last_ref[...] = last
    tables = [pos_ref[...], p1_ref[...], p2_ref[...], p3_ref[...], last]
    vec = []
    for axis in range(3):
        got = None
        for index, table in enumerate(tables):
            spread = spread_rows(table[axis : axis + 1, :], entries)
            part = jnp.take_along_axis(spread, lane, axis=1)
            got = part if index == 0 else jnp.where(block == index, part, got)
        vec.append(got - pos_ref[axis : axis + 1, :])
    r_sq = vec[0] * vec[0] + vec[1] * vec[1] + vec[2] * vec[2]
    dist = jnp.sqrt(r_sq)
    rinv = 1.0 / dist
    ux, uy, uz = (v * rinv for v in vec)
    rinv_ref[...] = rinv
    unit_ref[0:entries, :] = ux
    unit_ref[entries : 2 * entries, :] = uy
    unit_ref[2 * entries : 3 * entries, :] = uz
    basis, slopes = radial_parts(dist, rinv, keep_ref[...].astype(F32), True)
    for k in range(NB):
        basis_ref[k * entries : (k + 1) * entries, :] = basis[k]
        slope_ref[k * entries : (k + 1) * entries, :] = slopes[k]
    angular = harmonics(ux, uy, uz)
    for m in range(9):
        for k in range(NB):
            prod = basis[k] if m == 0 else basis[k] * angular[m]
            mom_ref[k : k + 1, m * atoms : (m + 1) * atoms] = jnp.sum(prod, axis=0, keepdims=True)
    amp = SPREAD * dot3(radial_ref[...], mom_ref[...], 0, 0)
    amp_ref[...] = amp
    inv = invariants([amp[:, m * atoms : (m + 1) * atoms] for m in range(9)])
    h1 = dot(mix_ref[...], inv, 0, 0)
    h1 = h1 + columns(embed_ref[...], atoms)
    h1b = h1.astype(BF16)
    h0_ref[...] = h1b
    both = dot(h1b, onehot(face_row(side_ref, fx_ref), atoms))
    to_near_ref[...], to_far_ref[...] = pack_halves(both)


def radial_parts(dist, rinv, weight, with_slope):
    scaled = jnp.minimum(dist * (1.0 / CUTOFF), 1.0)
    phase = scaled * math.pi
    sine = jnp.sin(phase)
    cosine = jnp.cos(phase)
    inner = 1.0 - scaled * scaled
    weight = weight * (2.0 / CUTOFF) ** 0.5
    env = weight * inner * inner * rinv
    env_slope = -env * rinv - weight * rinv * (4.0 / CUTOFF) * scaled * inner
    twice = 2.0 * cosine
    s_prev, s_now = jnp.zeros_like(sine), sine
    c_prev, c_now = jnp.ones_like(cosine), cosine
    basis, slopes = [], []
    for k in range(NB):
        basis.append(s_now * env)
        if with_slope:
            slopes.append(c_now * env * ((k + 1) * math.pi / CUTOFF) + s_now * env_slope)
            c_prev, c_now = c_now, twice * c_now - c_prev
        s_prev, s_now = s_now, twice * s_now - s_prev
    return basis, slopes


def harmonics(ux, uy, uz):
    return [
        None,
        ROOT3 * ux,
        ROOT3 * uy,
        ROOT3 * uz,
        ROOT15 * ux * uy,
        ROOT15 * uy * uz,
        0.5 * ROOT5 * (3.0 * uz * uz - 1.0),
        ROOT15 * ux * uz,
        0.5 * ROOT15 * (ux * ux - uy * uy),
    ]


def invariants(amp):
    first = amp[1] * amp[1] + amp[2] * amp[2] + amp[3] * amp[3]
    second = amp[4] * amp[4] + amp[5] * amp[5] + amp[6] * amp[6]
    second = second + amp[7] * amp[7] + amp[8] * amp[8]
    return jnp.concatenate([amp[0], first, second], axis=0).astype(BF16)


def pack_halves(both):
    rows, _ = both.shape
    top, low = both[0 : rows // 2], both[rows // 2 :]
    first = low_lanes(top.shape)
    near = jnp.where(first, top, half_turn(low))
    far = jnp.where(first, half_turn(top), low)
    return near.astype(BF16), far.astype(BF16)


def unpack_halves(low, high):
    first = low_lanes(low.shape)
    top = jnp.where(first, low, half_turn(high))
    bottom = jnp.where(first, half_turn(low), high)
    return jnp.concatenate([top, bottom], axis=0)


def feat_y_kernel(side_ref, h0_ref, near_ref, far_ref, fy_ref, h1_ref, to_near_ref, to_far_ref):
    near, far = near_ref[...].astype(F32), far_ref[...].astype(F32)
    low, high = by_side(side_ref, 0, near, far), by_side(side_ref, 0, far, near)
    ghost = unpack_halves(low, high).astype(BF16)
    h1_ref[...] = ghost
    table = jnp.concatenate([h0_ref[...], ghost], axis=1)
    size = table.shape[1]
    near, far = near_far(side_ref, 1, fy_ref)
    to_near_ref[...] = dot(table, onehot(near, size)).astype(BF16)
    to_far_ref[...] = dot(table, onehot(far, size)).astype(BF16)


def sides(side_ref, axis, near_ref, far_ref):
    near, far = near_ref[...].astype(F32), far_ref[...].astype(F32)
    low, high = by_side(side_ref, axis, near, far), by_side(side_ref, axis, far, near)
    return low.astype(BF16), high.astype(BF16)


def feat_z_kernel(side_ref, h0_ref, h1_ref, near_ref, far_ref, fz_ref, out_ref, h2_ref, h3_ref):
    low, high = sides(side_ref, 1, near_ref, far_ref)
    h2_ref[...] = low
    h3_ref[...] = high
    table = jnp.concatenate([h0_ref[...], h1_ref[...], low, high], axis=1)
    out_ref[...] = dot(table, onehot(fz_ref[...], table.shape[1])).astype(BF16)


def entry_rows(ref, first):
    return jnp.concatenate([ref[pl.ds(first + jj, 1), :] for jj in range(GROUP)], axis=1)


def hot_kernel(nbr_ref, keep_ref, hot_ref, lane_ref, count_ref):
    atoms = nbr_ref.shape[1]
    count_ref[...] = jnp.zeros_like(count_ref)
    ids = lax.broadcasted_iota(jnp.int32, (atoms, atoms), 0) + 4 * atoms

    def body(step, carry):
        first = step * GROUP
        row = entry_rows(nbr_ref, first)
        hot_ref[step] = onehot(row, hot_ref.shape[1])
        lane_ref[step] = onehot(row & (atoms - 1), atoms)
        count = count_ref[...]
        for jj in range(GROUP):
            at = pl.ds(first + jj, 1)
            count = count + jnp.where(ids == nbr_ref[at, :], keep_ref[at, :].astype(F32), 0.0)
        count_ref[...] = count
        return carry

    lax.fori_loop(0, hot_ref.shape[0], body, 0)


def pair_kernel(pos_ref, last_ref, count_ref, radial_ref, pair_ref, wide_ref):
    atoms = pos_ref.shape[1]
    weight = count_ref[...]
    vec = []
    for axis in range(3):
        vec.append(columns(last_ref[axis : axis + 1, :], atoms) - pos_ref[axis : axis + 1, :])
    r_sq = vec[0] * vec[0] + vec[1] * vec[1] + vec[2] * vec[2]
    dist = jnp.sqrt(jnp.where(weight > 0.0, r_sq, 1.0))
    rinv = 1.0 / dist
    basis, _ = radial_parts(dist, rinv, weight, False)
    angular = harmonics(*(v * rinv for v in vec))
    for k in range(NB):
        wide_ref[:, k * atoms : (k + 1) * atoms] = columns(radial_ref[k : k + 1, :], atoms)
        for m in range(9):
            value = basis[k] if m == 0 else basis[k] * angular[m]
            pair_ref[k * atoms : (k + 1) * atoms, m * atoms : (m + 1) * atoms] = value.astype(BF16)


def stack3(hi, lo):
    return jnp.concatenate([hi, lo, hi], axis=0).astype(BF16)


def radial_kernel(basis_ref, slope_ref, unit_ref, radial_ref, rad_ref, slo_ref, y_ref, rts_ref):
    entries = basis_ref.shape[0] // NB
    channels = radial_ref.shape[1]
    rt = radial_ref[...]
    hi = rt.astype(BF16).astype(F32)
    lo = rt - hi
    pad = jnp.zeros((channels - 3 * NB, channels), F32)
    rts_ref[...] = jnp.transpose(jnp.concatenate([hi, hi, lo, pad], axis=0)).astype(BF16)
    ux = unit_ref[0:entries, :]
    uy = unit_ref[entries : 2 * entries, :]
    uz = unit_ref[2 * entries : 3 * entries, :]
    for m, val in enumerate(harmonics(ux, uy, uz)):
        if m:
            y_ref[(m - 1) * entries : m * entries, :] = val

    def radial_cols(ref, first):
        cols = [ref[pl.ds(first + jj, NB, stride=entries), :] for jj in range(GROUP)]
        value = jnp.concatenate(cols, axis=1)
        top = value.astype(BF16).astype(F32)
        return stack3(top, value - top)

    rts = rts_ref[:, 0 : 3 * NB]
    for step in range(rad_ref.shape[0]):
        rad_ref[step] = dot(rts, radial_cols(basis_ref, step * GROUP))
        slo_ref[step] = dot(rts, radial_cols(slope_ref, step * GROUP))


def gather_first_kernel(h0_ref, h1_ref, hot_ref, hg_ref, table_ref):
    atoms = h0_ref.shape[1]
    table_ref[:, 0:atoms] = h0_ref[...]
    table_ref[:, atoms:] = h1_ref[...]

    for step in range(hot_ref.shape[0]):
        hg_ref[step] = dot(table_ref[...], hot_ref[step, 0 : 2 * atoms, :])


def gather_more_kernel(h2_ref, h3_ref, hot_ref, old_ref, hg_ref, table_ref):
    atoms = h2_ref.shape[1]
    table_ref[:, 0:atoms] = h2_ref[...]
    table_ref[:, atoms:] = h3_ref[...]

    for step in range(hot_ref.shape[0]):
        more = dot(table_ref[...], hot_ref[step, 2 * atoms : 4 * atoms, :])
        hg_ref[step] = old_ref[step] + more


def gather_last_kernel(h4_ref, hot_ref, old_ref, hg_ref):
    atoms = h4_ref.shape[1]
    for step in range(hot_ref.shape[0]):
        hg_ref[step] = old_ref[step] + dot(h4_ref[...], hot_ref[step, 4 * atoms :, :])


def partial_kernel(hg_ref, rad_ref, y_ref, acc_ref):
    steps, channels, width = hg_ref.shape
    atoms = width // GROUP
    entries = steps * GROUP
    blocks = channels // 8
    acc_ref[...] = jnp.zeros_like(acc_ref)

    def accumulate(step):
        first = step * GROUP
        for pair in range(blocks // 2):
            spans = [slice(cb * 8, cb * 8 + 8) for cb in (2 * pair, 2 * pair + 1)]
            msgs = []
            for rows in spans:
                line = []
                for jj in range(GROUP):
                    cols = slice(jj * atoms, (jj + 1) * atoms)
                    line.append(hg_ref[step, rows, cols] * rad_ref[step, rows, cols])
                msgs.append(line)
            for m in range(9):
                if m:
                    at = (m - 1) * entries + first
                    yvs = [y_ref[pl.ds(at + jj, 1), :] for jj in range(GROUP)]
                for rows, line in zip(spans, msgs):
                    if m:
                        terms = [line[jj] * yvs[jj] for jj in range(GROUP)]
                    else:
                        terms = line
                    while len(terms) > 1:
                        terms = [a + b for a, b in zip(terms[::2], terms[1::2])]
                    acc_ref[m, rows, :] += terms[0]

    def body(trip, carry):
        for part in range(2):
            accumulate(2 * trip + part)
        return carry

    lax.fori_loop(0, steps // 2, body, 0)


def layer_two_kernel(
    h0_ref,
    h4_ref,
    acc_ref,
    pair_ref,
    wide_ref,
    occ_ref,
    mix_ref,
    radial_ref,
    rone_ref,
    rhid_ref,
    rout_ref,
    en_ref,
    raw_ref,
    extra_ref,
    gz_ref,
    wz_ref,
    dcat_ref,
):
    channels, atoms = h0_ref.shape
    h4 = h4_ref[...].astype(F32)
    for k in range(NB):
        cols = slice(k * atoms, (k + 1) * atoms)
        wz_ref[:, cols] = (h4 * wide_ref[:, cols]).astype(BF16)
    more = dot(wz_ref[...], pair_ref[...])
    amp = [SPREAD * (acc_ref[m] + more[:, m * atoms : (m + 1) * atoms]) for m in range(9)]
    occ = occ_ref[...].astype(F32)
    own = h0_ref[...].astype(F32)
    h2 = dot(mix_ref[...], invariants(amp), 0, 0) + own
    pre = dot3(rhid_ref[...], h2, 1, 0)
    sig = 1.0 / (1.0 + jnp.exp(-pre))
    rout = columns(rout_ref[...], atoms)
    rone = columns(rone_ref[...], atoms)
    energy = jnp.sum(own * rone, axis=0, keepdims=True)
    energy = energy + jnp.sum(rout * pre * sig, axis=0, keepdims=True)
    en_ref[...] = occ * energy
    dpre = occ * rout * sig * (1.0 + pre * (1.0 - sig))
    dh2 = dot3(rhid_ref[...], dpre, 0, 0)
    dinv = dot_split(mix_ref[...], dh2)
    low = dinv[channels : 2 * channels]
    top = dinv[2 * channels :]
    extra_ref[...] = dh2 + occ * rone
    twice = 2.0 * SPREAD
    for m in range(9):
        value = (twice * amp[m]) * (low if m < 4 else top) if m else SPREAD * dinv[0:channels]
        raw_ref[m] = value
        dcat_ref[:, m * atoms : (m + 1) * atoms] = value.astype(BF16)
    back = dot(pair_ref[...], dcat_ref[...], 1, 1)
    total = None
    for k in range(NB):
        part = radial_ref[k : k + 1, :] * back[k * atoms : (k + 1) * atoms, :]
        total = part if total is None else total + part
    gz_ref[...] = total.astype(BF16)


def reverse_kernel(raw_ref, rad_ref, y_ref, rq_ref, q_ref):
    steps, channels, width = rad_ref.shape
    atoms = width // GROUP
    entries = steps * GROUP
    blocks = channels // 8

    def reverse(step):
        first = step * GROUP
        for pair in range(blocks // 2):
            spans = [slice(cb * 8, cb * 8 + 8) for cb in (2 * pair, 2 * pair + 1)]
            ds = [[raw_ref[m, rows, :] for m in range(9)] for rows in spans]
            for jj in range(GROUP):
                cols = slice(jj * atoms, (jj + 1) * atoms)
                yvs = [y_ref[pl.ds((m - 1) * entries + first + jj, 1), :] for m in range(1, 9)]
                parts = []
                for rows, d in zip(spans, ds):
                    terms = [d[0]] + [yv * dm for yv, dm in zip(yvs, d[1:])]
                    q = terms[0] + terms[1]
                    for a, b in ((2, 3), (4, 5), (6, 7)):
                        q = q + (terms[a] + terms[b])
                    q = q + terms[8]
                    q_ref[step, rows, cols] = q
                    parts.append(rad_ref[step, rows, cols] * q)
                value = jnp.concatenate(parts, axis=0).astype(BF16)
                rq_ref[step, pair * 16 : pair * 16 + 16, cols] = value

    def body(trip, carry):
        for part in range(2):
            reverse(2 * trip + part)
        return carry

    lax.fori_loop(0, steps // 2, body, 0)


def scatter_kernel(first, hot_ref, rq_ref, out_ref):
    size = out_ref.shape[0]
    total = None
    for step in range(hot_ref.shape[0]):
        part = dot(hot_ref[step, first : first + size, :], rq_ref[step], 1, 1)
        total = part if total is None else total + part
    out_ref[...] = total


def edge_kernel(start, hg_ref, rad_ref, slo_ref, q_ref, d_ref, unit_ref, grad_ref, dd_ref):
    channels, atoms = d_ref.shape[1:]
    entries = hg_ref.shape[0] * GROUP
    count = grad_ref.shape[0] // (4 * GROUP)
    for m in range(1, 9):
        if m < 4:
            dd_ref[m] = ROOT3 * d_ref[m]
        else:
            dd_ref[m] = (3.0 * ROOT5 if m == 6 else ROOT15) * d_ref[m]

    def body(step, carry):
        first = step * GROUP
        units = []
        for jj in range(GROUP):
            units.append([unit_ref[pl.ds(i * entries + first + jj, 1), :] for i in range(3)])
        sums = [[None] * 4 for _ in range(GROUP)]
        for cb in range(channels // 8):
            rows = slice(cb * 8, cb * 8 + 8)
            d = [None] + [dd_ref[m, rows, :] for m in range(1, 9)]
            for jj in range(GROUP):
                cols = slice(jj * atoms, (jj + 1) * atoms)
                hg = hg_ref[step, rows, cols]
                vx, vy, vz = units[jj]
                msg = hg * rad_ref[step, rows, cols]
                parts = [
                    msg * ((d[1] + vy * d[4]) + (vz * d[7] + vx * d[8])),
                    msg * ((d[2] + vx * d[4]) + (vz * d[5] - vy * d[8])),
                    msg * ((d[3] + vy * d[5]) + (vx * d[7] + vz * d[6])),
                    hg * q_ref[step, rows, cols] * slo_ref[step, rows, cols],
                ]
                for i in range(4):
                    prior = sums[jj][i]
                    sums[jj][i] = parts[i] if prior is None else prior + parts[i]
        for jj in range(GROUP):
            for i in range(4):
                row = pl.ds(i * count * GROUP + first - start * GROUP + jj, 1)
                grad_ref[row, :] = jnp.sum(sums[jj][i], axis=0, keepdims=True)
        return carry

    lax.fori_loop(start, start + count, body, 0)


def fold_z_kernel(side_ref, gy_ref, az_ref, fz_ref, acc_ref, to_near_ref, to_far_ref):
    size = gy_ref.shape[0]
    quarter = size // 2
    add = dot(onehot(fz_ref[...], 2 * size), az_ref[...])
    acc_ref[...] = add[0:size]
    rows = rounded(gy_ref[...]) + add[size:]
    low, high = rows[0:quarter], rows[quarter:]
    to_near_ref[...] = by_side(side_ref, 1, low, high).astype(BF16)
    to_far_ref[...] = by_side(side_ref, 1, high, low).astype(BF16)


def fold_y_kernel(
    side_ref, acc_ref, gx_ref, extra_ref, near_ref, far_ref, fy_ref, own_ref, to_near_ref, to_far_ref
):
    size = acc_ref.shape[0]
    half = size // 2
    quarter = half // 2
    near, far = near_far(side_ref, 1, fy_ref)
    rows = acc_ref[...] + dot(onehot(near, size), near_ref[...])
    rows = rows + dot(onehot(far, size), far_ref[...])
    own = gx_ref[0:half, :] + jnp.transpose(extra_ref[...])
    own_ref[...] = rows[0:half] + own.astype(BF16).astype(F32)
    ghost = rows[half:] + gx_ref[half:, :].astype(BF16).astype(F32)
    low, high = ghost[0:quarter], ghost[quarter:]
    to_near_ref[...] = by_side(side_ref, 0, low, high).astype(BF16)
    to_far_ref[...] = by_side(side_ref, 0, high, low).astype(BF16)


def layer_one_reverse_kernel(
    side_ref,
    own_ref,
    near_ref,
    far_ref,
    fx_ref,
    amp_ref,
    nbr_ref,
    unit_ref,
    rinv_ref,
    basis_ref,
    slope_ref,
    gb_ref,
    gc_ref,
    lane_ref,
    radial_ref,
    mix_ref,
    f0_ref,
    f1_ref,
    f2_ref,
    f3_ref,
    f4_ref,
    dv_ref,
    sc_ref,
):
    entries, atoms = nbr_ref.shape
    channels = own_ref.shape[1]
    rows = own_ref[...]
    near, far = near_far(side_ref, 0, fx_ref)
    rows = rows + dot(onehot(near, atoms), near_ref[...])
    rows = rows + dot(onehot(far, atoms), far_ref[...])
    cot = jnp.transpose(rows)
    dinv = dot_split(mix_ref[...], cot)
    low = dinv[channels : 2 * channels]
    top = dinv[2 * channels :]
    pieces = [dinv[0:channels]]
    for m in range(1, 9):
        amp = amp_ref[:, m * atoms : (m + 1) * atoms]
        pieces.append(2.0 * amp * (low if m < 4 else top))
    dmom = SPREAD * dot3(radial_ref[...], jnp.concatenate(pieces, axis=1), 1, 0)
    ux = unit_ref[0:entries, :]
    uy = unit_ref[entries : 2 * entries, :]
    uz = unit_ref[2 * entries : 3 * entries, :]
    basis = [basis_ref[k * entries : (k + 1) * entries, :] for k in range(NB)]
    slope = [slope_ref[k * entries : (k + 1) * entries, :] for k in range(NB)]
    angular = harmonics(ux, uy, uz)
    edge = []
    for i in range(4):
        rows = []
        for ref in (gb_ref, gc_ref):
            count = ref.shape[0] // 4
            rows.append(ref[i * count : (i + 1) * count, :])
        edge.append(jnp.concatenate(rows, axis=0))
    dr = edge[3]
    dy = []
    for m in range(9):
        part = None
        sl = None
        for k in range(NB):
            row = dmom[k : k + 1, m * atoms : (m + 1) * atoms]
            sl = slope[k] * row if sl is None else sl + slope[k] * row
            if m:
                part = basis[k] * row if part is None else part + basis[k] * row
        dr = dr + (sl if m == 0 else sl * angular[m])
        dy.append(part)
    wx = edge[0] + ROOT3 * dy[1]
    wx = wx + ROOT15 * (uy * dy[4] + uz * dy[7] + ux * dy[8])
    wy = edge[1] + ROOT3 * dy[2]
    wy = wy + ROOT15 * (ux * dy[4] + uz * dy[5] - uy * dy[8])
    wz = edge[2] + ROOT3 * dy[3]
    wz = wz + ROOT15 * (uy * dy[5] + ux * dy[7]) + (3.0 * ROOT5) * uz * dy[6]
    rinv = rinv_ref[...]
    along = dr - rinv * (ux * wx + uy * wy + uz * wz)
    grads = [wx * rinv + along * ux, wy * rinv + along * uy, wz * rinv + along * uz]
    centre = []
    for i in range(3):
        centre.append(jnp.sum(grads[i], axis=0, keepdims=True))
        top16 = grads[i].astype(BF16).astype(F32)
        dv_ref[i * entries : (i + 1) * entries, :] = top16
        dv_ref[(3 + i) * entries : (4 + i) * entries, :] = grads[i] - top16
    shift = atoms.bit_length() - 1
    total = None
    for step in range(entries // GROUP):
        first = step * GROUP
        block = entry_rows(nbr_ref, first) >> shift
        cols = [dv_ref[pl.ds(first + jj, 6, stride=entries), :] for jj in range(GROUP)]
        value = jnp.concatenate(cols, axis=1)
        value = jnp.concatenate([value, jnp.zeros_like(value[0:2])], axis=0)
        parts = [jnp.where(block == index, value, 0.0) for index in range(5)]
        part = dot(jnp.concatenate(parts, axis=0).astype(BF16), lane_ref[step], 1, 1)
        total = part if total is None else total + part
    sc_ref[...] = total
    zero = jnp.zeros((5, atoms), F32)
    own = jnp.concatenate(centre + [zero], axis=0)
    for index, ref in enumerate((f0_ref, f1_ref, f2_ref, f3_ref, f4_ref)):
        base = index * 8
        value = sc_ref[base : base + 3, :] + sc_ref[base + 3 : base + 6, :]
        value = jnp.concatenate([value, zero], axis=0)
        ref[...] = value - own if index == 0 else value


def scatter_lanes(values, row, size):
    hi = rounded(values)
    mid = rounded(values - hi)
    parts = jnp.concatenate([hi, mid, values - hi - mid], axis=0).astype(BF16)
    out = dot(parts, onehot(row, size), 1, 1)
    rows = values.shape[0]
    return out[0:rows] + out[rows : 2 * rows] + out[2 * rows :]


def force_z_kernel(
    side_ref, f0_ref, f1_ref, f2_ref, f3_ref, az_ref, fz_ref, out_ref, to_near_ref, to_far_ref
):
    atoms = f0_ref.shape[1]
    add = scatter_lanes(az_ref[...], fz_ref[...], 4 * atoms)
    out_ref[:, 0:atoms] = f0_ref[...] + add[:, 0:atoms]
    out_ref[:, atoms : 2 * atoms] = f1_ref[...] + add[:, atoms : 2 * atoms]
    low = f2_ref[...] + add[:, 2 * atoms : 3 * atoms]
    high = f3_ref[...] + add[:, 3 * atoms :]
    to_near_ref[...] = by_side(side_ref, 1, low, high)
    to_far_ref[...] = by_side(side_ref, 1, high, low)


def force_y_kernel(side_ref, acc_ref, near_ref, far_ref, fy_ref, own_ref, ghost_ref):
    size = acc_ref.shape[1]
    rows = acc_ref[...]
    near, far = near_far(side_ref, 1, fy_ref)
    rows = rows + scatter_lanes(near_ref[...], near, size)
    rows = rows + scatter_lanes(far_ref[...], far, size)
    own_ref[...] = rows[:, 0 : size // 2]
    ghost = rows[:, size // 2 :]
    ghost_ref[...] = by_side(side_ref, 0, ghost, half_turn(ghost))


def force_x_kernel(side_ref, own_ref, near_ref, far_ref, fx_ref, en_ref, out_ref, total_ref):
    total_ref[...] = en_ref[...]
    size = own_ref.shape[1]
    both = jnp.where(low_lanes(own_ref.shape), near_ref[...], far_ref[...])
    rows = own_ref[...] + scatter_lanes(both, face_row(side_ref, fx_ref), size)
    for i in range(3):
        out_ref[i] = -rows[i : i + 1]


def call(kernel, outs, *args, scratch=(), vmem=8, aliases={}, cost=1):
    specs = []
    for arg in args:
        specs.append(pl.BlockSpec(memory_space=pltpu.VMEM))
    single = not isinstance(outs, (list, tuple))
    shapes = [outs] if single else list(outs)
    result = pl.pallas_call(
        kernel,
        out_shape=shapes,
        in_specs=specs,
        out_specs=[pl.BlockSpec(memory_space=pltpu.VMEM)] * len(shapes),
        scratch_shapes=list(scratch),
        input_output_aliases=aliases,
        cost_estimate=pl.CostEstimate(
            flops=cost * 10**9, bytes_accessed=cost * 10**6, transcendentals=0
        ),
        compiler_params=pltpu.CompilerParams(vmem_limit_bytes=vmem * 1024 * 1024),
    )(*args)
    return result[0] if single else result


def pair_swap(x, axis, far):
    count = lax.axis_size(axis)
    assert count % 2 == 0
    pairs = []
    for i in range(count):
        up = (i % 2 == 0) != far
        pairs.append((i, (i + (1 if up else -1)) % count))
    return lax.ppermute(x, axis, pairs)


def partner(x):
    axis = "gz"
    return lax.ppermute(x, axis, [(i, i ^ 1) for i in range(lax.axis_size(axis))])


def swap_both(near, far, axis):
    from_far = pair_swap(far, axis, True)
    from_near = pair_swap(near, axis, False)
    return from_near, from_far


def per_device(
    positions,
    occupancy,
    neighbours,
    keep,
    face_x,
    face_y,
    face_z,
    radial_one,
    mix_one,
    embed,
    radial_two,
    mix_two,
    read_one,
    read_hidden,
    read_out,
):
    atoms = positions.shape[-1]
    entries = neighbours.shape[0]
    channels = radial_one.shape[1]
    pos = positions.reshape(3, 1, atoms)
    nbr = neighbours.reshape(entries, atoms)
    kept = keep.reshape(entries, atoms)
    occ = occupancy.reshape(1, atoms)
    fx = face_x.reshape(2, face_x.shape[-1])
    fy = face_y.reshape(2, face_y.shape[-1])
    fz = face_z.reshape(1, face_z.shape[-1])
    embed = embed.reshape(1, channels)
    read_one = read_one.reshape(1, channels)
    read_out = read_out.reshape(1, read_out.shape[0])
    read_hidden = read_hidden.T

    def f32(*shape):
        return jax.ShapeDtypeStruct(shape, F32)

    def b16(*shape):
        return jax.ShapeDtypeStruct(shape, BF16)

    small = f32(8, atoms)
    side = jax.ShapeDtypeStruct((8, atoms), jnp.int32)
    side, pos, sent = call(pos_x_kernel, [side, small, small], pos, fx)
    steps = entries // GROUP
    width = GROUP * atoms
    hot, lanes, count = call(
        hot_kernel,
        [b16(steps, 5 * atoms, width), b16(steps, atoms, width), f32(atoms, atoms)],
        nbr,
        kept,
    )
    near, far = swap_both(sent, sent, "gx")
    p1, near, far = call(pos_y_kernel, [small] * 3, side, pos, near, far, fy)
    near, far = swap_both(near, far, "gy")
    p2, p3, sent = call(pos_z_kernel, [small] * 3, side, pos, p1, near, far, fz)
    pz = partner(sent)

    half = atoms // 2
    square = b16(channels, atoms)
    unit, rinv, basis, slope, amp, h0, near, far, last = call(
        layer_one_kernel,
        [
            f32(3 * entries, atoms),
            f32(entries, atoms),
            f32(NB * entries, atoms),
            f32(NB * entries, atoms),
            f32(channels, 9 * atoms),
            square,
            b16(channels // 2, atoms),
            b16(channels // 2, atoms),
            small,
        ],
        side,
        pos,
        p1,
        p2,
        p3,
        pz,
        nbr,
        kept,
        fx,
        radial_one,
        mix_one,
        embed,
        scratch=[pltpu.VMEM((NB, 9 * atoms), F32)],
    )
    big = f32(steps, channels, width)
    rad, slo, ylm = call(
        radial_kernel,
        [big, big, f32(8 * entries, atoms)],
        basis,
        slope,
        unit,
        radial_two,
        scratch=[pltpu.VMEM((channels, channels), BF16)],
    )
    pairs, wide = call(
        pair_kernel,
        [b16(NB * atoms, 9 * atoms), f32(channels, NB * atoms)],
        pos,
        last,
        count,
        radial_two,
    )
    near, far = swap_both(near, far, "gx")
    h1, near, far = call(feat_y_kernel, [square] * 3, side, h0, near, far, fy)
    table = [pltpu.VMEM((channels, 2 * atoms), BF16)]
    hg = call(gather_first_kernel, big, h0, h1, hot, scratch=table)
    near, far = swap_both(near, far, "gy")
    sent, h2, h3 = call(feat_z_kernel, [square] * 3, side, h0, h1, near, far, fz)
    hg = call(gather_more_kernel, big, h2, h3, hot, hg, scratch=table, aliases={3: 0})
    part = call(partial_kernel, f32(9, channels, atoms), hg, rad, ylm)
    h4 = partner(sent)

    energies, raw, extra, gz = call(
        layer_two_kernel,
        [f32(1, atoms), f32(9, channels, atoms), f32(channels, atoms), b16(atoms, channels)],
        h0,
        h4,
        part,
        pairs,
        wide,
        occ,
        mix_two,
        radial_two,
        read_one,
        read_hidden,
        read_out,
        scratch=[
            pltpu.VMEM((channels, NB * atoms), BF16),
            pltpu.VMEM((channels, 9 * atoms), BF16),
        ],
    )
    rows = f32(2 * atoms, channels)
    rq, quad = call(reverse_kernel, [b16(steps, channels, width), big], raw, rad, ylm)
    gy = call(functools.partial(scatter_kernel, 2 * atoms), rows, hot, rq)
    hg = call(gather_last_kernel, big, h4, hot, hg, aliases={2: 0})
    az = partner(gz)

    def edges(start, count):
        out = f32(4 * count * GROUP, atoms)
        scaled = [pltpu.VMEM((9, channels, atoms), F32)]
        kernel = functools.partial(edge_kernel, start)
        return call(kernel, out, hg, rad, slo, quad, raw, unit, scratch=scaled)

    cut = steps // 7
    acc, near, far = call(
        fold_z_kernel,
        [rows, b16(atoms, channels), b16(atoms, channels)],
        side,
        gy,
        az,
        fz,
    )
    dx = call(functools.partial(scatter_kernel, 0), rows, hot, rq)
    gb = edges(0, cut)
    near, far = swap_both(near, far, "gy")
    own, near, far = call(
        fold_y_kernel,
        [f32(atoms, channels), b16(half, channels), b16(half, channels)],
        side,
        acc,
        dx,
        extra,
        near,
        far,
        fy,
    )
    gc = edges(cut, steps - cut)
    near, far = swap_both(near, far, "gx")
    f0, f1, f2, f3, f4 = call(
        layer_one_reverse_kernel,
        [small] * 5,
        side,
        own,
        near,
        far,
        fx,
        amp,
        nbr,
        unit,
        rinv,
        basis,
        slope,
        gb,
        gc,
        lanes,
        radial_one,
        mix_one,
        scratch=[pltpu.VMEM((6 * entries, atoms), F32), pltpu.VMEM((40, atoms), F32)],
    )
    az = partner(f4)
    acc, near, far = call(
        force_z_kernel, [f32(8, 2 * atoms), small, small], side, f0, f1, f2, f3, az, fz
    )
    near, far = swap_both(near, far, "gy")
    own, ghost = call(force_y_kernel, [small, small], side, acc, near, far, fy)
    near, far = swap_both(ghost, ghost, "gx")
    forces, energies = call(
        force_x_kernel, [f32(3, 1, atoms), f32(1, atoms)], side, own, near, far, fx, energies
    )
    return (energies.reshape(occupancy.shape), forces.reshape(positions.shape))


def solution(mesh):
    return jax.shard_map(
        per_device,
        mesh=mesh,
        in_specs=(
            P(None, "gx", "gy", "gz", None),
            P("gx", "gy", "gz", None),
            P(None, "gx", "gy", "gz", None),
            P(None, "gx", "gy", "gz", None),
            P("gx", "gy", "gz", None, None),
            P("gx", "gy", "gz", None, None),
            P("gx", "gy", "gz", None),
            P(),
            P(),
            P(),
            P(),
            P(),
            P(),
            P(),
            P(),
        ),
        out_specs=(P("gx", "gy", "gz", None), P(None, "gx", "gy", "gz", None)),
        check_vma=False,
    )
```

```python
import functools
import math

import jax
import jax.numpy as jnp
from jax import lax
from jax.experimental import pallas as pl
from jax.experimental.pallas import tpu as pltpu
from jax.sharding import PartitionSpec as P

NB = 8
LX = 4
LY = 4
LZ = 8

SPACING = 1.8
CUTOFF = 5.0
SPREAD = 0.4
F32 = jnp.float32
BF16 = jnp.bfloat16

ROOT3 = 3.0**0.5
ROOT5 = 5.0**0.5
ROOT15 = 15.0**0.5
GROUP = 4


def dot(a, b, ca=1, cb=0, precision=None):
    return lax.dot_general(
        a, b, (((ca,), (cb,)), ((), ())), precision=precision, preferred_element_type=F32
    )


def rounded(x):
    return x.astype(BF16).astype(F32)


def dot3(a, b, ca=1, cb=0):
    a_hi, b_hi = rounded(a), rounded(b)
    left = jnp.concatenate([a_hi, a_hi, a - a_hi], axis=ca).astype(BF16)
    right = jnp.concatenate([b_hi, b - b_hi, b_hi], axis=cb).astype(BF16)
    return dot(left, right, ca, cb)


def dot_split(a, b):
    hi = rounded(b)
    right = jnp.concatenate([hi, b - hi], axis=0).astype(BF16)
    return dot(jnp.concatenate([a, a], axis=1), right)


def columns(row, count):
    hi = rounded(row)
    mid = rounded(row - hi)
    parts = jnp.concatenate([hi, mid, row - hi - mid], axis=0).astype(BF16)
    return dot(parts, jnp.ones((3, count), BF16), 0, 0)


def onehot(row, size):
    count = row.shape[-1]
    ids = lax.broadcasted_iota(jnp.int32, (size, count), 0)
    return jnp.where(ids == row, 1.0, 0.0).astype(BF16)


def lane_pick(blocks, rows):
    width = blocks[0].shape[-1]
    shift = width.bit_length() - 1
    lane = rows & (width - 1)
    block = rows >> shift
    out = jnp.take_along_axis(blocks[0], lane, axis=1)
    for index in range(1, len(blocks)):
        part = jnp.take_along_axis(blocks[index], lane, axis=1)
        out = jnp.where(block == index, part, out)
    return out


def spread_rows(row, count):
    return jnp.broadcast_to(row, (count, row.shape[-1]))


def by_side(side_ref, axis, if_odd, if_even):
    odd = side_ref[axis : axis + 1, 0 : if_odd.shape[1]] == 1
    return jnp.where(odd, if_odd, if_even)


def near_far(side_ref, axis, face_ref):
    low, high = face_ref[0:1, :], face_ref[1:2, :]
    return by_side(side_ref, axis, low, high), by_side(side_ref, axis, high, low)


def face_row(side_ref, fx_ref):
    return jnp.concatenate(near_far(side_ref, 0, fx_ref), axis=1)


def half_turn(x):
    half = x.shape[1] // 2
    return jnp.concatenate([x[:, half:], x[:, :half]], axis=1)


def low_lanes(shape):
    return lax.broadcasted_iota(jnp.int32, shape, 1) < shape[1] // 2


def shift_rows(shape, axis, amount):
    ids = lax.broadcasted_iota(jnp.int32, shape, 0)
    return jnp.where(ids == axis, amount, 0.0)


def side_kernel(side_ref):
    ids = lax.broadcasted_iota(jnp.int32, side_ref.shape, 0)
    first, second = lax.axis_index("gx") % 2, lax.axis_index("gy") % 2
    value = jnp.where(ids == 0, first, jnp.where(ids == 1, second, lax.axis_index("gz")))
    side_ref[...] = value


def pos_x_kernel(side_ref, pos_ref, fx_ref, coords_ref, send_ref):
    rows = [pos_ref[i] for i in range(3)]
    coords = jnp.concatenate(rows + [jnp.zeros_like(rows[0])] * 5, axis=0)
    coords_ref[...] = coords
    send_ref[...] = lane_pick([coords], spread_rows(face_row(side_ref, fx_ref), 8))


def pos_y_kernel(side_ref, pos_ref, near_ref, far_ref, fy_ref, p1_ref, to_near_ref, to_far_ref):
    coords = pos_ref[...]
    shape = coords.shape
    first = low_lanes(shape)
    both = jnp.where(first, near_ref[...], far_ref[...])
    both = by_side(side_ref, 0, both, half_turn(both))
    step = shift_rows(shape, 0, LX * SPACING)
    ghost = jnp.where(first, both - step, both + step)
    p1_ref[...] = ghost
    near, far = near_far(side_ref, 1, fy_ref)
    to_near_ref[...] = lane_pick([coords, ghost], spread_rows(near, 8))
    to_far_ref[...] = lane_pick([coords, ghost], spread_rows(far, 8))


def pos_z_kernel(side_ref, pos_ref, p1_ref, near_ref, far_ref, fz_ref, p2_ref, p3_ref, out_ref):
    coords = pos_ref[...]
    shape = coords.shape
    near, far = near_ref[...], far_ref[...]
    low = by_side(side_ref, 1, near, far) - shift_rows(shape, 1, LY * SPACING)
    high = by_side(side_ref, 1, far, near) + shift_rows(shape, 1, LY * SPACING)
    p2_ref[...] = low
    p3_ref[...] = high
    out_ref[...] = lane_pick([coords, p1_ref[...], low, high], spread_rows(fz_ref[...], 8))


def layer_one_kernel(
    side_ref,
    pos_ref,
    p1_ref,
    p2_ref,
    p3_ref,
    pz_ref,
    nbr_ref,
    keep_ref,
    fx_ref,
    radial_ref,
    mix_ref,
    embed_ref,
    unit_ref,
    rinv_ref,
    basis_ref,
    slope_ref,
    amp_ref,
    h0_ref,
    to_near_ref,
    to_far_ref,
    last_ref,
    mom_ref,
):
    entries, atoms = nbr_ref.shape
    nbr = nbr_ref[...]
    lane = nbr & (atoms - 1)
    block = nbr >> (atoms.bit_length() - 1)
    rise = jnp.where(side_ref[2:3, :] == 0, LZ * SPACING, -LZ * SPACING)
    last = pz_ref[...] + shift_rows(pz_ref.shape, 2, rise)
    last_ref[...] = last
    tables = [pos_ref[...], p1_ref[...], p2_ref[...], p3_ref[...], last]
    vec = []
    for axis in range(3):
        got = None
        for index, table in enumerate(tables):
            spread = spread_rows(table[axis : axis + 1, :], entries)
            part = jnp.take_along_axis(spread, lane, axis=1)
            got = part if index == 0 else jnp.where(block == index, part, got)
        vec.append(got - pos_ref[axis : axis + 1, :])
    r_sq = vec[0] * vec[0] + vec[1] * vec[1] + vec[2] * vec[2]
    dist = jnp.sqrt(r_sq)
    rinv = 1.0 / dist
    ux, uy, uz = (v * rinv for v in vec)
    rinv_ref[...] = rinv
    unit_ref[0:entries, :] = ux
    unit_ref[entries : 2 * entries, :] = uy
    unit_ref[2 * entries : 3 * entries, :] = uz
    basis, slopes = radial_parts(dist, rinv, keep_ref[...].astype(F32), True)
    for k in range(NB):
        basis_ref[k * entries : (k + 1) * entries, :] = basis[k]
        slope_ref[k * entries : (k + 1) * entries, :] = slopes[k]
    angular = harmonics(ux, uy, uz)
    for m in range(9):
        for k in range(NB):
            prod = basis[k] if m == 0 else basis[k] * angular[m]
            mom_ref[k : k + 1, m * atoms : (m + 1) * atoms] = jnp.sum(prod, axis=0, keepdims=True)
    amp = SPREAD * dot3(radial_ref[...], mom_ref[...], 0, 0)
    amp_ref[...] = amp
    inv = invariants([amp[:, m * atoms : (m + 1) * atoms] for m in range(9)])
    h1 = dot(mix_ref[...], inv, 0, 0)
    h1 = h1 + columns(embed_ref[...], atoms)
    h1b = h1.astype(BF16)
    h0_ref[...] = h1b
    both = dot(h1b, onehot(face_row(side_ref, fx_ref), atoms))
    to_near_ref[...], to_far_ref[...] = pack_halves(both)


def sine_cosine(turn):
    angle = (turn - 0.5) * math.pi
    sq = angle * angle
    even = jnp.full_like(sq, 1.0 / math.factorial(12))
    odd = jnp.full_like(sq, 1.0 / math.factorial(13))
    for order in range(5, -1, -1):
        sign = 1.0 if order % 2 == 0 else -1.0
        even = even * sq + sign / math.factorial(2 * order)
        odd = odd * sq + sign / math.factorial(2 * order + 1)
    return even, -(angle * odd)


def radial_parts(dist, rinv, weight, with_slope):
    scaled = jnp.minimum(dist * (1.0 / CUTOFF), 1.0)
    sine, cosine = sine_cosine(scaled)
    inner = 1.0 - scaled * scaled
    weight = weight * (2.0 / CUTOFF) ** 0.5
    env = weight * inner * inner * rinv
    env_slope = -env * rinv - weight * rinv * (4.0 / CUTOFF) * scaled * inner
    twice = 2.0 * cosine
    s_prev, s_now = jnp.zeros_like(sine), sine
    c_prev, c_now = jnp.ones_like(cosine), cosine
    basis, slopes = [], []
    for k in range(NB):
        basis.append(s_now * env)
        if with_slope:
            slopes.append(c_now * env * ((k + 1) * math.pi / CUTOFF) + s_now * env_slope)
            c_prev, c_now = c_now, twice * c_now - c_prev
        s_prev, s_now = s_now, twice * s_now - s_prev
    return basis, slopes


def harmonics(ux, uy, uz):
    return [
        None,
        ROOT3 * ux,
        ROOT3 * uy,
        ROOT3 * uz,
        ROOT15 * ux * uy,
        ROOT15 * uy * uz,
        0.5 * ROOT5 * (3.0 * uz * uz - 1.0),
        ROOT15 * ux * uz,
        0.5 * ROOT15 * (ux * ux - uy * uy),
    ]


def invariants(amp):
    first = amp[1] * amp[1] + amp[2] * amp[2] + amp[3] * amp[3]
    second = amp[4] * amp[4] + amp[5] * amp[5] + amp[6] * amp[6]
    second = second + amp[7] * amp[7] + amp[8] * amp[8]
    return jnp.concatenate([amp[0], first, second], axis=0).astype(BF16)


def pack_halves(both):
    rows, _ = both.shape
    top, low = both[0 : rows // 2], both[rows // 2 :]
    first = low_lanes(top.shape)
    near = jnp.where(first, top, half_turn(low))
    far = jnp.where(first, half_turn(top), low)
    return near.astype(BF16), far.astype(BF16)


def unpack_halves(low, high):
    first = low_lanes(low.shape)
    top = jnp.where(first, low, half_turn(high))
    bottom = jnp.where(first, half_turn(low), high)
    return jnp.concatenate([top, bottom], axis=0)


def feat_y_kernel(side_ref, h0_ref, near_ref, far_ref, fy_ref, h1_ref, to_near_ref, to_far_ref):
    near, far = near_ref[...].astype(F32), far_ref[...].astype(F32)
    low, high = by_side(side_ref, 0, near, far), by_side(side_ref, 0, far, near)
    ghost = unpack_halves(low, high).astype(BF16)
    h1_ref[...] = ghost
    table = jnp.concatenate([h0_ref[...], ghost], axis=1)
    size = table.shape[1]
    near, far = near_far(side_ref, 1, fy_ref)
    to_near_ref[...] = dot(table, onehot(near, size)).astype(BF16)
    to_far_ref[...] = dot(table, onehot(far, size)).astype(BF16)


def sides(side_ref, axis, near_ref, far_ref):
    near, far = near_ref[...].astype(F32), far_ref[...].astype(F32)
    low, high = by_side(side_ref, axis, near, far), by_side(side_ref, axis, far, near)
    return low.astype(BF16), high.astype(BF16)


def feat_z_kernel(side_ref, h0_ref, h1_ref, near_ref, far_ref, fz_ref, out_ref, h2_ref, h3_ref):
    low, high = sides(side_ref, 1, near_ref, far_ref)
    h2_ref[...] = low
    h3_ref[...] = high
    table = jnp.concatenate([h0_ref[...], h1_ref[...], low, high], axis=1)
    out_ref[...] = dot(table, onehot(fz_ref[...], table.shape[1])).astype(BF16)


def entry_rows(ref, first):
    return jnp.concatenate([ref[pl.ds(first + jj, 1), :] for jj in range(GROUP)], axis=1)


def hot_kernel(nbr_ref, keep_ref, hot_ref, lane_ref, count_ref):
    atoms = nbr_ref.shape[1]
    count_ref[...] = jnp.zeros_like(count_ref)
    ids = lax.broadcasted_iota(jnp.int32, (atoms, atoms), 0) + 4 * atoms

    def body(step, carry):
        first = step * GROUP
        row = entry_rows(nbr_ref, first)
        hot_ref[step] = onehot(row, hot_ref.shape[1])
        lane_ref[step] = onehot(row & (atoms - 1), atoms)
        count = count_ref[...]
        for jj in range(GROUP):
            at = pl.ds(first + jj, 1)
            count = count + jnp.where(ids == nbr_ref[at, :], keep_ref[at, :].astype(F32), 0.0)
        count_ref[...] = count
        return carry

    lax.fori_loop(0, hot_ref.shape[0], body, 0)


def pair_kernel(pos_ref, last_ref, count_ref, radial_ref, pair_ref, wide_ref):
    atoms = pos_ref.shape[1]
    weight = count_ref[...]
    vec = []
    for axis in range(3):
        vec.append(columns(last_ref[axis : axis + 1, :], atoms) - pos_ref[axis : axis + 1, :])
    r_sq = vec[0] * vec[0] + vec[1] * vec[1] + vec[2] * vec[2]
    dist = jnp.sqrt(jnp.where(weight > 0.0, r_sq, 1.0))
    rinv = 1.0 / dist
    basis, _ = radial_parts(dist, rinv, weight, False)
    angular = harmonics(*(v * rinv for v in vec))
    for k in range(NB):
        wide_ref[:, k * atoms : (k + 1) * atoms] = columns(radial_ref[k : k + 1, :], atoms)
        for m in range(9):
            value = basis[k] if m == 0 else basis[k] * angular[m]
            pair_ref[k * atoms : (k + 1) * atoms, m * atoms : (m + 1) * atoms] = value.astype(BF16)


def stack3(hi, lo):
    return jnp.concatenate([hi, lo, hi], axis=0).astype(BF16)


def radial_kernel(basis_ref, slope_ref, unit_ref, radial_ref, rad_ref, slo_ref, y_ref, rts_ref):
    entries = basis_ref.shape[0] // NB
    channels = radial_ref.shape[1]
    rt = radial_ref[...]
    hi = rt.astype(BF16).astype(F32)
    lo = rt - hi
    pad = jnp.zeros((channels - 3 * NB, channels), F32)
    rts_ref[...] = jnp.transpose(jnp.concatenate([hi, hi, lo, pad], axis=0)).astype(BF16)
    ux = unit_ref[0:entries, :]
    uy = unit_ref[entries : 2 * entries, :]
    uz = unit_ref[2 * entries : 3 * entries, :]
    for m, val in enumerate(harmonics(ux, uy, uz)):
        if m:
            y_ref[(m - 1) * entries : m * entries, :] = val

    def radial_cols(ref, first):
        cols = [ref[pl.ds(first + jj, NB, stride=entries), :] for jj in range(GROUP)]
        value = jnp.concatenate(cols, axis=1)
        top = value.astype(BF16).astype(F32)
        return stack3(top, value - top)

    rts = rts_ref[:, 0 : 3 * NB]
    for step in range(rad_ref.shape[0]):
        rad_ref[step] = dot(rts, radial_cols(basis_ref, step * GROUP))
        slo_ref[step] = dot(rts, radial_cols(slope_ref, step * GROUP))


def gather_first_kernel(h0_ref, h1_ref, hot_ref, hg_ref, table_ref):
    atoms = h0_ref.shape[1]
    table_ref[:, 0:atoms] = h0_ref[...]
    table_ref[:, atoms:] = h1_ref[...]

    for step in range(hot_ref.shape[0]):
        hg_ref[step] = dot(table_ref[...], hot_ref[step, 0 : 2 * atoms, :])


def gather_more_kernel(h2_ref, h3_ref, hot_ref, old_ref, hg_ref, table_ref):
    atoms = h2_ref.shape[1]
    table_ref[:, 0:atoms] = h2_ref[...]
    table_ref[:, atoms:] = h3_ref[...]

    for step in range(hot_ref.shape[0]):
        more = dot(table_ref[...], hot_ref[step, 2 * atoms : 4 * atoms, :])
        hg_ref[step] = old_ref[step] + more


def partial_kernel(hg_ref, rad_ref, y_ref, acc_ref):
    steps, channels, width = hg_ref.shape
    atoms = width // GROUP
    entries = steps * GROUP
    blocks = channels // 8
    acc_ref[...] = jnp.zeros_like(acc_ref)

    def accumulate(step):
        first = step * GROUP
        for pair in range(blocks // 2):
            spans = [slice(cb * 8, cb * 8 + 8) for cb in (2 * pair, 2 * pair + 1)]
            msgs = []
            for rows in spans:
                line = []
                for jj in range(GROUP):
                    cols = slice(jj * atoms, (jj + 1) * atoms)
                    line.append(hg_ref[step, rows, cols] * rad_ref[step, rows, cols])
                msgs.append(line)
            for m in range(9):
                if m:
                    at = (m - 1) * entries + first
                    yvs = [y_ref[pl.ds(at + jj, 1), :] for jj in range(GROUP)]
                for rows, line in zip(spans, msgs):
                    if m:
                        terms = [line[jj] * yvs[jj] for jj in range(GROUP)]
                    else:
                        terms = line
                    while len(terms) > 1:
                        terms = [a + b for a, b in zip(terms[::2], terms[1::2])]
                    acc_ref[m, rows, :] += terms[0]

    def body(trip, carry):
        for part in range(2):
            accumulate(2 * trip + part)
        return carry

    lax.fori_loop(0, steps // 2, body, 0)


def layer_two_kernel(
    h0_ref,
    h4_ref,
    acc_ref,
    pair_ref,
    wide_ref,
    occ_ref,
    mix_ref,
    radial_ref,
    rone_ref,
    rhid_ref,
    rout_ref,
    en_ref,
    raw_ref,
    extra_ref,
    gz_ref,
    wz_ref,
    dcat_ref,
):
    channels, atoms = h0_ref.shape
    h4 = h4_ref[...].astype(F32)
    for k in range(NB):
        cols = slice(k * atoms, (k + 1) * atoms)
        wz_ref[:, cols] = (h4 * wide_ref[:, cols]).astype(BF16)
    more = dot(wz_ref[...], pair_ref[...])
    amp = [SPREAD * (acc_ref[m] + more[:, m * atoms : (m + 1) * atoms]) for m in range(9)]
    occ = occ_ref[...].astype(F32)
    own = h0_ref[...].astype(F32)
    h2 = dot(mix_ref[...], invariants(amp), 0, 0) + own
    pre = dot3(rhid_ref[...], h2, 1, 0)
    sig = 1.0 / (1.0 + jnp.exp(-pre))
    rout = columns(rout_ref[...], atoms)
    rone = columns(rone_ref[...], atoms)
    energy = jnp.sum(own * rone, axis=0, keepdims=True)
    energy = energy + jnp.sum(rout * pre * sig, axis=0, keepdims=True)
    en_ref[...] = occ * energy
    dpre = occ * rout * sig * (1.0 + pre * (1.0 - sig))
    dh2 = dot3(rhid_ref[...], dpre, 0, 0)
    dinv = dot_split(mix_ref[...], dh2)
    low = dinv[channels : 2 * channels]
    top = dinv[2 * channels :]
    extra_ref[...] = dh2 + occ * rone
    twice = 2.0 * SPREAD
    for m in range(9):
        value = (twice * amp[m]) * (low if m < 4 else top) if m else SPREAD * dinv[0:channels]
        raw_ref[m] = value
        dcat_ref[:, m * atoms : (m + 1) * atoms] = value.astype(BF16)
    back = dot(pair_ref[...], dcat_ref[...], 1, 1)
    total = None
    for k in range(NB):
        part = radial_ref[k : k + 1, :] * back[k * atoms : (k + 1) * atoms, :]
        total = part if total is None else total + part
    gz_ref[...] = total.astype(BF16)


def reverse_kernel(raw_ref, rad_ref, y_ref, hot_ref, rq_ref, q_ref, gy_ref):
    steps, channels, width = rad_ref.shape
    atoms = width // GROUP
    entries = steps * GROUP
    blocks = channels // 8

    def reverse(step):
        first = step * GROUP
        for pair in range(blocks // 2):
            spans = [slice(cb * 8, cb * 8 + 8) for cb in (2 * pair, 2 * pair + 1)]
            ds = [[raw_ref[m, rows, :] for m in range(9)] for rows in spans]
            for jj in range(GROUP):
                cols = slice(jj * atoms, (jj + 1) * atoms)
                yvs = [y_ref[pl.ds((m - 1) * entries + first + jj, 1), :] for m in range(1, 9)]
                parts = []
                for rows, d in zip(spans, ds):
                    terms = [d[0]] + [yv * dm for yv, dm in zip(yvs, d[1:])]
                    q = terms[0] + terms[1]
                    for a, b in ((2, 3), (4, 5), (6, 7)):
                        q = q + (terms[a] + terms[b])
                    q = q + terms[8]
                    q_ref[step, rows, cols] = q
                    parts.append(rad_ref[step, rows, cols] * q)
                value = jnp.concatenate(parts, axis=0).astype(BF16)
                rq_ref[step, pair * 16 : pair * 16 + 16, cols] = value

    def scatter(step):
        parts = []
        for at in (step, step + 1):
            parts.append(dot(hot_ref[at, 2 * atoms : 4 * atoms, :], rq_ref[at], 1, 1))
        return parts[0] + parts[1]

    gy_ref[...] = jnp.zeros_like(gy_ref)
    reverse(0)
    reverse(1)

    def body(trip, carry):
        gy_ref[...] += scatter(2 * trip)
        for part in range(2):
            reverse(2 * trip + 2 + part)
        return carry

    lax.fori_loop(0, steps // 2 - 1, body, 0)
    gy_ref[...] += scatter(steps - 2)


def scatter_kernel(first, hot_ref, rq_ref, out_ref):
    size = out_ref.shape[0]
    total = None
    for step in range(hot_ref.shape[0]):
        part = dot(hot_ref[step, first : first + size, :], rq_ref[step], 1, 1)
        total = part if total is None else total + part
    out_ref[...] = total


def edge_kernel(
    start,
    h4_ref,
    hot_ref,
    old_ref,
    rad_ref,
    slo_ref,
    q_ref,
    d_ref,
    unit_ref,
    grad_ref,
    dd_ref,
    hg_ref,
):
    channels, atoms = d_ref.shape[1:]
    steps = old_ref.shape[0]
    entries = steps * GROUP
    count = grad_ref.shape[0] // (4 * GROUP)
    for m in range(1, 9):
        if m < 4:
            dd_ref[m] = ROOT3 * d_ref[m]
        else:
            dd_ref[m] = (3.0 * ROOT5 if m == 6 else ROOT15) * d_ref[m]

    def prepare(step, slot):
        hg_ref[slot] = old_ref[step] + dot(h4_ref[...], hot_ref[step, 4 * atoms :, :])

    def edges(step, slot):
        first = step * GROUP
        units = []
        for jj in range(GROUP):
            units.append([unit_ref[pl.ds(i * entries + first + jj, 1), :] for i in range(3)])
        sums = [[None] * 4 for _ in range(GROUP)]
        for cb in range(channels // 8):
            rows = slice(cb * 8, cb * 8 + 8)
            d = [None] + [dd_ref[m, rows, :] for m in range(1, 9)]
            for jj in range(GROUP):
                cols = slice(jj * atoms, (jj + 1) * atoms)
                hg = hg_ref[slot, rows, cols]
                vx, vy, vz = units[jj]
                msg = hg * rad_ref[step, rows, cols]
                parts = [
                    msg * ((d[1] + vy * d[4]) + (vz * d[7] + vx * d[8])),
                    msg * ((d[2] + vx * d[4]) + (vz * d[5] - vy * d[8])),
                    msg * ((d[3] + vy * d[5]) + (vx * d[7] + vz * d[6])),
                    hg * q_ref[step, rows, cols] * slo_ref[step, rows, cols],
                ]
                for i in range(4):
                    prior = sums[jj][i]
                    sums[jj][i] = parts[i] if prior is None else prior + parts[i]
        for jj in range(GROUP):
            for i in range(4):
                row = pl.ds(i * count * GROUP + first - start * GROUP + jj, 1)
                grad_ref[row, :] = jnp.sum(sums[jj][i], axis=0, keepdims=True)

    prepare(start, 0)
    prepare(start + 1, 1)

    def body(trip, carry):
        step = start + 2 * trip
        for part in range(2):
            edges(step + part, part)
        for part in range(2):
            prepare(jnp.minimum(step + 2 + part, steps - 1), part)
        return carry

    lax.fori_loop(0, count // 2, body, 0)


def fold_z_kernel(side_ref, gy_ref, az_ref, fz_ref, acc_ref, to_near_ref, to_far_ref):
    size = gy_ref.shape[0]
    quarter = size // 2
    add = dot(onehot(fz_ref[...], 2 * size), az_ref[...])
    acc_ref[...] = add[0:size]
    rows = rounded(gy_ref[...]) + add[size:]
    low, high = rows[0:quarter], rows[quarter:]
    to_near_ref[...] = by_side(side_ref, 1, low, high).astype(BF16)
    to_far_ref[...] = by_side(side_ref, 1, high, low).astype(BF16)


def fold_y_kernel(
    side_ref, acc_ref, gx_ref, extra_ref, near_ref, far_ref, fy_ref, own_ref, to_near_ref, to_far_ref
):
    size = acc_ref.shape[0]
    half = size // 2
    quarter = half // 2
    near, far = near_far(side_ref, 1, fy_ref)
    rows = acc_ref[...] + dot(onehot(near, size), near_ref[...])
    rows = rows + dot(onehot(far, size), far_ref[...])
    own = gx_ref[0:half, :] + jnp.transpose(extra_ref[...])
    own_ref[...] = rows[0:half] + own.astype(BF16).astype(F32)
    ghost = rows[half:] + gx_ref[half:, :].astype(BF16).astype(F32)
    low, high = ghost[0:quarter], ghost[quarter:]
    to_near_ref[...] = by_side(side_ref, 0, low, high).astype(BF16)
    to_far_ref[...] = by_side(side_ref, 0, high, low).astype(BF16)


def layer_one_reverse_kernel(
    side_ref,
    own_ref,
    near_ref,
    far_ref,
    fx_ref,
    amp_ref,
    nbr_ref,
    unit_ref,
    rinv_ref,
    basis_ref,
    slope_ref,
    gb_ref,
    gc_ref,
    lane_ref,
    radial_ref,
    mix_ref,
    f0_ref,
    f1_ref,
    f2_ref,
    f3_ref,
    f4_ref,
    dv_ref,
    sc_ref,
):
    entries, atoms = nbr_ref.shape
    channels = own_ref.shape[1]
    rows = own_ref[...]
    near, far = near_far(side_ref, 0, fx_ref)
    rows = rows + dot(onehot(near, atoms), near_ref[...])
    rows = rows + dot(onehot(far, atoms), far_ref[...])
    cot = jnp.transpose(rows)
    dinv = dot_split(mix_ref[...], cot)
    low = dinv[channels : 2 * channels]
    top = dinv[2 * channels :]
    pieces = [dinv[0:channels]]
    for m in range(1, 9):
        amp = amp_ref[:, m * atoms : (m + 1) * atoms]
        pieces.append(2.0 * amp * (low if m < 4 else top))
    dmom = SPREAD * dot3(radial_ref[...], jnp.concatenate(pieces, axis=1), 1, 0)
    ux = unit_ref[0:entries, :]
    uy = unit_ref[entries : 2 * entries, :]
    uz = unit_ref[2 * entries : 3 * entries, :]
    basis = [basis_ref[k * entries : (k + 1) * entries, :] for k in range(NB)]
    slope = [slope_ref[k * entries : (k + 1) * entries, :] for k in range(NB)]
    angular = harmonics(ux, uy, uz)
    edge = []
    for i in range(4):
        rows = []
        for ref in (gb_ref, gc_ref):
            count = ref.shape[0] // 4
            rows.append(ref[i * count : (i + 1) * count, :])
        edge.append(jnp.concatenate(rows, axis=0))
    dr = edge[3]
    dy = []
    for m in range(9):
        part = None
        sl = None
        for k in range(NB):
            row = dmom[k : k + 1, m * atoms : (m + 1) * atoms]
            sl = slope[k] * row if sl is None else sl + slope[k] * row
            if m:
                part = basis[k] * row if part is None else part + basis[k] * row
        dr = dr + (sl if m == 0 else sl * angular[m])
        dy.append(part)
    wx = edge[0] + ROOT3 * dy[1]
    wx = wx + ROOT15 * (uy * dy[4] + uz * dy[7] + ux * dy[8])
    wy = edge[1] + ROOT3 * dy[2]
    wy = wy + ROOT15 * (ux * dy[4] + uz * dy[5] - uy * dy[8])
    wz = edge[2] + ROOT3 * dy[3]
    wz = wz + ROOT15 * (uy * dy[5] + ux * dy[7]) + (3.0 * ROOT5) * uz * dy[6]
    rinv = rinv_ref[...]
    along = dr - rinv * (ux * wx + uy * wy + uz * wz)
    grads = [wx * rinv + along * ux, wy * rinv + along * uy, wz * rinv + along * uz]
    centre = []
    for i in range(3):
        centre.append(jnp.sum(grads[i], axis=0, keepdims=True))
        top16 = grads[i].astype(BF16).astype(F32)
        dv_ref[i * entries : (i + 1) * entries, :] = top16
        dv_ref[(3 + i) * entries : (4 + i) * entries, :] = grads[i] - top16
    shift = atoms.bit_length() - 1
    total = None
    for step in range(entries // GROUP):
        first = step * GROUP
        block = entry_rows(nbr_ref, first) >> shift
        cols = [dv_ref[pl.ds(first + jj, 6, stride=entries), :] for jj in range(GROUP)]
        value = jnp.concatenate(cols, axis=1)
        value = jnp.concatenate([value, jnp.zeros_like(value[0:2])], axis=0)
        parts = [jnp.where(block == index, value, 0.0) for index in range(5)]
        part = dot(jnp.concatenate(parts, axis=0).astype(BF16), lane_ref[step], 1, 1)
        total = part if total is None else total + part
    sc_ref[...] = total
    zero = jnp.zeros((5, atoms), F32)
    own = jnp.concatenate(centre + [zero], axis=0)
    for index, ref in enumerate((f0_ref, f1_ref, f2_ref, f3_ref, f4_ref)):
        base = index * 8
        value = sc_ref[base : base + 3, :] + sc_ref[base + 3 : base + 6, :]
        value = jnp.concatenate([value, zero], axis=0)
        ref[...] = value - own if index == 0 else value


def scatter_lanes(values, row, size):
    hi = rounded(values)
    mid = rounded(values - hi)
    parts = jnp.concatenate([hi, mid, values - hi - mid], axis=0).astype(BF16)
    out = dot(parts, onehot(row, size), 1, 1)
    rows = values.shape[0]
    return out[0:rows] + out[rows : 2 * rows] + out[2 * rows :]


def force_z_kernel(
    side_ref, f0_ref, f1_ref, f2_ref, f3_ref, az_ref, fz_ref, out_ref, to_near_ref, to_far_ref
):
    atoms = f0_ref.shape[1]
    add = scatter_lanes(az_ref[...], fz_ref[...], 4 * atoms)
    out_ref[:, 0:atoms] = f0_ref[...] + add[:, 0:atoms]
    out_ref[:, atoms : 2 * atoms] = f1_ref[...] + add[:, atoms : 2 * atoms]
    low = f2_ref[...] + add[:, 2 * atoms : 3 * atoms]
    high = f3_ref[...] + add[:, 3 * atoms :]
    to_near_ref[...] = by_side(side_ref, 1, low, high)
    to_far_ref[...] = by_side(side_ref, 1, high, low)


def force_y_kernel(side_ref, acc_ref, near_ref, far_ref, fy_ref, own_ref, ghost_ref):
    size = acc_ref.shape[1]
    rows = acc_ref[...]
    near, far = near_far(side_ref, 1, fy_ref)
    rows = rows + scatter_lanes(near_ref[...], near, size)
    rows = rows + scatter_lanes(far_ref[...], far, size)
    own_ref[...] = rows[:, 0 : size // 2]
    ghost = rows[:, size // 2 :]
    ghost_ref[...] = by_side(side_ref, 0, ghost, half_turn(ghost))


def force_x_kernel(side_ref, own_ref, near_ref, far_ref, fx_ref, en_ref, out_ref, total_ref):
    total_ref[...] = en_ref[...]
    size = own_ref.shape[1]
    both = jnp.where(low_lanes(own_ref.shape), near_ref[...], far_ref[...])
    rows = own_ref[...] + scatter_lanes(both, face_row(side_ref, fx_ref), size)
    for i in range(3):
        out_ref[i] = -rows[i : i + 1]


def call(kernel, outs, *args, scratch=(), vmem=8, aliases={}, cost=1):
    specs = []
    for arg in args:
        specs.append(pl.BlockSpec(memory_space=pltpu.VMEM))
    single = not isinstance(outs, (list, tuple))
    shapes = [outs] if single else list(outs)
    result = pl.pallas_call(
        kernel,
        out_shape=shapes,
        in_specs=specs,
        out_specs=[pl.BlockSpec(memory_space=pltpu.VMEM)] * len(shapes),
        scratch_shapes=list(scratch),
        input_output_aliases=aliases,
        cost_estimate=pl.CostEstimate(
            flops=cost * 10**9, bytes_accessed=cost * 10**6, transcendentals=0
        ),
        compiler_params=pltpu.CompilerParams(vmem_limit_bytes=vmem * 1024 * 1024),
    )(*args)
    return result[0] if single else result


def pair_swap(x, axis, far):
    count = lax.axis_size(axis)
    assert count % 2 == 0
    pairs = []
    for i in range(count):
        up = (i % 2 == 0) != far
        pairs.append((i, (i + (1 if up else -1)) % count))
    return lax.ppermute(x, axis, pairs)


def partner(x):
    axis = "gz"
    return lax.ppermute(x, axis, [(i, i ^ 1) for i in range(lax.axis_size(axis))])


def swap_both(near, far, axis):
    from_far = pair_swap(far, axis, True)
    from_near = pair_swap(near, axis, False)
    return from_near, from_far


def per_device(
    positions,
    occupancy,
    neighbours,
    keep,
    face_x,
    face_y,
    face_z,
    radial_one,
    mix_one,
    embed,
    radial_two,
    mix_two,
    read_one,
    read_hidden,
    read_out,
):
    atoms = positions.shape[-1]
    entries = neighbours.shape[0]
    channels = radial_one.shape[1]
    pos = positions.reshape(3, 1, atoms)
    nbr = neighbours.reshape(entries, atoms)
    kept = keep.reshape(entries, atoms)
    occ = occupancy.reshape(1, atoms)
    fx = face_x.reshape(2, face_x.shape[-1])
    fy = face_y.reshape(2, face_y.shape[-1])
    fz = face_z.reshape(1, face_z.shape[-1])
    embed = embed.reshape(1, channels)
    read_one = read_one.reshape(1, channels)
    read_out = read_out.reshape(1, read_out.shape[0])
    read_hidden = read_hidden.T

    def f32(*shape):
        return jax.ShapeDtypeStruct(shape, F32)

    def b16(*shape):
        return jax.ShapeDtypeStruct(shape, BF16)

    small = f32(8, atoms)
    side = jax.ShapeDtypeStruct((8, atoms), jnp.int32)
    side = call(side_kernel, side)
    pos, sent = call(pos_x_kernel, [small, small], side, pos, fx)
    steps = entries // GROUP
    width = GROUP * atoms
    hot, lanes, count = call(
        hot_kernel,
        [b16(steps, 5 * atoms, width), b16(steps, atoms, width), f32(atoms, atoms)],
        nbr,
        kept,
    )
    near, far = swap_both(sent, sent, "gx")
    p1, near, far = call(pos_y_kernel, [small] * 3, side, pos, near, far, fy)
    near, far = swap_both(near, far, "gy")
    p2, p3, sent = call(pos_z_kernel, [small] * 3, side, pos, p1, near, far, fz)
    pz = partner(sent)

    half = atoms // 2
    square = b16(channels, atoms)
    unit, rinv, basis, slope, amp, h0, near, far, last = call(
        layer_one_kernel,
        [
            f32(3 * entries, atoms),
            f32(entries, atoms),
            f32(NB * entries, atoms),
            f32(NB * entries, atoms),
            f32(channels, 9 * atoms),
            square,
            b16(channels // 2, atoms),
            b16(channels // 2, atoms),
            small,
        ],
        side,
        pos,
        p1,
        p2,
        p3,
        pz,
        nbr,
        kept,
        fx,
        radial_one,
        mix_one,
        embed,
        scratch=[pltpu.VMEM((NB, 9 * atoms), F32)],
    )
    big = f32(steps, channels, width)
    rad, slo, ylm = call(
        radial_kernel,
        [big, big, f32(8 * entries, atoms)],
        basis,
        slope,
        unit,
        radial_two,
        scratch=[pltpu.VMEM((channels, channels), BF16)],
    )
    pairs, wide = call(
        pair_kernel,
        [b16(NB * atoms, 9 * atoms), f32(channels, NB * atoms)],
        pos,
        last,
        count,
        radial_two,
    )
    near, far = swap_both(near, far, "gx")
    h1, near, far = call(feat_y_kernel, [square] * 3, side, h0, near, far, fy)
    table = [pltpu.VMEM((channels, 2 * atoms), BF16)]
    hg = call(gather_first_kernel, big, h0, h1, hot, scratch=table)
    near, far = swap_both(near, far, "gy")
    sent, h2, h3 = call(feat_z_kernel, [square] * 3, side, h0, h1, near, far, fz)
    hg = call(gather_more_kernel, big, h2, h3, hot, hg, scratch=table, aliases={3: 0})
    part = call(partial_kernel, f32(9, channels, atoms), hg, rad, ylm)
    h4 = partner(sent)

    energies, raw, extra, gz = call(
        layer_two_kernel,
        [f32(1, atoms), f32(9, channels, atoms), f32(channels, atoms), b16(atoms, channels)],
        h0,
        h4,
        part,
        pairs,
        wide,
        occ,
        mix_two,
        radial_two,
        read_one,
        read_hidden,
        read_out,
        scratch=[
            pltpu.VMEM((channels, NB * atoms), BF16),
            pltpu.VMEM((channels, 9 * atoms), BF16),
        ],
    )
    rows = f32(2 * atoms, channels)
    rq, quad, gy = call(
        reverse_kernel, [b16(steps, channels, width), big, rows], raw, rad, ylm, hot
    )
    az = partner(gz)

    def edges(start, count):
        out = f32(4 * count * GROUP, atoms)
        room = [pltpu.VMEM((9, channels, atoms), F32), pltpu.VMEM((2, channels, width), F32)]
        kernel = functools.partial(edge_kernel, start)
        return call(kernel, out, h4, hot, hg, rad, slo, quad, raw, unit, scratch=room)

    cut = steps // 7
    acc, near, far = call(
        fold_z_kernel,
        [rows, b16(atoms, channels), b16(atoms, channels)],
        side,
        gy,
        az,
        fz,
    )
    dx = call(functools.partial(scatter_kernel, 0), rows, hot, rq)
    gb = edges(0, cut)
    near, far = swap_both(near, far, "gy")
    own, near, far = call(
        fold_y_kernel,
        [f32(atoms, channels), b16(half, channels), b16(half, channels)],
        side,
        acc,
        dx,
        extra,
        near,
        far,
        fy,
    )
    gc = edges(cut, steps - cut)
    near, far = swap_both(near, far, "gx")
    f0, f1, f2, f3, f4 = call(
        layer_one_reverse_kernel,
        [small] * 5,
        side,
        own,
        near,
        far,
        fx,
        amp,
        nbr,
        unit,
        rinv,
        basis,
        slope,
        gb,
        gc,
        lanes,
        radial_one,
        mix_one,
        scratch=[pltpu.VMEM((6 * entries, atoms), F32), pltpu.VMEM((40, atoms), F32)],
    )
    az = partner(f4)
    acc, near, far = call(
        force_z_kernel, [f32(8, 2 * atoms), small, small], side, f0, f1, f2, f3, az, fz
    )
    near, far = swap_both(near, far, "gy")
    own, ghost = call(force_y_kernel, [small, small], side, acc, near, far, fy)
    near, far = swap_both(ghost, ghost, "gx")
    forces, energies = call(
        force_x_kernel, [f32(3, 1, atoms), f32(1, atoms)], side, own, near, far, fx, energies
    )
    return (energies.reshape(occupancy.shape), forces.reshape(positions.shape))


def solution(mesh):
    return jax.shard_map(
        per_device,
        mesh=mesh,
        in_specs=(
            P(None, "gx", "gy", "gz", None),
            P("gx", "gy", "gz", None),
            P(None, "gx", "gy", "gz", None),
            P(None, "gx", "gy", "gz", None),
            P("gx", "gy", "gz", None, None),
            P("gx", "gy", "gz", None, None),
            P("gx", "gy", "gz", None),
            P(),
            P(),
            P(),
            P(),
            P(),
            P(),
            P(),
            P(),
        ),
        out_specs=(P("gx", "gy", "gz", None), P(None, "gx", "gy", "gz", None)),
        check_vma=False,
    )
```

```python
import functools
import math

import jax
import jax.numpy as jnp
from jax import lax
from jax.experimental import pallas as pl
from jax.experimental.pallas import tpu as pltpu
from jax.sharding import PartitionSpec as P

NB = 8
LX = 4
LY = 4
LZ = 8

SPACING = 1.8
CUTOFF = 5.0
SPREAD = 0.4
F32 = jnp.float32
BF16 = jnp.bfloat16

ROOT3 = 3.0**0.5
ROOT5 = 5.0**0.5
ROOT15 = 15.0**0.5
GROUP = 4


def dot(a, b, ca=1, cb=0, precision=None):
    return lax.dot_general(
        a, b, (((ca,), (cb,)), ((), ())), precision=precision, preferred_element_type=F32
    )


def rounded(x):
    return x.astype(BF16).astype(F32)


def dot3(a, b, ca=1, cb=0):
    a_hi, b_hi = rounded(a), rounded(b)
    left = jnp.concatenate([a_hi, a_hi, a - a_hi], axis=ca).astype(BF16)
    right = jnp.concatenate([b_hi, b - b_hi, b_hi], axis=cb).astype(BF16)
    return dot(left, right, ca, cb)


def dot_split(a, b):
    hi = rounded(b)
    right = jnp.concatenate([hi, b - hi], axis=0).astype(BF16)
    return dot(jnp.concatenate([a, a], axis=1), right)


def columns(row, count):
    hi = rounded(row)
    mid = rounded(row - hi)
    parts = jnp.concatenate([hi, mid, row - hi - mid], axis=0).astype(BF16)
    return dot(parts, jnp.ones((3, count), BF16), 0, 0)


def onehot(row, size):
    count = row.shape[-1]
    ids = lax.broadcasted_iota(jnp.int32, (size, count), 0)
    return jnp.where(ids == row, 1.0, 0.0).astype(BF16)


def lane_pick(blocks, rows):
    width = blocks[0].shape[-1]
    shift = width.bit_length() - 1
    lane = rows & (width - 1)
    block = rows >> shift
    out = jnp.take_along_axis(blocks[0], lane, axis=1)
    for index in range(1, len(blocks)):
        part = jnp.take_along_axis(blocks[index], lane, axis=1)
        out = jnp.where(block == index, part, out)
    return out


def spread_rows(row, count):
    return jnp.broadcast_to(row, (count, row.shape[-1]))


def by_side(side_ref, axis, if_odd, if_even):
    odd = side_ref[axis : axis + 1, 0 : if_odd.shape[1]] == 1
    return jnp.where(odd, if_odd, if_even)


def near_far(side_ref, axis, face_ref):
    low, high = face_ref[0:1, :], face_ref[1:2, :]
    return by_side(side_ref, axis, low, high), by_side(side_ref, axis, high, low)


def face_row(side_ref, fx_ref):
    return jnp.concatenate(near_far(side_ref, 0, fx_ref), axis=1)


def half_turn(x):
    half = x.shape[1] // 2
    return jnp.concatenate([x[:, half:], x[:, :half]], axis=1)


def low_lanes(shape):
    return lax.broadcasted_iota(jnp.int32, shape, 1) < shape[1] // 2


def shift_rows(shape, axis, amount):
    ids = lax.broadcasted_iota(jnp.int32, shape, 0)
    return jnp.where(ids == axis, amount, 0.0)


def side_kernel(side_ref):
    ids = lax.broadcasted_iota(jnp.int32, side_ref.shape, 0)
    first, second = lax.axis_index("gx") % 2, lax.axis_index("gy") % 2
    value = jnp.where(ids == 0, first, jnp.where(ids == 1, second, lax.axis_index("gz")))
    side_ref[...] = value


def pos_x_kernel(side_ref, pos_ref, fx_ref, coords_ref, send_ref):
    rows = [pos_ref[i] for i in range(3)]
    coords = jnp.concatenate(rows + [jnp.zeros_like(rows[0])] * 5, axis=0)
    coords_ref[...] = coords
    send_ref[...] = lane_pick([coords], spread_rows(face_row(side_ref, fx_ref), 8))


def pos_y_kernel(side_ref, pos_ref, near_ref, far_ref, fy_ref, p1_ref, to_near_ref, to_far_ref):
    coords = pos_ref[...]
    shape = coords.shape
    first = low_lanes(shape)
    both = jnp.where(first, near_ref[...], far_ref[...])
    both = by_side(side_ref, 0, both, half_turn(both))
    step = shift_rows(shape, 0, LX * SPACING)
    ghost = jnp.where(first, both - step, both + step)
    p1_ref[...] = ghost
    near, far = near_far(side_ref, 1, fy_ref)
    to_near_ref[...] = lane_pick([coords, ghost], spread_rows(near, 8))
    to_far_ref[...] = lane_pick([coords, ghost], spread_rows(far, 8))


def pos_z_kernel(side_ref, pos_ref, p1_ref, near_ref, far_ref, fz_ref, p2_ref, p3_ref, out_ref):
    coords = pos_ref[...]
    shape = coords.shape
    near, far = near_ref[...], far_ref[...]
    low = by_side(side_ref, 1, near, far) - shift_rows(shape, 1, LY * SPACING)
    high = by_side(side_ref, 1, far, near) + shift_rows(shape, 1, LY * SPACING)
    p2_ref[...] = low
    p3_ref[...] = high
    out_ref[...] = lane_pick([coords, p1_ref[...], low, high], spread_rows(fz_ref[...], 8))


def layer_one_kernel(
    side_ref,
    pos_ref,
    p1_ref,
    p2_ref,
    p3_ref,
    pz_ref,
    nbr_ref,
    keep_ref,
    fx_ref,
    radial_ref,
    mix_ref,
    embed_ref,
    unit_ref,
    rinv_ref,
    basis_ref,
    slope_ref,
    amp_ref,
    h0_ref,
    to_near_ref,
    to_far_ref,
    last_ref,
    mom_ref,
):
    entries, atoms = nbr_ref.shape
    nbr = nbr_ref[...]
    lane = nbr & (atoms - 1)
    block = nbr >> (atoms.bit_length() - 1)
    rise = jnp.where(side_ref[2:3, :] == 0, LZ * SPACING, -LZ * SPACING)
    last = pz_ref[...] + shift_rows(pz_ref.shape, 2, rise)
    last_ref[...] = last
    tables = [pos_ref[...], p1_ref[...], p2_ref[...], p3_ref[...], last]
    vec = []
    for axis in range(3):
        got = None
        for index, table in enumerate(tables):
            spread = spread_rows(table[axis : axis + 1, :], entries)
            part = jnp.take_along_axis(spread, lane, axis=1)
            got = part if index == 0 else jnp.where(block == index, part, got)
        vec.append(got - pos_ref[axis : axis + 1, :])
    r_sq = vec[0] * vec[0] + vec[1] * vec[1] + vec[2] * vec[2]
    dist = jnp.sqrt(r_sq)
    rinv = 1.0 / dist
    ux, uy, uz = (v * rinv for v in vec)
    rinv_ref[...] = rinv
    unit_ref[0:entries, :] = ux
    unit_ref[entries : 2 * entries, :] = uy
    unit_ref[2 * entries : 3 * entries, :] = uz
    basis, slopes = radial_parts(dist, rinv, keep_ref[...].astype(F32), True)
    for k in range(NB):
        basis_ref[k * entries : (k + 1) * entries, :] = basis[k]
        slope_ref[k * entries : (k + 1) * entries, :] = slopes[k]
    angular = harmonics(ux, uy, uz)
    for m in range(9):
        for k in range(NB):
            prod = basis[k] if m == 0 else basis[k] * angular[m]
            mom_ref[k : k + 1, m * atoms : (m + 1) * atoms] = jnp.sum(prod, axis=0, keepdims=True)
    amp = SPREAD * dot3(radial_ref[...], mom_ref[...], 0, 0)
    amp_ref[...] = amp
    inv = invariants([amp[:, m * atoms : (m + 1) * atoms] for m in range(9)])
    h1 = dot(mix_ref[...], inv, 0, 0)
    h1 = h1 + columns(embed_ref[...], atoms)
    h1b = h1.astype(BF16)
    h0_ref[...] = h1b
    both = dot(h1b, onehot(face_row(side_ref, fx_ref), atoms))
    to_near_ref[...], to_far_ref[...] = pack_halves(both)


def sine_cosine(turn):
    angle = (turn - 0.5) * math.pi
    sq = angle * angle
    even = jnp.full_like(sq, 1.0 / math.factorial(12))
    odd = jnp.full_like(sq, 1.0 / math.factorial(13))
    for order in range(5, -1, -1):
        sign = 1.0 if order % 2 == 0 else -1.0
        even = even * sq + sign / math.factorial(2 * order)
        odd = odd * sq + sign / math.factorial(2 * order + 1)
    return even, -(angle * odd)


def radial_parts(dist, rinv, weight, with_slope):
    scaled = jnp.minimum(dist * (1.0 / CUTOFF), 1.0)
    sine, cosine = sine_cosine(scaled)
    inner = 1.0 - scaled * scaled
    weight = weight * (2.0 / CUTOFF) ** 0.5
    env = weight * inner * inner * rinv
    env_slope = -env * rinv - weight * rinv * (4.0 / CUTOFF) * scaled * inner
    twice = 2.0 * cosine
    s_prev, s_now = jnp.zeros_like(sine), sine
    c_prev, c_now = jnp.ones_like(cosine), cosine
    basis, slopes = [], []
    for k in range(NB):
        basis.append(s_now * env)
        if with_slope:
            slopes.append(c_now * env * ((k + 1) * math.pi / CUTOFF) + s_now * env_slope)
            c_prev, c_now = c_now, twice * c_now - c_prev
        s_prev, s_now = s_now, twice * s_now - s_prev
    return basis, slopes


def harmonics(ux, uy, uz):
    return [
        None,
        ROOT3 * ux,
        ROOT3 * uy,
        ROOT3 * uz,
        ROOT15 * ux * uy,
        ROOT15 * uy * uz,
        0.5 * ROOT5 * (3.0 * uz * uz - 1.0),
        ROOT15 * ux * uz,
        0.5 * ROOT15 * (ux * ux - uy * uy),
    ]


def invariants(amp):
    first = amp[1] * amp[1] + amp[2] * amp[2] + amp[3] * amp[3]
    second = amp[4] * amp[4] + amp[5] * amp[5] + amp[6] * amp[6]
    second = second + amp[7] * amp[7] + amp[8] * amp[8]
    return jnp.concatenate([amp[0], first, second], axis=0).astype(BF16)


def pack_halves(both):
    rows, _ = both.shape
    top, low = both[0 : rows // 2], both[rows // 2 :]
    first = low_lanes(top.shape)
    near = jnp.where(first, top, half_turn(low))
    far = jnp.where(first, half_turn(top), low)
    return near.astype(BF16), far.astype(BF16)


def unpack_halves(low, high):
    first = low_lanes(low.shape)
    top = jnp.where(first, low, half_turn(high))
    bottom = jnp.where(first, half_turn(low), high)
    return jnp.concatenate([top, bottom], axis=0)


def feat_y_kernel(side_ref, h0_ref, near_ref, far_ref, fy_ref, h1_ref, to_near_ref, to_far_ref):
    near, far = near_ref[...].astype(F32), far_ref[...].astype(F32)
    low, high = by_side(side_ref, 0, near, far), by_side(side_ref, 0, far, near)
    ghost = unpack_halves(low, high).astype(BF16)
    h1_ref[...] = ghost
    table = jnp.concatenate([h0_ref[...], ghost], axis=1)
    size = table.shape[1]
    near, far = near_far(side_ref, 1, fy_ref)
    to_near_ref[...] = dot(table, onehot(near, size)).astype(BF16)
    to_far_ref[...] = dot(table, onehot(far, size)).astype(BF16)


def sides(side_ref, axis, near_ref, far_ref):
    near, far = near_ref[...].astype(F32), far_ref[...].astype(F32)
    low, high = by_side(side_ref, axis, near, far), by_side(side_ref, axis, far, near)
    return low.astype(BF16), high.astype(BF16)


def feat_z_kernel(side_ref, h0_ref, h1_ref, near_ref, far_ref, fz_ref, out_ref, h2_ref, h3_ref):
    low, high = sides(side_ref, 1, near_ref, far_ref)
    h2_ref[...] = low
    h3_ref[...] = high
    table = jnp.concatenate([h0_ref[...], h1_ref[...], low, high], axis=1)
    out_ref[...] = dot(table, onehot(fz_ref[...], table.shape[1])).astype(BF16)


def entry_rows(ref, first):
    return jnp.concatenate([ref[pl.ds(first + jj, 1), :] for jj in range(GROUP)], axis=1)


def hot_kernel(nbr_ref, keep_ref, hot_ref, lane_ref, count_ref):
    atoms = nbr_ref.shape[1]
    count_ref[...] = jnp.zeros_like(count_ref)
    ids = lax.broadcasted_iota(jnp.int32, (atoms, atoms), 0) + 4 * atoms

    def body(step, carry):
        first = step * GROUP
        row = entry_rows(nbr_ref, first)
        hot_ref[step] = onehot(row, hot_ref.shape[1])
        lane_ref[step] = onehot(row & (atoms - 1), atoms)
        count = count_ref[...]
        for jj in range(GROUP):
            at = pl.ds(first + jj, 1)
            count = count + jnp.where(ids == nbr_ref[at, :], keep_ref[at, :].astype(F32), 0.0)
        count_ref[...] = count
        return carry

    lax.fori_loop(0, hot_ref.shape[0], body, 0)


def pair_kernel(pos_ref, last_ref, count_ref, radial_ref, pair_ref, wide_ref):
    atoms = pos_ref.shape[1]
    weight = count_ref[...]
    vec = []
    for axis in range(3):
        vec.append(columns(last_ref[axis : axis + 1, :], atoms) - pos_ref[axis : axis + 1, :])
    r_sq = vec[0] * vec[0] + vec[1] * vec[1] + vec[2] * vec[2]
    dist = jnp.sqrt(jnp.where(weight > 0.0, r_sq, 1.0))
    rinv = 1.0 / dist
    basis, _ = radial_parts(dist, rinv, weight, False)
    angular = harmonics(*(v * rinv for v in vec))
    for k in range(NB):
        wide_ref[:, k * atoms : (k + 1) * atoms] = columns(radial_ref[k : k + 1, :], atoms)
        for m in range(9):
            value = basis[k] if m == 0 else basis[k] * angular[m]
            pair_ref[k * atoms : (k + 1) * atoms, m * atoms : (m + 1) * atoms] = value.astype(BF16)


def stack3(hi, lo):
    return jnp.concatenate([hi, lo, hi], axis=0).astype(BF16)


def radial_kernel(basis_ref, slope_ref, unit_ref, radial_ref, rad_ref, slo_ref, y_ref, rts_ref):
    entries = basis_ref.shape[0] // NB
    channels = radial_ref.shape[1]
    rt = radial_ref[...]
    hi = rt.astype(BF16).astype(F32)
    lo = rt - hi
    pad = jnp.zeros((channels - 3 * NB, channels), F32)
    rts_ref[...] = jnp.transpose(jnp.concatenate([hi, hi, lo, pad], axis=0)).astype(BF16)
    ux = unit_ref[0:entries, :]
    uy = unit_ref[entries : 2 * entries, :]
    uz = unit_ref[2 * entries : 3 * entries, :]
    for m, val in enumerate(harmonics(ux, uy, uz)):
        if m:
            y_ref[(m - 1) * entries : m * entries, :] = val

    def radial_cols(ref, first):
        cols = [ref[pl.ds(first + jj, NB, stride=entries), :] for jj in range(GROUP)]
        value = jnp.concatenate(cols, axis=1)
        top = value.astype(BF16).astype(F32)
        return stack3(top, value - top)

    rts = rts_ref[:, 0 : 3 * NB]
    for step in range(rad_ref.shape[0]):
        rad_ref[step] = dot(rts, radial_cols(basis_ref, step * GROUP))
        slo_ref[step] = dot(rts, radial_cols(slope_ref, step * GROUP))


def gather_first_kernel(h0_ref, h1_ref, hot_ref, hg_ref, table_ref):
    atoms = h0_ref.shape[1]
    table_ref[:, 0:atoms] = h0_ref[...]
    table_ref[:, atoms:] = h1_ref[...]

    for step in range(hot_ref.shape[0]):
        hg_ref[step] = dot(table_ref[...], hot_ref[step, 0 : 2 * atoms, :])


def gather_more_kernel(h2_ref, h3_ref, hot_ref, old_ref, hg_ref, table_ref):
    atoms = h2_ref.shape[1]
    table_ref[:, 0:atoms] = h2_ref[...]
    table_ref[:, atoms:] = h3_ref[...]

    for step in range(hot_ref.shape[0]):
        more = dot(table_ref[...], hot_ref[step, 2 * atoms : 4 * atoms, :])
        hg_ref[step] = old_ref[step] + more


def partial_kernel(hg_ref, rad_ref, y_ref, acc_ref):
    steps, channels, width = hg_ref.shape
    atoms = width // GROUP
    entries = steps * GROUP
    blocks = channels // 8
    acc_ref[...] = jnp.zeros_like(acc_ref)

    def accumulate(step):
        first = step * GROUP
        for pair in range(blocks // 2):
            spans = [slice(cb * 8, cb * 8 + 8) for cb in (2 * pair, 2 * pair + 1)]
            msgs = []
            for rows in spans:
                line = []
                for jj in range(GROUP):
                    cols = slice(jj * atoms, (jj + 1) * atoms)
                    line.append(hg_ref[step, rows, cols] * rad_ref[step, rows, cols])
                msgs.append(line)
            for m in range(9):
                if m:
                    at = (m - 1) * entries + first
                    yvs = [y_ref[pl.ds(at + jj, 1), :] for jj in range(GROUP)]
                for rows, line in zip(spans, msgs):
                    if m:
                        terms = [line[jj] * yvs[jj] for jj in range(GROUP)]
                    else:
                        terms = line
                    while len(terms) > 1:
                        terms = [a + b for a, b in zip(terms[::2], terms[1::2])]
                    acc_ref[m, rows, :] += terms[0]

    def body(trip, carry):
        for part in range(2):
            accumulate(2 * trip + part)
        return carry

    lax.fori_loop(0, steps // 2, body, 0)


def layer_two_kernel(
    h0_ref,
    h4_ref,
    acc_ref,
    pair_ref,
    wide_ref,
    occ_ref,
    mix_ref,
    radial_ref,
    rone_ref,
    rhid_ref,
    rout_ref,
    en_ref,
    raw_ref,
    extra_ref,
    gz_ref,
    wz_ref,
    dcat_ref,
):
    channels, atoms = h0_ref.shape
    h4 = h4_ref[...].astype(F32)
    for k in range(NB):
        cols = slice(k * atoms, (k + 1) * atoms)
        wz_ref[:, cols] = (h4 * wide_ref[:, cols]).astype(BF16)
    more = dot(wz_ref[...], pair_ref[...])
    amp = [SPREAD * (acc_ref[m] + more[:, m * atoms : (m + 1) * atoms]) for m in range(9)]
    occ = occ_ref[...].astype(F32)
    own = h0_ref[...].astype(F32)
    h2 = dot(mix_ref[...], invariants(amp), 0, 0) + own
    pre = dot3(rhid_ref[...], h2, 1, 0)
    sig = 1.0 / (1.0 + jnp.exp(-pre))
    rout = columns(rout_ref[...], atoms)
    rone = columns(rone_ref[...], atoms)
    energy = jnp.sum(own * rone, axis=0, keepdims=True)
    energy = energy + jnp.sum(rout * pre * sig, axis=0, keepdims=True)
    en_ref[...] = occ * energy
    dpre = occ * rout * sig * (1.0 + pre * (1.0 - sig))
    dh2 = dot3(rhid_ref[...], dpre, 0, 0)
    dinv = dot_split(mix_ref[...], dh2)
    low = dinv[channels : 2 * channels]
    top = dinv[2 * channels :]
    extra_ref[...] = dh2 + occ * rone
    twice = 2.0 * SPREAD
    for m in range(9):
        value = (twice * amp[m]) * (low if m < 4 else top) if m else SPREAD * dinv[0:channels]
        raw_ref[m] = value
        dcat_ref[:, m * atoms : (m + 1) * atoms] = value.astype(BF16)
    back = dot(pair_ref[...], dcat_ref[...], 1, 1)
    total = None
    for k in range(NB):
        part = radial_ref[k : k + 1, :] * back[k * atoms : (k + 1) * atoms, :]
        total = part if total is None else total + part
    gz_ref[...] = total.astype(BF16)


def reverse_kernel(raw_ref, rad_ref, y_ref, hot_ref, rq_ref, q_ref, gy_ref):
    steps, channels, width = rad_ref.shape
    atoms = width // GROUP
    entries = steps * GROUP
    blocks = channels // 8

    def reverse(step):
        first = step * GROUP
        for pair in range(blocks // 2):
            spans = [slice(cb * 8, cb * 8 + 8) for cb in (2 * pair, 2 * pair + 1)]
            ds = [[raw_ref[m, rows, :] for m in range(9)] for rows in spans]
            for jj in range(GROUP):
                cols = slice(jj * atoms, (jj + 1) * atoms)
                yvs = [y_ref[pl.ds((m - 1) * entries + first + jj, 1), :] for m in range(1, 9)]
                parts = []
                for rows, d in zip(spans, ds):
                    terms = [d[0]] + [yv * dm for yv, dm in zip(yvs, d[1:])]
                    q = terms[0] + terms[1]
                    for a, b in ((2, 3), (4, 5), (6, 7)):
                        q = q + (terms[a] + terms[b])
                    q = q + terms[8]
                    q_ref[step, rows, cols] = q
                    parts.append(rad_ref[step, rows, cols] * q)
                value = jnp.concatenate(parts, axis=0).astype(BF16)
                rq_ref[step, pair * 16 : pair * 16 + 16, cols] = value

    def scatter(step):
        parts = []
        for at in (step, step + 1):
            parts.append(dot(hot_ref[at, 2 * atoms : 4 * atoms, :], rq_ref[at], 1, 1))
        return parts[0] + parts[1]

    total = None
    for step in range(0, steps, 2):
        reverse(step)
        reverse(step + 1)
        part = scatter(step)
        total = part if total is None else total + part
    gy_ref[...] = total


def scatter_kernel(first, hot_ref, rq_ref, out_ref):
    size = out_ref.shape[0]
    total = None
    for step in range(hot_ref.shape[0]):
        part = dot(hot_ref[step, first : first + size, :], rq_ref[step], 1, 1)
        total = part if total is None else total + part
    out_ref[...] = total


def edge_kernel(
    start,
    h4_ref,
    hot_ref,
    old_ref,
    rad_ref,
    slo_ref,
    q_ref,
    d_ref,
    unit_ref,
    grad_ref,
    dd_ref,
    hg_ref,
):
    channels, atoms = d_ref.shape[1:]
    steps = old_ref.shape[0]
    entries = steps * GROUP
    count = grad_ref.shape[0] // (4 * GROUP)
    for m in range(1, 9):
        if m < 4:
            dd_ref[m] = ROOT3 * d_ref[m]
        else:
            dd_ref[m] = (3.0 * ROOT5 if m == 6 else ROOT15) * d_ref[m]

    def prepare(step, slot):
        hg_ref[slot] = old_ref[step] + dot(h4_ref[...], hot_ref[step, 4 * atoms :, :])

    def edges(step, slot):
        first = step * GROUP
        units = []
        for jj in range(GROUP):
            units.append([unit_ref[pl.ds(i * entries + first + jj, 1), :] for i in range(3)])
        sums = [[None] * 4 for _ in range(GROUP)]
        for cb in range(channels // 8):
            rows = slice(cb * 8, cb * 8 + 8)
            d = [None] + [dd_ref[m, rows, :] for m in range(1, 9)]
            for jj in range(GROUP):
                cols = slice(jj * atoms, (jj + 1) * atoms)
                hg = hg_ref[slot, rows, cols]
                vx, vy, vz = units[jj]
                msg = hg * rad_ref[step, rows, cols]
                parts = [
                    msg * ((d[1] + vy * d[4]) + (vz * d[7] + vx * d[8])),
                    msg * ((d[2] + vx * d[4]) + (vz * d[5] - vy * d[8])),
                    msg * ((d[3] + vy * d[5]) + (vx * d[7] + vz * d[6])),
                    hg * q_ref[step, rows, cols] * slo_ref[step, rows, cols],
                ]
                for i in range(4):
                    prior = sums[jj][i]
                    sums[jj][i] = parts[i] if prior is None else prior + parts[i]
        for jj in range(GROUP):
            for i in range(4):
                row = pl.ds(i * count * GROUP + first - start * GROUP + jj, 1)
                grad_ref[row, :] = jnp.sum(sums[jj][i], axis=0, keepdims=True)

    prepare(start, 0)
    prepare(start + 1, 1)

    def body(trip, carry):
        step = start + 2 * trip
        for part in range(2):
            edges(step + part, part)
        for part in range(2):
            prepare(jnp.minimum(step + 2 + part, steps - 1), part)
        return carry

    lax.fori_loop(0, count // 2, body, 0)


def fold_z_kernel(side_ref, gy_ref, az_ref, fz_ref, acc_ref, to_near_ref, to_far_ref):
    size = gy_ref.shape[0]
    quarter = size // 2
    add = dot(onehot(fz_ref[...], 2 * size), az_ref[...])
    acc_ref[...] = add[0:size]
    rows = rounded(gy_ref[...]) + add[size:]
    low, high = rows[0:quarter], rows[quarter:]
    to_near_ref[...] = by_side(side_ref, 1, low, high).astype(BF16)
    to_far_ref[...] = by_side(side_ref, 1, high, low).astype(BF16)


def fold_y_kernel(
    side_ref, acc_ref, gx_ref, extra_ref, near_ref, far_ref, fy_ref, own_ref, to_near_ref, to_far_ref
):
    size = acc_ref.shape[0]
    half = size // 2
    quarter = half // 2
    near, far = near_far(side_ref, 1, fy_ref)
    rows = acc_ref[...] + dot(onehot(near, size), near_ref[...])
    rows = rows + dot(onehot(far, size), far_ref[...])
    own = gx_ref[0:half, :] + jnp.transpose(extra_ref[...])
    own_ref[...] = rows[0:half] + own.astype(BF16).astype(F32)
    ghost = rows[half:] + gx_ref[half:, :].astype(BF16).astype(F32)
    low, high = ghost[0:quarter], ghost[quarter:]
    to_near_ref[...] = by_side(side_ref, 0, low, high).astype(BF16)
    to_far_ref[...] = by_side(side_ref, 0, high, low).astype(BF16)


def layer_one_reverse_kernel(
    side_ref,
    own_ref,
    near_ref,
    far_ref,
    fx_ref,
    amp_ref,
    nbr_ref,
    unit_ref,
    rinv_ref,
    basis_ref,
    slope_ref,
    gb_ref,
    gc_ref,
    lane_ref,
    radial_ref,
    mix_ref,
    f0_ref,
    f1_ref,
    f2_ref,
    f3_ref,
    f4_ref,
    dv_ref,
    sc_ref,
):
    entries, atoms = nbr_ref.shape
    channels = own_ref.shape[1]
    rows = own_ref[...]
    near, far = near_far(side_ref, 0, fx_ref)
    rows = rows + dot(onehot(near, atoms), near_ref[...])
    rows = rows + dot(onehot(far, atoms), far_ref[...])
    cot = jnp.transpose(rows)
    dinv = dot_split(mix_ref[...], cot)
    low = dinv[channels : 2 * channels]
    top = dinv[2 * channels :]
    pieces = [dinv[0:channels]]
    for m in range(1, 9):
        amp = amp_ref[:, m * atoms : (m + 1) * atoms]
        pieces.append(2.0 * amp * (low if m < 4 else top))
    dmom = SPREAD * dot3(radial_ref[...], jnp.concatenate(pieces, axis=1), 1, 0)
    ux = unit_ref[0:entries, :]
    uy = unit_ref[entries : 2 * entries, :]
    uz = unit_ref[2 * entries : 3 * entries, :]
    basis = [basis_ref[k * entries : (k + 1) * entries, :] for k in range(NB)]
    slope = [slope_ref[k * entries : (k + 1) * entries, :] for k in range(NB)]
    angular = harmonics(ux, uy, uz)
    edge = []
    for i in range(4):
        rows = []
        for ref in (gb_ref, gc_ref):
            count = ref.shape[0] // 4
            rows.append(ref[i * count : (i + 1) * count, :])
        edge.append(jnp.concatenate(rows, axis=0))
    dr = edge[3]
    dy = []
    for m in range(9):
        part = None
        sl = None
        for k in range(NB):
            row = dmom[k : k + 1, m * atoms : (m + 1) * atoms]
            sl = slope[k] * row if sl is None else sl + slope[k] * row
            if m:
                part = basis[k] * row if part is None else part + basis[k] * row
        dr = dr + (sl if m == 0 else sl * angular[m])
        dy.append(part)
    wx = edge[0] + ROOT3 * dy[1]
    wx = wx + ROOT15 * (uy * dy[4] + uz * dy[7] + ux * dy[8])
    wy = edge[1] + ROOT3 * dy[2]
    wy = wy + ROOT15 * (ux * dy[4] + uz * dy[5] - uy * dy[8])
    wz = edge[2] + ROOT3 * dy[3]
    wz = wz + ROOT15 * (uy * dy[5] + ux * dy[7]) + (3.0 * ROOT5) * uz * dy[6]
    rinv = rinv_ref[...]
    along = dr - rinv * (ux * wx + uy * wy + uz * wz)
    grads = [wx * rinv + along * ux, wy * rinv + along * uy, wz * rinv + along * uz]
    centre = []
    for i in range(3):
        centre.append(jnp.sum(grads[i], axis=0, keepdims=True))
        top16 = grads[i].astype(BF16).astype(F32)
        dv_ref[i * entries : (i + 1) * entries, :] = top16
        dv_ref[(3 + i) * entries : (4 + i) * entries, :] = grads[i] - top16
    shift = atoms.bit_length() - 1
    total = None
    for step in range(entries // GROUP):
        first = step * GROUP
        block = entry_rows(nbr_ref, first) >> shift
        cols = [dv_ref[pl.ds(first + jj, 6, stride=entries), :] for jj in range(GROUP)]
        value = jnp.concatenate(cols, axis=1)
        value = jnp.concatenate([value, jnp.zeros_like(value[0:2])], axis=0)
        parts = [jnp.where(block == index, value, 0.0) for index in range(5)]
        part = dot(jnp.concatenate(parts, axis=0).astype(BF16), lane_ref[step], 1, 1)
        total = part if total is None else total + part
    sc_ref[...] = total
    zero = jnp.zeros((5, atoms), F32)
    own = jnp.concatenate(centre + [zero], axis=0)
    for index, ref in enumerate((f0_ref, f1_ref, f2_ref, f3_ref, f4_ref)):
        base = index * 8
        value = sc_ref[base : base + 3, :] + sc_ref[base + 3 : base + 6, :]
        value = jnp.concatenate([value, zero], axis=0)
        ref[...] = value - own if index == 0 else value


def scatter_lanes(values, row, size):
    hi = rounded(values)
    mid = rounded(values - hi)
    parts = jnp.concatenate([hi, mid, values - hi - mid], axis=0).astype(BF16)
    out = dot(parts, onehot(row, size), 1, 1)
    rows = values.shape[0]
    return out[0:rows] + out[rows : 2 * rows] + out[2 * rows :]


def force_z_kernel(
    side_ref, f0_ref, f1_ref, f2_ref, f3_ref, az_ref, fz_ref, out_ref, to_near_ref, to_far_ref
):
    atoms = f0_ref.shape[1]
    add = scatter_lanes(az_ref[...], fz_ref[...], 4 * atoms)
    out_ref[:, 0:atoms] = f0_ref[...] + add[:, 0:atoms]
    out_ref[:, atoms : 2 * atoms] = f1_ref[...] + add[:, atoms : 2 * atoms]
    low = f2_ref[...] + add[:, 2 * atoms : 3 * atoms]
    high = f3_ref[...] + add[:, 3 * atoms :]
    to_near_ref[...] = by_side(side_ref, 1, low, high)
    to_far_ref[...] = by_side(side_ref, 1, high, low)


def force_y_kernel(side_ref, acc_ref, near_ref, far_ref, fy_ref, own_ref, ghost_ref):
    size = acc_ref.shape[1]
    rows = acc_ref[...]
    near, far = near_far(side_ref, 1, fy_ref)
    rows = rows + scatter_lanes(near_ref[...], near, size)
    rows = rows + scatter_lanes(far_ref[...], far, size)
    own_ref[...] = rows[:, 0 : size // 2]
    ghost = rows[:, size // 2 :]
    ghost_ref[...] = by_side(side_ref, 0, ghost, half_turn(ghost))


def force_x_kernel(side_ref, own_ref, near_ref, far_ref, fx_ref, en_ref, out_ref, total_ref):
    total_ref[...] = en_ref[...]
    size = own_ref.shape[1]
    both = jnp.where(low_lanes(own_ref.shape), near_ref[...], far_ref[...])
    rows = own_ref[...] + scatter_lanes(both, face_row(side_ref, fx_ref), size)
    for i in range(3):
        out_ref[i] = -rows[i : i + 1]


def call(kernel, outs, *args, scratch=(), vmem=8, aliases={}, cost=1):
    specs = []
    for arg in args:
        specs.append(pl.BlockSpec(memory_space=pltpu.VMEM))
    single = not isinstance(outs, (list, tuple))
    shapes = [outs] if single else list(outs)
    result = pl.pallas_call(
        kernel,
        out_shape=shapes,
        in_specs=specs,
        out_specs=[pl.BlockSpec(memory_space=pltpu.VMEM)] * len(shapes),
        scratch_shapes=list(scratch),
        input_output_aliases=aliases,
        cost_estimate=pl.CostEstimate(
            flops=cost * 10**9, bytes_accessed=cost * 10**6, transcendentals=0
        ),
        compiler_params=pltpu.CompilerParams(vmem_limit_bytes=vmem * 1024 * 1024),
    )(*args)
    return result[0] if single else result


def pair_swap(x, axis, far):
    count = lax.axis_size(axis)
    assert count % 2 == 0
    pairs = []
    for i in range(count):
        up = (i % 2 == 0) != far
        pairs.append((i, (i + (1 if up else -1)) % count))
    return lax.ppermute(x, axis, pairs)


def partner(x):
    axis = "gz"
    return lax.ppermute(x, axis, [(i, i ^ 1) for i in range(lax.axis_size(axis))])


def swap_both(near, far, axis):
    from_far = pair_swap(far, axis, True)
    from_near = pair_swap(near, axis, False)
    return from_near, from_far


def per_device(
    positions,
    occupancy,
    neighbours,
    keep,
    face_x,
    face_y,
    face_z,
    radial_one,
    mix_one,
    embed,
    radial_two,
    mix_two,
    read_one,
    read_hidden,
    read_out,
):
    atoms = positions.shape[-1]
    entries = neighbours.shape[0]
    channels = radial_one.shape[1]
    pos = positions.reshape(3, 1, atoms)
    nbr = neighbours.reshape(entries, atoms)
    kept = keep.reshape(entries, atoms)
    occ = occupancy.reshape(1, atoms)
    fx = face_x.reshape(2, face_x.shape[-1])
    fy = face_y.reshape(2, face_y.shape[-1])
    fz = face_z.reshape(1, face_z.shape[-1])
    embed = embed.reshape(1, channels)
    read_one = read_one.reshape(1, channels)
    read_out = read_out.reshape(1, read_out.shape[0])
    read_hidden = read_hidden.T

    def f32(*shape):
        return jax.ShapeDtypeStruct(shape, F32)

    def b16(*shape):
        return jax.ShapeDtypeStruct(shape, BF16)

    small = f32(8, atoms)
    side = jax.ShapeDtypeStruct((8, atoms), jnp.int32)
    side = call(side_kernel, side)
    pos, sent = call(pos_x_kernel, [small, small], side, pos, fx)
    steps = entries // GROUP
    width = GROUP * atoms
    hot, lanes, count = call(
        hot_kernel,
        [b16(steps, 5 * atoms, width), b16(steps, atoms, width), f32(atoms, atoms)],
        nbr,
        kept,
    )
    near, far = swap_both(sent, sent, "gx")
    p1, near, far = call(pos_y_kernel, [small] * 3, side, pos, near, far, fy)
    near, far = swap_both(near, far, "gy")
    p2, p3, sent = call(pos_z_kernel, [small] * 3, side, pos, p1, near, far, fz)
    pz = partner(sent)

    half = atoms // 2
    square = b16(channels, atoms)
    unit, rinv, basis, slope, amp, h0, near, far, last = call(
        layer_one_kernel,
        [
            f32(3 * entries, atoms),
            f32(entries, atoms),
            f32(NB * entries, atoms),
            f32(NB * entries, atoms),
            f32(channels, 9 * atoms),
            square,
            b16(channels // 2, atoms),
            b16(channels // 2, atoms),
            small,
        ],
        side,
        pos,
        p1,
        p2,
        p3,
        pz,
        nbr,
        kept,
        fx,
        radial_one,
        mix_one,
        embed,
        scratch=[pltpu.VMEM((NB, 9 * atoms), F32)],
    )
    big = f32(steps, channels, width)
    rad, slo, ylm = call(
        radial_kernel,
        [big, big, f32(8 * entries, atoms)],
        basis,
        slope,
        unit,
        radial_two,
        scratch=[pltpu.VMEM((channels, channels), BF16)],
    )
    pairs, wide = call(
        pair_kernel,
        [b16(NB * atoms, 9 * atoms), f32(channels, NB * atoms)],
        pos,
        last,
        count,
        radial_two,
    )
    near, far = swap_both(near, far, "gx")
    h1, near, far = call(feat_y_kernel, [square] * 3, side, h0, near, far, fy)
    table = [pltpu.VMEM((channels, 2 * atoms), BF16)]
    hg = call(gather_first_kernel, big, h0, h1, hot, scratch=table)
    near, far = swap_both(near, far, "gy")
    sent, h2, h3 = call(feat_z_kernel, [square] * 3, side, h0, h1, near, far, fz)
    hg = call(gather_more_kernel, big, h2, h3, hot, hg, scratch=table, aliases={3: 0})
    part = call(partial_kernel, f32(9, channels, atoms), hg, rad, ylm)
    h4 = partner(sent)

    energies, raw, extra, gz = call(
        layer_two_kernel,
        [f32(1, atoms), f32(9, channels, atoms), f32(channels, atoms), b16(atoms, channels)],
        h0,
        h4,
        part,
        pairs,
        wide,
        occ,
        mix_two,
        radial_two,
        read_one,
        read_hidden,
        read_out,
        scratch=[
            pltpu.VMEM((channels, NB * atoms), BF16),
            pltpu.VMEM((channels, 9 * atoms), BF16),
        ],
    )
    rows = f32(2 * atoms, channels)
    rq, quad, gy = call(
        reverse_kernel, [b16(steps, channels, width), big, rows], raw, rad, ylm, hot
    )
    az = partner(gz)

    def edges(start, count):
        out = f32(4 * count * GROUP, atoms)
        room = [pltpu.VMEM((9, channels, atoms), F32), pltpu.VMEM((2, channels, width), F32)]
        kernel = functools.partial(edge_kernel, start)
        return call(kernel, out, h4, hot, hg, rad, slo, quad, raw, unit, scratch=room)

    cut = steps // 7
    acc, near, far = call(
        fold_z_kernel,
        [rows, b16(atoms, channels), b16(atoms, channels)],
        side,
        gy,
        az,
        fz,
    )
    dx = call(functools.partial(scatter_kernel, 0), rows, hot, rq)
    gb = edges(0, cut)
    near, far = swap_both(near, far, "gy")
    own, near, far = call(
        fold_y_kernel,
        [f32(atoms, channels), b16(half, channels), b16(half, channels)],
        side,
        acc,
        dx,
        extra,
        near,
        far,
        fy,
    )
    gc = edges(cut, steps - cut)
    near, far = swap_both(near, far, "gx")
    f0, f1, f2, f3, f4 = call(
        layer_one_reverse_kernel,
        [small] * 5,
        side,
        own,
        near,
        far,
        fx,
        amp,
        nbr,
        unit,
        rinv,
        basis,
        slope,
        gb,
        gc,
        lanes,
        radial_one,
        mix_one,
        scratch=[pltpu.VMEM((6 * entries, atoms), F32), pltpu.VMEM((40, atoms), F32)],
    )
    az = partner(f4)
    acc, near, far = call(
        force_z_kernel, [f32(8, 2 * atoms), small, small], side, f0, f1, f2, f3, az, fz
    )
    near, far = swap_both(near, far, "gy")
    own, ghost = call(force_y_kernel, [small, small], side, acc, near, far, fy)
    near, far = swap_both(ghost, ghost, "gx")
    forces, energies = call(
        force_x_kernel, [f32(3, 1, atoms), f32(1, atoms)], side, own, near, far, fx, energies
    )
    return (energies.reshape(occupancy.shape), forces.reshape(positions.shape))


def solution(mesh):
    return jax.shard_map(
        per_device,
        mesh=mesh,
        in_specs=(
            P(None, "gx", "gy", "gz", None),
            P("gx", "gy", "gz", None),
            P(None, "gx", "gy", "gz", None),
            P(None, "gx", "gy", "gz", None),
            P("gx", "gy", "gz", None, None),
            P("gx", "gy", "gz", None, None),
            P("gx", "gy", "gz", None),
            P(),
            P(),
            P(),
            P(),
            P(),
            P(),
            P(),
            P(),
        ),
        out_specs=(P("gx", "gy", "gz", None), P(None, "gx", "gy", "gz", None)),
        check_vma=False,
    )
```
